32 devices in a mesh: tile: 16 (over z, x, core), mem: 2 (over y).
Axes of the slice: x: 2, y: 2, z: 4, core: 2. Of those that a mesh axis runs over, the one named last changes fastest.
Arguments:
- anomalies: bfloat16 [80, 137, 2048], P('mem', None, 'tile'), may hold values from -6 to 6
- analysis_weights: bfloat16 [16, 80, 80], P('tile'), may hold values from -0.6 to 1.7
- background_mean: bfloat16 [137, 2048], P(None, 'tile'), may hold values from -6 to 6
- background: bfloat16 [80, 137, 2048], P('mem', None, 'tile'), may hold values from -6 to 6
- jacobian_table: bfloat16 [8461, 137], replicated, may hold values from -0.5 to 0.5
- channel_list: int32 [96], replicated, may hold values from 0 to 8460
- send_slots: int32 [16, 16, 32], P('tile'), may hold values from -1 to 127, as said below
- footprint: int32 [8192, 4], P('tile'), may hold values from 0 to 511, as said below
- footprint_weight: bfloat16 [8192, 4], P('tile'), may hold values from 0.25 to 1
- channel_bias: float32 [96], replicated, may hold values from -4 to 4
Outputs:
- analysis_members: bfloat16 [80, 137, 2048], P('mem', None, 'tile')
- radiance_prior: float32 [96, 80, 8192], P(None, 'mem', 'tile')
The draws below stay inside these ranges and needn't reach their ends.
Inputs may be any that keep to these rules, and one draw needn't show every extreme that they name: `send_slots`: entry [s, d, i] is a column within owner s's block of 128 columns that owner s sends to tile d in slot i, or -1 for an empty slot; the filled slots of a pair come first, each pair fills 1 to 32 slots, and in every draw one tile receives 32 filled slots from every owner. `footprint`: entry [o, j] is a slot of the buffer of observation o's tile, which holds 32 slots from each owner in owner order; every entry names a filled slot, the 4 entries of a row differ, and every filled slot is named by some row of that tile.
All inputs are finite; a program needn't handle non-finite values.
Results may differ from the reference program's by a relative error of at most 0.0021.
Values may be sent and summed in bfloat16 or wider, within the bound.
A program may use at most 128 MiB of HBM per device.

```python
import math
import jax
import jax.numpy as jnp
from jax import lax

MEMBERS = 80
LEVELS = 137
SPECTRUM = 8461
CHANNELS = 96
COLS_DEV = 128
GROUP = 128
SLOTS = 32
OBS_DEV = 512
FOOT = 4
COLUMNS = 2048
POINTS = 16
OBSERVATIONS = 8192
N_TILE = 16


def draw_analysis_weights(key, part):
    identity = jnp.eye(MEMBERS, dtype=jnp.float32)[None]
    noise_draw = jnp.clip(jax.random.normal(jax.random.fold_in(key, 1), (POINTS, MEMBERS, MEMBERS), jnp.float32), -4.0, 4.0)
    diag_part = identity
    return (diag_part + noise_draw * (0.6 / math.sqrt(MEMBERS))).astype(jnp.bfloat16)


def slot_counts(key):
    tile_count = COLUMNS // COLS_DEV
    uniform_part = jax.random.randint(jax.random.fold_in(key, 11), (tile_count, tile_count), 1, SLOTS + 1)
    receiver_load = jax.random.randint(jax.random.fold_in(key, 12), (1, tile_count), 1, 5)
    counts = jnp.clip(uniform_part * receiver_load // 3, 1, SLOTS)
    full_receiver = jax.random.randint(jax.random.fold_in(key, 13), (), 0, tile_count)
    counts = jnp.where(jnp.arange(tile_count)[None, :] == full_receiver, SLOTS, counts)
    return counts.astype(jnp.int32)


def draw_send_slots(key, part):
    tile_count = COLUMNS // COLS_DEV
    counts = slot_counts(key)
    columns = jax.random.randint(jax.random.fold_in(key, 14), (tile_count, tile_count, SLOTS), 0, COLS_DEV)
    filled = jnp.arange(SLOTS)[None, None, :] < counts[:, :, None]
    return jnp.where(filled, columns, -1).astype(jnp.int32)


def draw_footprint(key, part):
    tile_count = COLUMNS // COLS_DEV
    buffer_size = tile_count * SLOTS
    counts = slot_counts(key)
    filled = jnp.arange(SLOTS)[None, None, :] < jnp.transpose(counts)[:, :, None]
    filled = filled.reshape(tile_count, buffer_size)
    receiver_keys = jax.random.split(jax.random.fold_in(key, 15), tile_count)

    def shuffle_one(subkey):
        return jax.random.permutation(subkey, buffer_size).astype(jnp.int32)
    shuffle = jax.vmap(shuffle_one)(receiver_keys)
    scores = jnp.where(filled, shuffle, buffer_size + shuffle)
    slot_order = jnp.argsort(scores, axis=1, stable=True).astype(jnp.int32)
    filled_count = jnp.sum(filled.astype(jnp.int32), axis=1, keepdims=True)
    position = jnp.arange(OBS_DEV * FOOT, dtype=jnp.int32)[None, :] % filled_count
    foot_slots = jnp.take_along_axis(slot_order, position, axis=1)
    return foot_slots.reshape(tile_count * OBS_DEV, FOOT).astype(jnp.int32)


def set_ends(entries, stream_key, low, high):
    longest = entries.shape.index(max(entries.shape))
    spots = []
    for shift in (0, 1):
        where = [jax.random.randint(jax.random.fold_in(stream_key, axis), (), 0, length) for axis, length in enumerate(entries.shape)]
        where[longest] = (where[longest] + shift) % entries.shape[longest]
        spots.append(tuple(where))
    return entries.at[spots[0]].set(low).at[spots[1]].set(high)


def levels(key, extent, shards, low, largest):
    factor_of = 1.0
    for dim, parts in shards:
        draws = jax.random.uniform(jax.random.fold_in(jax.random.fold_in(key, 6), dim), (parts,), jnp.float32, low / len(shards), largest / len(shards))
        factor_of = factor_of * jnp.repeat(jnp.exp(draws), extent[dim] // parts).reshape((-1,) + (1,) * (len(extent) - 1 - dim))
    return factor_of


def gaussian(rng, shape, scale, limit, shards=(), kind=jnp.bfloat16):
    values = scale * jax.random.normal(rng, shape, jnp.float32)
    if shards:
        values = values * levels(rng, shape, shards, -0.22, 0.18)
    return jnp.clip(values, -limit, limit).astype(kind)


def setup_inputs(seed: int = 0) -> dict:
    key_list = jax.random.split(jax.random.key(seed), 11)
    anomalies = gaussian(key_list[0], (MEMBERS, LEVELS, COLUMNS), 1.0, 6.0, ((0, 2), (2, 16)))
    analysis_weights = draw_analysis_weights(jax.random.fold_in(key_list[10], 71), 0)
    background_mean = gaussian(key_list[2], (LEVELS, COLUMNS), 1.0, 6.0, ((1, 16),))
    background = gaussian(key_list[3], (MEMBERS, LEVELS, COLUMNS), 1.0, 6.0, ((0, 2), (2, 16)))
    jacobian_table = gaussian(key_list[4], (SPECTRUM, LEVELS), LEVELS ** -0.5, 0.5)
    channel_list = set_ends(jax.random.randint(key_list[5], (CHANNELS,), 0, SPECTRUM), jax.random.fold_in(key_list[5], 1), 0, SPECTRUM - 1).astype(jnp.int32)
    send_slots = draw_send_slots(jax.random.fold_in(key_list[10], 71), 0)
    footprint = draw_footprint(jax.random.fold_in(key_list[10], 71), 0)
    footprint_weight = jnp.clip(jnp.exp(math.log(1.0) - 1.3862944 * jax.random.uniform(key_list[8], (OBSERVATIONS, FOOT), jnp.float32) ** levels(key_list[8], (OBSERVATIONS, FOOT), ((0, 16),), -0.2, 0.2)), 0.25, 1.0).astype(jnp.bfloat16)
    channel_bias = gaussian(key_list[9], (CHANNELS,), 1.0, 4.0, (), jnp.float32)
    return {"anomalies": anomalies, "analysis_weights": analysis_weights, "background_mean": background_mean, "background": background, "jacobian_table": jacobian_table, "channel_list": channel_list, "send_slots": send_slots, "footprint": footprint, "footprint_weight": footprint_weight, "channel_bias": channel_bias}


def reference(anomalies, analysis_weights, background_mean, background, jacobian_table, channel_list, send_slots, footprint, footprint_weight, channel_bias):
    points = analysis_weights.shape[0]
    shaped = anomalies.astype(jnp.float32).reshape(MEMBERS, LEVELS, points, GROUP)
    mixture = jnp.einsum('klgc,gkm->mlgc', shaped, analysis_weights.astype(jnp.float32))
    mixture = mixture.reshape(MEMBERS, LEVELS, points * GROUP)
    analysis_members = (background_mean.astype(jnp.float32)[None] + mixture).astype(jnp.bfloat16)

    selected = jnp.take(jacobian_table, channel_list, axis=0).astype(jnp.float32)
    foot_slots = footprint.reshape(N_TILE, OBS_DEV, FOOT)
    foot_weight = footprint_weight.astype(jnp.float32).reshape(N_TILE, OBS_DEV, FOOT)

    def per_receiver(receiver):
        slot_ids = lax.dynamic_index_in_dim(foot_slots, receiver, 0, keepdims=False)
        weight = lax.dynamic_index_in_dim(foot_weight, receiver, 0, keepdims=False)
        source = (slot_ids // SLOTS).astype(jnp.int32)
        slot_place = (slot_ids % SLOTS).astype(jnp.int32)
        local_col = send_slots[source, receiver, slot_place]
        column = (source * COLS_DEV + local_col).astype(jnp.int32)
        profiles = jnp.take(background, column.reshape(-1), axis=2).astype(jnp.float32)
        radiance = jnp.einsum('cl,kls->cks', selected, profiles).astype(jnp.bfloat16)
        radiance = lax.optimization_barrier(radiance).astype(jnp.float32)
        radiance = radiance.reshape(CHANNELS, MEMBERS, OBS_DEV, FOOT)
        combined = jnp.sum(radiance * weight[None, None], axis=3)
        return combined + channel_bias.astype(jnp.float32)[:, None, None]

    stacked = lax.map(per_receiver, jnp.arange(N_TILE, dtype=jnp.int32))
    radiance_prior = jnp.transpose(stacked, (1, 2, 0, 3)).reshape(CHANNELS, MEMBERS, N_TILE * OBS_DEV)
    return analysis_members, radiance_prior
```

```python
import functools

import jax
import jax.numpy as jnp
from jax import lax
from jax.experimental import pallas as pl
from jax.experimental.pallas import tpu as pltpu
from jax.sharding import PartitionSpec as P

LANES = 128
MESH = pl.DeviceIdType.MESH
ZONES = 4

OWN, OUTER, PARTNER, FAR = range(4)
NEAR_ZONE = (0, 1, 2, 3)
AWAY = {OWN: 4, PARTNER: 5, FAR: 6}


def exchange_kernel(
    n,
    nm,
    chunks,
    owned_ref,
    slots_ref,
    anom_ref,
    weight_ref,
    mean_ref,
    foot_ref,
    fweight_ref,
    recv_ref,
    analysis_ref,
    spread_ref,
    send_buf,
    block_buf,
    own_table,
    tables,
    picks,
    pieces,
    mixed,
    spread,
    mean_wide,
    weight_wide,
    stream_send,
    stream_recv,
    table_send,
    table_recv,
    m_send,
    m_recv,
    p_send,
    a_recv,
    local_sem,
):
    tile = lax.axis_index("tile")
    mem = lax.axis_index("mem")
    rows, cols = owned_ref.shape
    slots = slots_ref.shape[1]
    groups = LANES // slots
    obs = foot_ref.shape[1]
    levels, mem_dev = anom_ref.shape[0], anom_ref.shape[1]
    zone_tiles = n // ZONES
    pairs = zone_tiles // 2
    chunk = rows // chunks
    part = chunk // groups

    zone = tile // zone_tiles
    place = lax.rem(tile, zone_tiles)
    sign = 1 - 2 * (zone // 2)
    inner = jnp.logical_or(zone == 1, zone == 2)
    outer = jnp.logical_not(inner)
    stride = sign * zone_tiles
    ahead = lax.rem(tile + stride + n, n)
    source = (
        tile,
        lax.rem(tile - stride + n, n),
        ahead,
        lax.rem(tile + 2 * stride + n, n),
    )
    zone_base = zone * zone_tiles
    away_base = lax.rem(zone_base - stride + n, n)

    barrier = pltpu.get_barrier_semaphore()

    def greet(k, carry):
        pl.semaphore_signal(
            barrier, inc=1, device_id=(lax.rem(tile + k, n), mem), device_id_type=MESH
        )
        return carry

    lax.fori_loop(1, n, greet, 0)
    for k in range(1, nm):
        pl.semaphore_signal(
            barrier, inc=1, device_id=(tile, lax.rem(mem + k, nm)), device_id_type=MESH
        )
    own_piece = pltpu.make_async_copy(anom_ref, pieces.at[mem], local_sem.at[0])
    own_piece.start()

    columns = jnp.maximum(slots_ref[...], 0)
    own_table[...] = jnp.concatenate([columns + g * cols for g in range(groups)], axis=1)

    def build(table_ref, base, combo):
        row_id = lax.broadcasted_iota(jnp.int32, (groups * cols, 2 * LANES), 0)

        def pair(h, carry):
            first = base + 2 * h
            want = jnp.concatenate(
                [table_ref[pl.ds(first, 1), :], table_ref[pl.ds(first + 1, 1), :]], axis=1
            )
            picks[combo, h] = jnp.where(row_id == want, 1.0, 0.0).astype(jnp.bfloat16)
            return carry

        lax.fori_loop(0, pairs, pair, 0)

    build(own_table, zone_base, NEAR_ZONE[OWN])

    @pl.when(inner)
    def _():
        build(own_table, away_base, AWAY[OWN])

    pl.semaphore_wait(barrier, n - 1 + nm - 1)

    def span(c):
        return pl.ds(pl.multiple_of(c * chunk, chunk), chunk)

    def narrow(c):
        return pl.ds(pl.multiple_of(c * part, part), part)

    landing = jnp.where(inner, 1, 0)

    def own_stream(c):
        return pltpu.make_async_remote_copy(
            src_ref=owned_ref.at[span(c)],
            dst_ref=block_buf.at[landing, span(c)],
            send_sem=stream_send.at[0, c],
            recv_sem=stream_recv.at[landing, c],
            device_id=(ahead, mem),
            device_id_type=MESH,
        )

    def own_table_copy():
        return pltpu.make_async_remote_copy(
            src_ref=own_table,
            dst_ref=tables.at[landing],
            send_sem=table_send.at[0],
            recv_sem=table_recv.at[landing],
            device_id=(ahead, mem),
            device_id_type=MESH,
        )

    def forward_stream(c):
        return pltpu.make_async_remote_copy(
            src_ref=block_buf.at[0, span(c)],
            dst_ref=block_buf.at[2, span(c)],
            send_sem=stream_send.at[1, c],
            recv_sem=stream_recv.at[2, c],
            device_id=(ahead, mem),
            device_id_type=MESH,
        )

    def forward_table():
        return pltpu.make_async_remote_copy(
            src_ref=tables.at[0],
            dst_ref=tables.at[2],
            send_sem=table_send.at[1],
            recv_sem=table_recv.at[2],
            device_id=(ahead, mem),
            device_id_type=MESH,
        )

    def stream_arrival(block, c):
        return pltpu.make_async_remote_copy(
            src_ref=owned_ref.at[span(c)],
            dst_ref=block_buf.at[block - 1, span(c)],
            send_sem=stream_send.at[0, c],
            recv_sem=stream_recv.at[block - 1, c],
            device_id=(ahead, mem),
            device_id_type=MESH,
        )

    def table_arrival(block):
        return pltpu.make_async_remote_copy(
            src_ref=own_table,
            dst_ref=tables.at[block - 1],
            send_sem=table_send.at[0],
            recv_sem=table_recv.at[block - 1],
            device_id=(ahead, mem),
            device_id_type=MESH,
        )

    def member_copy(k):
        peer = lax.rem(mem + k, nm)
        return pltpu.make_async_remote_copy(
            src_ref=anom_ref,
            dst_ref=pieces.at[mem],
            send_sem=m_send.at[k],
            recv_sem=m_recv.at[k],
            device_id=(tile, peer),
            device_id_type=MESH,
        )

    def parcel(block, combo, base, t, rows_of):
        return pltpu.make_async_remote_copy(
            src_ref=send_buf.at[combo, t, rows_of],
            dst_ref=recv_ref.at[source[block], rows_of],
            send_sem=p_send.at[combo, t],
            recv_sem=a_recv.at[source[block]],
            device_id=(base + t, mem),
            device_id_type=MESH,
        )

    def pack(block, combo, c):
        block_ref = owned_ref if block == OWN else block_buf.at[block - 1]
        wide = jnp.concatenate(
            [
                block_ref[pl.ds(pl.multiple_of(c * chunk + g * part, part), part), :]
                for g in range(groups)
            ],
            axis=1,
        )

        def pair(h, carry):
            out = jnp.dot(wide, picks[combo, h], preferred_element_type=jnp.float32)
            out = out.astype(jnp.bfloat16)
            send_buf[combo, 2 * h, narrow(c)] = out[:, :LANES]
            send_buf[combo, 2 * h + 1, narrow(c)] = out[:, LANES:]
            return carry

        lax.fori_loop(0, pairs, pair, 0, unroll=pairs <= 2)

    def send(block, combo, base, c):
        def one(t, carry):
            @pl.when(base + t != tile)
            def _():
                parcel(block, combo, base, t, narrow(c)).start()

            return carry

        lax.fori_loop(0, zone_tiles, one, 0)

    def pack_near(block, c):
        pack(block, NEAR_ZONE[block], c)

    def send_near(block, c):
        send(block, NEAR_ZONE[block], zone_base, c)

    def pack_away(block, c):
        pack(block, AWAY[block], c)

    def send_away(block, c):
        send(block, AWAY[block], away_base, c)

    def keep(block):
        return pltpu.make_async_copy(
            send_buf.at[NEAR_ZONE[block], place], recv_ref.at[source[block]], local_sem.at[4 + block]
        )

    own_table_copy().start()

    def start_own(c, carry):
        own_stream(c).start()
        return carry

    lax.fori_loop(0, chunks, start_own, 0)

    @pl.when(inner)
    def _():
        def own_step(c, carry):
            pack_away(OWN, c)
            pack_near(OWN, c)
            send_away(OWN, c)

            @pl.when(c > 0)
            def _():
                send_near(OWN, c - 1)

            return carry

        lax.fori_loop(0, chunks, own_step, 0)

    @pl.when(outer)
    def _():
        def own_step(c, carry):
            pack_near(OWN, c)

            @pl.when(c > 0)
            def _():
                send_near(OWN, c - 1)

            return carry

        lax.fori_loop(0, chunks, own_step, 0)

    for k in range(1, nm):
        member_copy(k).start()

    @pl.when(inner)
    def _():
        table_arrival(OUTER).wait_recv()
        forward_table().start()
        build(tables.at[OUTER - 1], zone_base, NEAR_ZONE[OUTER])
        table_arrival(PARTNER).wait_recv()
        build(tables.at[PARTNER - 1], away_base, AWAY[PARTNER])
        build(tables.at[PARTNER - 1], zone_base, NEAR_ZONE[PARTNER])

    send_near(OWN, chunks - 1)
    keep(OWN).start()

    @pl.when(inner)
    def _():
        def mid_step(c, carry):
            stream_arrival(OUTER, c).wait_recv()
            forward_stream(c).start()
            stream_arrival(PARTNER, c).wait_recv()
            pack_away(PARTNER, c)
            pack_near(PARTNER, c)
            send_away(PARTNER, c)
            pack_near(OUTER, c)
            send_near(PARTNER, c)

            @pl.when(c > 0)
            def _():
                send_near(OUTER, c - 1)

            return carry

        lax.fori_loop(0, chunks, mid_step, 0)
        table_arrival(FAR).wait_recv()
        build(tables.at[FAR - 1], away_base, AWAY[FAR])
        build(tables.at[FAR - 1], zone_base, NEAR_ZONE[FAR])
        send_near(OUTER, chunks - 1)
        keep(OUTER).start()
        keep(PARTNER).start()

        def far_step(c, carry):
            stream_arrival(FAR, c).wait_recv()
            pack_away(FAR, c)
            pack_near(FAR, c)
            send_away(FAR, c)

            @pl.when(c > 0)
            def _():
                send_near(FAR, c - 1)

            return carry

        lax.fori_loop(0, chunks, far_step, 0)

    fweight = fweight_ref[...].astype(jnp.float32)

    def spread_rows(s, carry):
        ids = lax.broadcasted_iota(jnp.int32, (slots, obs), 0) + s * slots
        total = jnp.zeros((slots, obs), jnp.float32)
        for j in range(foot_ref.shape[0]):
            total = total + jnp.where(
                ids == foot_ref[j : j + 1, :], fweight[j : j + 1, :], 0.0
            )
        spread[pl.ds(pl.multiple_of(s * slots, slots), slots), :] = total.astype(jnp.bfloat16)
        return carry

    lax.fori_loop(0, n, spread_rows, 0)

    @pl.when(inner)
    def _():
        send_near(FAR, chunks - 1)
        keep(FAR).start()

    spread_out = pltpu.make_async_copy(spread, spread_ref, local_sem.at[2])
    spread_out.start()
    own_piece.wait()
    for k in range(1, nm):
        member_copy(k).wait()

    mean_wide[...] = mean_ref[...].astype(jnp.float32)
    weight_wide[...] = jnp.transpose(weight_ref[...].astype(jnp.float32))
    mine = weight_wide[pl.ds(mem * mem_dev, mem_dev), :].astype(jnp.bfloat16)
    shares = [mine[:, p * mem_dev : (p + 1) * mem_dev] for p in range(nm)]

    def mix(l, carry):
        total = jnp.broadcast_to(mean_wide[pl.ds(l, 1), :], (mem_dev, cols))
        mixture = jnp.zeros_like(total)
        for p in range(nm):
            mixture = mixture + jnp.dot(
                shares[p], pieces[p, l], preferred_element_type=jnp.float32
            )
        mixed[l] = (total + mixture).astype(jnp.bfloat16)
        return carry

    lax.fori_loop(0, levels, mix, 0)

    analysis_out = pltpu.make_async_copy(mixed, analysis_ref, local_sem.at[3])
    analysis_out.start()

    whole = pl.ds(0, rows // groups)

    def sent(block, combo, base):
        def one(t, carry):
            @pl.when(base + t != tile)
            def _():
                parcel(block, combo, base, t, whole).wait_send()

            return carry

        lax.fori_loop(0, zone_tiles, one, 0)

    def own_sent(c, carry):
        own_stream(c).wait_send()
        return carry

    lax.fori_loop(0, chunks, own_sent, 0)
    own_table_copy().wait_send()
    sent(OWN, NEAR_ZONE[OWN], zone_base)

    @pl.when(inner)
    def _():
        def forwarded(c, carry):
            forward_stream(c).wait_send()
            return carry

        lax.fori_loop(0, chunks, forwarded, 0)
        forward_table().wait_send()
        for block in (OUTER, PARTNER, FAR):
            sent(block, NEAR_ZONE[block], zone_base)
            keep(block).wait()
        for block in AWAY:
            sent(block, AWAY[block], away_base)

    def arrived(s, carry):
        here = jnp.logical_or(
            s == tile, jnp.logical_and(inner, lax.rem(s, zone_tiles) == place)
        )

        @pl.when(jnp.logical_not(here))
        def _():
            pltpu.make_async_remote_copy(
                src_ref=send_buf.at[0, 0],
                dst_ref=recv_ref.at[s],
                send_sem=p_send.at[0, 0],
                recv_sem=a_recv.at[s],
                device_id=(ahead, mem),
                device_id_type=MESH,
            ).wait_recv()

        return carry

    lax.fori_loop(0, n, arrived, 0)
    keep(OWN).wait()
    spread_out.wait()
    analysis_out.wait()


def combine_kernel(n, groups, bias_ref, recv_ref, spread_ref, out_ref):
    step = pl.program_id(0)
    slots = spread_ref.shape[0] // n
    channels, members = out_ref.shape[0], out_ref.shape[1]
    stacked = jnp.concatenate(
        [
            jnp.concatenate(
                [recv_ref[s, :, g * slots : (g + 1) * slots] for s in range(n)], axis=1
            )
            for g in range(groups)
        ],
        axis=0,
    )
    prior = jnp.dot(stacked, spread_ref[...], preferred_element_type=jnp.float32)
    for c in range(channels):
        bias = bias_ref[step * channels + c]
        out_ref[c] = prior[c * members : (c + 1) * members, :] + bias


def chunk_count(channels, mem_dev, groups):
    def fits(count):
        part = channels * mem_dev // (count * groups)
        return channels % count == 0 and part * count * groups == channels * mem_dev and part % 16 == 0

    return next(count for count in (6, 4, 3, 2, 1) if count == 1 or fits(count))


def shards(
    n,
    nm,
    anomalies,
    analysis_weights,
    background_mean,
    background,
    jacobian_table,
    channel_list,
    send_slots,
    footprint,
    footprint_weight,
    channel_bias,
):
    mem_dev, levels, cols = anomalies.shape
    channels = channel_list.shape[0]
    slots = send_slots.shape[2]
    obs, foot = footprint.shape
    groups = LANES // slots
    rows = channels * mem_dev
    members = analysis_weights.shape[1]
    chunks = chunk_count(channels, mem_dev, groups)
    zone_tiles = n // ZONES
    combos = len(NEAR_ZONE) + len(AWAY)

    chosen = (
        jnp.arange(jacobian_table.shape[0], dtype=jnp.int32)[:, None] == channel_list[None, :]
    ).astype(jnp.bfloat16)
    selected = jnp.einsum(
        "sl,sc->cl", jacobian_table, chosen, preferred_element_type=jnp.float32
    ).astype(jnp.bfloat16)
    owned = jnp.einsum(
        "cl,klx->ckx", selected, background, preferred_element_type=jnp.float32
    ).astype(jnp.bfloat16)
    vmem = pl.BlockSpec(memory_space=pltpu.VMEM)
    hbm = pl.BlockSpec(memory_space=pl.ANY)
    dma = pltpu.SemaphoreType.DMA
    received, analysis, spread = pl.pallas_call(
        functools.partial(exchange_kernel, n, nm, chunks),
        out_shape=(
            jax.ShapeDtypeStruct((n, rows // groups, LANES), jnp.bfloat16),
            jax.ShapeDtypeStruct((levels, mem_dev, cols), jnp.bfloat16),
            jax.ShapeDtypeStruct((n * slots, obs), jnp.bfloat16),
        ),
        in_specs=[vmem, vmem, hbm, vmem, vmem, vmem, vmem],
        out_specs=(hbm, hbm, hbm),
        scratch_shapes=[
            pltpu.VMEM((combos, zone_tiles, rows // groups, LANES), jnp.bfloat16),
            pltpu.VMEM((3, rows, cols), jnp.bfloat16),
            pltpu.VMEM((n, LANES), jnp.int32),
            pltpu.VMEM((3, n, LANES), jnp.int32),
            pltpu.VMEM((combos, zone_tiles // 2, groups * cols, 2 * LANES), jnp.bfloat16),
            pltpu.VMEM((nm, levels, mem_dev, cols), jnp.bfloat16),
            pltpu.VMEM((levels, mem_dev, cols), jnp.bfloat16),
            pltpu.VMEM((n * slots, obs), jnp.bfloat16),
            pltpu.VMEM((levels, cols), jnp.float32),
            pltpu.VMEM((members, members), jnp.float32),
            dma((2, chunks)),
            dma((3, chunks)),
            dma((2,)),
            dma((3,)),
            dma((nm,)),
            dma((nm,)),
            dma((combos, zone_tiles)),
            dma((n,)),
            dma((8,)),
        ],
        compiler_params=pltpu.CompilerParams(
            collective_id=0, has_side_effects=True, vmem_limit_bytes=40 * 1024 * 1024
        ),
        name="exchange",
    )(
        owned.reshape(rows, cols),
        send_slots[0],
        jnp.transpose(anomalies, (1, 0, 2)),
        analysis_weights[0],
        background_mean,
        jnp.transpose(footprint),
        jnp.transpose(footprint_weight),
    )
    analysis_members = jnp.transpose(analysis, (1, 0, 2))

    part = rows // (groups * chunks)
    prior = pl.pallas_call(
        functools.partial(combine_kernel, n, groups),
        out_shape=jax.ShapeDtypeStruct((channels, mem_dev, obs), jnp.float32),
        grid=(chunks,),
        in_specs=[
            pl.BlockSpec(memory_space=pltpu.SMEM),
            pl.BlockSpec((n, part, LANES), lambda i: (0, i, 0)),
            pl.BlockSpec((n * slots, obs), lambda i: (0, 0)),
        ],
        out_specs=pl.BlockSpec((channels // chunks, mem_dev, obs), lambda i: (i, 0, 0)),
        compiler_params=pltpu.CompilerParams(vmem_limit_bytes=24 * 1024 * 1024),
        name="combine",
    )(channel_bias, received, spread)
    return analysis_members, prior


def solution(mesh):
    placed = (
        P("mem", None, "tile"),
        P("tile", None, None),
        P(None, "tile"),
        P("mem", None, "tile"),
        P(),
        P(),
        P("tile", None, None),
        P("tile", None),
        P("tile", None),
        P(),
    )
    return jax.shard_map(
        functools.partial(shards, mesh.shape["tile"], mesh.shape["mem"]),
        mesh=mesh,
        in_specs=placed,
        out_specs=(P("mem", None, "tile"), P(None, "mem", "tile")),
        check_vma=False,
    )
```

```python
import functools

import jax
import jax.numpy as jnp
from jax import lax
from jax.experimental import pallas as pl
from jax.experimental.pallas import tpu as pltpu
from jax.sharding import PartitionSpec as P

LANES = 128
MESH = pl.DeviceIdType.MESH
ZONES = 4
MIX_LEVELS = 8

OWN, OUTER, PARTNER, FAR = range(4)
NEAR_ZONE = (0, 1, 2, 3)
AWAY = {OWN: 4, PARTNER: 5, FAR: 6}


def exchange_kernel(
    n,
    nm,
    chunks,
    owned_ref,
    slots_ref,
    anom_ref,
    weight_ref,
    mean_ref,
    foot_ref,
    fweight_ref,
    recv_ref,
    analysis_ref,
    spread_ref,
    send_buf,
    block_buf,
    own_table,
    tables,
    picks,
    pieces,
    mixed,
    spread,
    mean_wide,
    weight_wide,
    stream_send,
    stream_recv,
    table_send,
    table_recv,
    m_send,
    m_recv,
    p_send,
    a_recv,
    local_sem,
):
    tile = lax.axis_index("tile")
    mem = lax.axis_index("mem")
    rows, cols = owned_ref.shape
    slots = slots_ref.shape[1]
    groups = LANES // slots
    obs = foot_ref.shape[1]
    levels, mem_dev = anom_ref.shape[0], anom_ref.shape[1]
    zone_tiles = n // ZONES
    pairs = zone_tiles // 2
    chunk = rows // chunks
    part = chunk // groups

    zone = tile // zone_tiles
    place = lax.rem(tile, zone_tiles)
    sign = 1 - 2 * (zone // 2)
    inner = jnp.logical_or(zone == 1, zone == 2)
    outer = jnp.logical_not(inner)
    stride = sign * zone_tiles
    ahead = lax.rem(tile + stride + n, n)
    source = (
        tile,
        lax.rem(tile - stride + n, n),
        ahead,
        lax.rem(tile + 2 * stride + n, n),
    )
    zone_base = zone * zone_tiles
    away_base = lax.rem(zone_base - stride + n, n)

    barrier = pltpu.get_barrier_semaphore()

    def greet(k, carry):
        pl.semaphore_signal(
            barrier, inc=1, device_id=(lax.rem(tile + k, n), mem), device_id_type=MESH
        )
        return carry

    lax.fori_loop(1, n, greet, 0)
    for k in range(1, nm):
        pl.semaphore_signal(
            barrier, inc=1, device_id=(tile, lax.rem(mem + k, nm)), device_id_type=MESH
        )
    own_piece = pltpu.make_async_copy(anom_ref, pieces.at[mem], local_sem.at[0])
    own_piece.start()

    columns = jnp.maximum(slots_ref[...], 0)
    own_table[...] = jnp.concatenate([columns + g * cols for g in range(groups)], axis=1)

    def build(table_ref, base, combo):
        row_id = lax.broadcasted_iota(jnp.int32, (groups * cols, 2 * LANES), 0)

        def pair(h, carry):
            first = base + 2 * h
            want = jnp.concatenate(
                [table_ref[pl.ds(first, 1), :], table_ref[pl.ds(first + 1, 1), :]], axis=1
            )
            picks[combo, h] = jnp.where(row_id == want, 1.0, 0.0).astype(jnp.bfloat16)
            return carry

        lax.fori_loop(0, pairs, pair, 0)

    build(own_table, zone_base, NEAR_ZONE[OWN])

    @pl.when(inner)
    def _():
        build(own_table, away_base, AWAY[OWN])

    pl.semaphore_wait(barrier, n - 1 + nm - 1)

    def span(c):
        return pl.ds(pl.multiple_of(c * chunk, chunk), chunk)

    def narrow(c):
        return pl.ds(pl.multiple_of(c * part, part), part)

    landing = jnp.where(inner, 1, 0)

    def own_stream(c):
        return pltpu.make_async_remote_copy(
            src_ref=owned_ref.at[span(c)],
            dst_ref=block_buf.at[landing, span(c)],
            send_sem=stream_send.at[0, c],
            recv_sem=stream_recv.at[landing, c],
            device_id=(ahead, mem),
            device_id_type=MESH,
        )

    def own_table_copy():
        return pltpu.make_async_remote_copy(
            src_ref=own_table,
            dst_ref=tables.at[landing],
            send_sem=table_send.at[0],
            recv_sem=table_recv.at[landing],
            device_id=(ahead, mem),
            device_id_type=MESH,
        )

    def forward_stream(c):
        return pltpu.make_async_remote_copy(
            src_ref=block_buf.at[0, span(c)],
            dst_ref=block_buf.at[2, span(c)],
            send_sem=stream_send.at[1, c],
            recv_sem=stream_recv.at[2, c],
            device_id=(ahead, mem),
            device_id_type=MESH,
        )

    def forward_table():
        return pltpu.make_async_remote_copy(
            src_ref=tables.at[0],
            dst_ref=tables.at[2],
            send_sem=table_send.at[1],
            recv_sem=table_recv.at[2],
            device_id=(ahead, mem),
            device_id_type=MESH,
        )

    def stream_arrival(block, c):
        return pltpu.make_async_remote_copy(
            src_ref=owned_ref.at[span(c)],
            dst_ref=block_buf.at[block - 1, span(c)],
            send_sem=stream_send.at[0, c],
            recv_sem=stream_recv.at[block - 1, c],
            device_id=(ahead, mem),
            device_id_type=MESH,
        )

    def table_arrival(block):
        return pltpu.make_async_remote_copy(
            src_ref=own_table,
            dst_ref=tables.at[block - 1],
            send_sem=table_send.at[0],
            recv_sem=table_recv.at[block - 1],
            device_id=(ahead, mem),
            device_id_type=MESH,
        )

    def member_copy(k):
        peer = lax.rem(mem + k, nm)
        return pltpu.make_async_remote_copy(
            src_ref=anom_ref,
            dst_ref=pieces.at[mem],
            send_sem=m_send.at[k],
            recv_sem=m_recv.at[k],
            device_id=(tile, peer),
            device_id_type=MESH,
        )

    def parcel(block, combo, base, t, rows_of):
        return pltpu.make_async_remote_copy(
            src_ref=send_buf.at[combo, t, rows_of],
            dst_ref=recv_ref.at[source[block], rows_of],
            send_sem=p_send.at[combo, t],
            recv_sem=a_recv.at[source[block]],
            device_id=(base + t, mem),
            device_id_type=MESH,
        )

    def pack(block, combo, c):
        block_ref = owned_ref if block == OWN else block_buf.at[block - 1]
        wide = jnp.concatenate(
            [
                block_ref[pl.ds(pl.multiple_of(c * chunk + g * part, part), part), :]
                for g in range(groups)
            ],
            axis=1,
        )

        def pair(h, carry):
            out = jnp.dot(wide, picks[combo, h], preferred_element_type=jnp.float32)
            out = out.astype(jnp.bfloat16)
            send_buf[combo, 2 * h, narrow(c)] = out[:, :LANES]
            send_buf[combo, 2 * h + 1, narrow(c)] = out[:, LANES:]
            return carry

        lax.fori_loop(0, pairs, pair, 0, unroll=pairs <= 2)

    def send(block, combo, base, c):
        def one(t, carry):
            @pl.when(base + t != tile)
            def _():
                parcel(block, combo, base, t, narrow(c)).start()

            return carry

        lax.fori_loop(0, zone_tiles, one, 0)

    def pack_near(block, c):
        pack(block, NEAR_ZONE[block], c)

    def send_near(block, c):
        send(block, NEAR_ZONE[block], zone_base, c)

    def pack_away(block, c):
        pack(block, AWAY[block], c)

    def send_away(block, c):
        send(block, AWAY[block], away_base, c)

    def keep(block):
        return pltpu.make_async_copy(
            send_buf.at[NEAR_ZONE[block], place], recv_ref.at[source[block]], local_sem.at[4 + block]
        )

    own_table_copy().start()

    def start_own(c, carry):
        own_stream(c).start()
        return carry

    lax.fori_loop(0, chunks, start_own, 0)

    @pl.when(inner)
    def _():
        def own_step(c, carry):
            pack_away(OWN, c)
            pack_near(OWN, c)
            send_away(OWN, c)

            @pl.when(c > 0)
            def _():
                send_near(OWN, c - 1)

            return carry

        lax.fori_loop(0, chunks, own_step, 0)

    @pl.when(outer)
    def _():
        def own_step(c, carry):
            pack_near(OWN, c)

            @pl.when(c > 0)
            def _():
                send_near(OWN, c - 1)

            return carry

        lax.fori_loop(0, chunks, own_step, 0)

    for k in range(1, nm):
        member_copy(k).start()

    @pl.when(inner)
    def _():
        table_arrival(OUTER).wait_recv()
        forward_table().start()
        build(tables.at[OUTER - 1], zone_base, NEAR_ZONE[OUTER])
        table_arrival(PARTNER).wait_recv()
        build(tables.at[PARTNER - 1], away_base, AWAY[PARTNER])
        build(tables.at[PARTNER - 1], zone_base, NEAR_ZONE[PARTNER])

    send_near(OWN, chunks - 1)
    keep(OWN).start()

    @pl.when(inner)
    def _():
        def mid_step(c, carry):
            stream_arrival(OUTER, c).wait_recv()
            forward_stream(c).start()
            stream_arrival(PARTNER, c).wait_recv()
            pack_away(PARTNER, c)
            pack_near(PARTNER, c)
            send_away(PARTNER, c)
            pack_near(OUTER, c)
            send_near(PARTNER, c)

            @pl.when(c > 0)
            def _():
                send_near(OUTER, c - 1)

            return carry

        lax.fori_loop(0, chunks, mid_step, 0)
        table_arrival(FAR).wait_recv()
        build(tables.at[FAR - 1], away_base, AWAY[FAR])
        build(tables.at[FAR - 1], zone_base, NEAR_ZONE[FAR])
        send_near(OUTER, chunks - 1)
        keep(OUTER).start()
        keep(PARTNER).start()

        def far_step(c, carry):
            stream_arrival(FAR, c).wait_recv()
            pack_away(FAR, c)
            pack_near(FAR, c)
            send_away(FAR, c)

            @pl.when(c > 0)
            def _():
                send_near(FAR, c - 1)

            return carry

        lax.fori_loop(0, chunks, far_step, 0)

    fweight = fweight_ref[...].astype(jnp.float32)

    def spread_rows(s, carry):
        ids = lax.broadcasted_iota(jnp.int32, (slots, obs), 0) + s * slots
        total = jnp.zeros((slots, obs), jnp.float32)
        for j in range(foot_ref.shape[0]):
            total = total + jnp.where(
                ids == foot_ref[j : j + 1, :], fweight[j : j + 1, :], 0.0
            )
        spread[pl.ds(pl.multiple_of(s * slots, slots), slots), :] = total.astype(jnp.bfloat16)
        return carry

    lax.fori_loop(0, n, spread_rows, 0)

    @pl.when(inner)
    def _():
        send_near(FAR, chunks - 1)
        keep(FAR).start()

    spread_out = pltpu.make_async_copy(spread, spread_ref, local_sem.at[2])
    spread_out.start()
    own_piece.wait()
    for k in range(1, nm):
        member_copy(k).wait()

    mean_wide[...] = mean_ref[...].astype(jnp.float32)
    weight_wide[...] = jnp.transpose(weight_ref[...].astype(jnp.float32))
    mine = weight_wide[pl.ds(mem * mem_dev, mem_dev), :].astype(jnp.bfloat16)
    shares = [mine[:, p * mem_dev : (p + 1) * mem_dev] for p in range(nm)]

    def mix(first, count):
        mixture = jnp.zeros((mem_dev, count * cols), jnp.float32)
        for p in range(nm):
            side = jnp.concatenate([pieces[p, first + i] for i in range(count)], axis=1)
            mixture = mixture + jnp.dot(shares[p], side, preferred_element_type=jnp.float32)
        for i in range(count):
            total = mean_wide[pl.ds(first + i, 1), :] + mixture[:, i * cols : (i + 1) * cols]
            mixed[first + i] = total.astype(jnp.bfloat16)

    def mix_block(b, carry):
        mix(b * MIX_LEVELS, MIX_LEVELS)
        return carry

    full = levels // MIX_LEVELS
    lax.fori_loop(0, full, mix_block, 0)
    if levels % MIX_LEVELS:
        mix(full * MIX_LEVELS, levels % MIX_LEVELS)

    analysis_out = pltpu.make_async_copy(mixed, analysis_ref, local_sem.at[3])
    analysis_out.start()

    whole = pl.ds(0, rows // groups)

    def sent(block, combo, base):
        def one(t, carry):
            @pl.when(base + t != tile)
            def _():
                parcel(block, combo, base, t, whole).wait_send()

            return carry

        lax.fori_loop(0, zone_tiles, one, 0)

    def own_sent(c, carry):
        own_stream(c).wait_send()
        return carry

    lax.fori_loop(0, chunks, own_sent, 0)
    own_table_copy().wait_send()
    sent(OWN, NEAR_ZONE[OWN], zone_base)

    @pl.when(inner)
    def _():
        def forwarded(c, carry):
            forward_stream(c).wait_send()
            return carry

        lax.fori_loop(0, chunks, forwarded, 0)
        forward_table().wait_send()
        for block in (OUTER, PARTNER, FAR):
            sent(block, NEAR_ZONE[block], zone_base)
            keep(block).wait()
        for block in AWAY:
            sent(block, AWAY[block], away_base)

    def arrived(s, carry):
        here = jnp.logical_or(
            s == tile, jnp.logical_and(inner, lax.rem(s, zone_tiles) == place)
        )

        @pl.when(jnp.logical_not(here))
        def _():
            pltpu.make_async_remote_copy(
                src_ref=send_buf.at[0, 0],
                dst_ref=recv_ref.at[s],
                send_sem=p_send.at[0, 0],
                recv_sem=a_recv.at[s],
                device_id=(ahead, mem),
                device_id_type=MESH,
            ).wait_recv()

        return carry

    lax.fori_loop(0, n, arrived, 0)
    keep(OWN).wait()
    spread_out.wait()
    analysis_out.wait()


def combine_kernel(
    n, groups, bias_ref, recv_ref, spread_ref, mixed_ref, out_ref, analysis_ref, sem
):
    step = pl.program_id(0)
    carry_out = pltpu.make_async_copy(mixed_ref, analysis_ref, sem)

    @pl.when(step == 0)
    def _():
        carry_out.start()

    slots = spread_ref.shape[0] // n
    channels, members = out_ref.shape[0], out_ref.shape[1]
    stacked = jnp.concatenate(
        [
            jnp.concatenate(
                [recv_ref[s, :, g * slots : (g + 1) * slots] for s in range(n)], axis=1
            )
            for g in range(groups)
        ],
        axis=0,
    )
    prior = jnp.dot(stacked, spread_ref[...], preferred_element_type=jnp.float32)
    for c in range(channels):
        bias = bias_ref[step * channels + c]
        out_ref[c] = prior[c * members : (c + 1) * members, :] + bias

    @pl.when(step == pl.num_programs(0) - 1)
    def _():
        carry_out.wait()


def chunk_count(channels, mem_dev, groups):
    def fits(count):
        part = channels * mem_dev // (count * groups)
        return channels % count == 0 and part * count * groups == channels * mem_dev and part % 16 == 0

    return next(count for count in (6, 4, 3, 2, 1) if count == 1 or fits(count))


def shards(
    n,
    nm,
    anomalies,
    analysis_weights,
    background_mean,
    background,
    jacobian_table,
    channel_list,
    send_slots,
    footprint,
    footprint_weight,
    channel_bias,
):
    mem_dev, levels, cols = anomalies.shape
    channels = channel_list.shape[0]
    slots = send_slots.shape[2]
    obs, foot = footprint.shape
    groups = LANES // slots
    rows = channels * mem_dev
    members = analysis_weights.shape[1]
    chunks = chunk_count(channels, mem_dev, groups)
    zone_tiles = n // ZONES
    combos = len(NEAR_ZONE) + len(AWAY)

    chosen = (
        jnp.arange(jacobian_table.shape[0], dtype=jnp.int32)[:, None] == channel_list[None, :]
    ).astype(jnp.bfloat16)
    selected = jnp.einsum(
        "sl,sc->cl", jacobian_table, chosen, preferred_element_type=jnp.float32
    ).astype(jnp.bfloat16)
    owned = jnp.einsum(
        "cl,klx->ckx", selected, background, preferred_element_type=jnp.float32
    ).astype(jnp.bfloat16)
    vmem = pl.BlockSpec(memory_space=pltpu.VMEM)
    hbm = pl.BlockSpec(memory_space=pl.ANY)
    dma = pltpu.SemaphoreType.DMA
    received, mixed, spread = pl.pallas_call(
        functools.partial(exchange_kernel, n, nm, chunks),
        out_shape=(
            jax.ShapeDtypeStruct((n, rows // groups, LANES), jnp.bfloat16),
            jax.ShapeDtypeStruct((levels, mem_dev, cols), jnp.bfloat16),
            jax.ShapeDtypeStruct((n * slots, obs), jnp.bfloat16),
        ),
        in_specs=[vmem, vmem, hbm, vmem, vmem, vmem, vmem],
        out_specs=(hbm, hbm, hbm),
        scratch_shapes=[
            pltpu.VMEM((combos, zone_tiles, rows // groups, LANES), jnp.bfloat16),
            pltpu.VMEM((3, rows, cols), jnp.bfloat16),
            pltpu.VMEM((n, LANES), jnp.int32),
            pltpu.VMEM((3, n, LANES), jnp.int32),
            pltpu.VMEM((combos, zone_tiles // 2, groups * cols, 2 * LANES), jnp.bfloat16),
            pltpu.VMEM((nm, levels, mem_dev, cols), jnp.bfloat16),
            pltpu.VMEM((levels, mem_dev, cols), jnp.bfloat16),
            pltpu.VMEM((n * slots, obs), jnp.bfloat16),
            pltpu.VMEM((levels, cols), jnp.float32),
            pltpu.VMEM((members, members), jnp.float32),
            dma((2, chunks)),
            dma((3, chunks)),
            dma((2,)),
            dma((3,)),
            dma((nm,)),
            dma((nm,)),
            dma((combos, zone_tiles)),
            dma((n,)),
            dma((8,)),
        ],
        compiler_params=pltpu.CompilerParams(
            collective_id=0, has_side_effects=True, vmem_limit_bytes=40 * 1024 * 1024
        ),
        name="exchange",
    )(
        owned.reshape(rows, cols),
        send_slots[0],
        jnp.transpose(anomalies, (1, 0, 2)),
        analysis_weights[0],
        background_mean,
        jnp.transpose(footprint),
        jnp.transpose(footprint_weight),
    )
    part = rows // (groups * chunks)
    prior, analysis = pl.pallas_call(
        functools.partial(combine_kernel, n, groups),
        out_shape=(
            jax.ShapeDtypeStruct((channels, mem_dev, obs), jnp.float32),
            jax.ShapeDtypeStruct(mixed.shape, mixed.dtype),
        ),
        grid=(chunks,),
        in_specs=[
            pl.BlockSpec(memory_space=pltpu.SMEM),
            pl.BlockSpec((n, part, LANES), lambda i: (0, i, 0)),
            pl.BlockSpec((n * slots, obs), lambda i: (0, 0)),
            vmem,
        ],
        out_specs=(
            pl.BlockSpec((channels // chunks, mem_dev, obs), lambda i: (i, 0, 0)),
            hbm,
        ),
        scratch_shapes=[dma],
        compiler_params=pltpu.CompilerParams(vmem_limit_bytes=24 * 1024 * 1024),
        name="combine",
    )(channel_bias, received, spread, mixed)
    return jnp.transpose(analysis, (1, 0, 2)), prior


def solution(mesh):
    placed = (
        P("mem", None, "tile"),
        P("tile", None, None),
        P(None, "tile"),
        P("mem", None, "tile"),
        P(),
        P(),
        P("tile", None, None),
        P("tile", None),
        P("tile", None),
        P(),
    )
    return jax.shard_map(
        functools.partial(shards, mesh.shape["tile"], mesh.shape["mem"]),
        mesh=mesh,
        in_specs=placed,
        out_specs=(P("mem", None, "tile"), P(None, "mem", "tile")),
        check_vma=False,
    )
```

```python
import functools

import jax
import jax.numpy as jnp
from jax import lax
from jax.experimental import pallas as pl
from jax.experimental.pallas import tpu as pltpu
from jax.sharding import PartitionSpec as P

LANES = 128
MESH = pl.DeviceIdType.MESH
ZONES = 4
MIX_LEVELS = 8

OWN, OUTER, PARTNER, FAR = range(4)
AWAY = {OWN: 0, PARTNER: 1, FAR: 2}
CAP = 80
FOLD = 8


def needed(table_ref, source, base, count, cols):
    column = lax.broadcasted_iota(jnp.int32, (cols, LANES), 0)

    def one(t, hit):
        row = table_ref[source, pl.ds(base + t, 1), :]
        return jnp.where(column == row, 1.0, hit)

    hit = lax.fori_loop(0, count, one, jnp.zeros((cols, LANES), jnp.float32))
    return jnp.max(hit, axis=1, keepdims=True)


def positions(mask, cols):
    before = lax.broadcasted_iota(jnp.int32, (cols, cols), 1) < lax.broadcasted_iota(
        jnp.int32, (cols, cols), 0
    )
    full = jnp.broadcast_to(mask, (cols, LANES)).astype(jnp.bfloat16)
    return jnp.dot(
        jnp.where(before, 1.0, 0.0).astype(jnp.bfloat16), full, preferred_element_type=jnp.float32
    )


def front_kernel(
    n,
    select,
    *refs,
):
    if select:
        (table_ref, list_ref, field_ref, slots_ref, owned_ref, tables_ref, count_ref,
         message, gathered, counted, counts, table, field, wide, chosen, radiance,
         sends, arrives, local_sem) = refs
    else:
        (slots_ref, tables_ref, count_ref, message, gathered, counted, counts,
         sends, arrives, local_sem) = refs
    tile = lax.axis_index("tile")
    mem = lax.axis_index("mem")
    slots = slots_ref.shape[1]
    groups = LANES // slots
    cols = LANES
    zone_tiles = n // ZONES
    zone = tile // zone_tiles
    barrier = pltpu.get_barrier_semaphore()

    def greet(k, carry):
        pl.semaphore_signal(
            barrier, inc=1, device_id=(lax.rem(tile + k, n), mem), device_id_type=MESH
        )
        return carry

    lax.fori_loop(1, n, greet, 0)
    if select:
        load_table = pltpu.make_async_copy(table_ref, table, local_sem.at[0])
        load_table.start()
        load_field = pltpu.make_async_copy(field_ref, field, local_sem.at[1])
        load_field.start()

    message[0] = jnp.concatenate([slots_ref[...]] * groups, axis=1)
    most = jnp.zeros((1, 1), jnp.float32)
    for far in (0, ZONES - 1):
        mask = needed(message, 0, far * zone_tiles, zone_tiles, cols)
        total = jnp.sum(mask, axis=0, keepdims=True)
        most = jnp.maximum(most, jnp.where(zone == far, 0.0, total))
    counted[0] = jnp.broadcast_to(most, (1, LANES)).astype(jnp.int32)
    pl.semaphore_wait(barrier, n - 1)

    def tell(k, carry):
        pltpu.make_async_remote_copy(
            src_ref=counted.at[0],
            dst_ref=counts.at[tile],
            send_sem=sends.at[0],
            recv_sem=arrives.at[0],
            device_id=(lax.rem(tile + k, n), mem),
            device_id_type=MESH,
        ).start()
        return carry

    lax.fori_loop(1, n, tell, 0)
    for k in range(1, ZONES):
        pltpu.make_async_remote_copy(
            src_ref=message.at[0],
            dst_ref=gathered.at[zone],
            send_sem=sends.at[1],
            recv_sem=arrives.at[1],
            device_id=(lax.rem(tile + k * zone_tiles, n), mem),
            device_id_type=MESH,
        ).start()

    if select:
        spectrum = table_ref.shape[1]
        levels, mem_dev = field_ref.shape[0], field_ref.shape[1]
        channels = list_ref.shape[1]
        load_field.wait()
        wide[...] = field[...].astype(jnp.float32)
        load_table.wait()
        block = 11 * LANES
        total = jnp.zeros((levels, channels), jnp.float32)
        for first in range(0, spectrum, block):
            size = min(block, spectrum - first)
            entry = lax.broadcasted_iota(jnp.int32, (size, channels), 0) + first
            pick = jnp.where(entry == list_ref[...], 1.0, 0.0).astype(jnp.bfloat16)
            total = total + jnp.dot(
                table[:, first : first + size], pick, preferred_element_type=jnp.float32
            )
        chosen[...] = jnp.zeros_like(chosen)
        chosen[0:levels, 0:channels] = total
        picked = jnp.transpose(chosen[...])[:channels, :levels].astype(jnp.bfloat16)
        flat = wide.reshape(levels * mem_dev, cols)

        def member(k, carry):
            profile = flat[pl.ds(k, levels, stride=mem_dev), :].astype(jnp.bfloat16)
            radiance[pl.ds(k, channels, stride=mem_dev), :] = jnp.dot(
                picked, profile, preferred_element_type=jnp.float32
            )
            return carry

        lax.fori_loop(0, mem_dev, member, 0, unroll=8)
        owned_ref[...] = radiance[...].astype(jnp.bfloat16)

    counts[tile] = counted[0]
    gathered[zone] = message[0]

    def everyone(ref, count, kind):
        span = ref.at[pl.ds(0, count)]
        return pltpu.make_async_remote_copy(
            src_ref=span,
            dst_ref=span,
            send_sem=sends.at[kind],
            recv_sem=arrives.at[kind],
            device_id=(lax.rem(tile + 1, n), mem),
            device_id_type=MESH,
        )

    everyone(gathered, ZONES - 1, 1).wait_recv()
    tables_ref[...] = gathered[...]
    everyone(counts, n - 1, 0).wait_recv()

    def highest(s, top):
        return jnp.maximum(top, counts[s])

    top = lax.fori_loop(0, n, highest, jnp.zeros((1, LANES), jnp.int32))
    count_ref[0, 0] = jnp.max(top.astype(jnp.float32))
    everyone(counts, n - 1, 0).wait_send()
    everyone(gathered, ZONES - 1, 1).wait_send()


def exchange_kernel(
    n,
    nm,
    chunks,
    tight,
    owned_ref,
    tables_ref,
    anom_ref,
    weight_ref,
    mean_ref,
    foot_ref,
    fweight_ref,
    recv_ref,
    analysis_ref,
    spread_ref,
    send_buf,
    away_buf,
    block_buf,
    compact_buf,
    picks,
    away_picks,
    open_picks,
    pieces,
    mixed,
    spread,
    mean_wide,
    weight_wide,
    shares,
    stream_send,
    stream_recv,
    m_send,
    m_recv,
    p_send,
    away_send,
    away_recv,
    a_recv,
    local_sem,
):
    tile = lax.axis_index("tile")
    mem = lax.axis_index("mem")
    rows, cols = owned_ref.shape
    slots = spread_ref.shape[0] // n
    groups = LANES // slots
    obs = foot_ref.shape[1]
    levels, mem_dev = anom_ref.shape[0], anom_ref.shape[1]
    zone_tiles = n // ZONES
    pairs = zone_tiles // 2
    chunk = rows // chunks
    part = chunk // groups

    zone = tile // zone_tiles
    place = lax.rem(tile, zone_tiles)
    sign = 1 - 2 * (zone // 2)
    inner = jnp.logical_or(zone == 1, zone == 2)
    outer = jnp.logical_not(inner)
    stride = sign * zone_tiles
    ahead = lax.rem(tile + stride + n, n)

    def along(steps):
        return lax.rem(tile + steps * stride + ZONES * n, n)

    if tight:
        source = (tile, along(jnp.where(inner, -1, 1)), along(jnp.where(inner, 1, 2)),
                  along(jnp.where(inner, 2, 3)))
    else:
        source = (tile, along(-1), along(1), along(2))
    zone_base = zone * zone_tiles
    away_base = lax.rem(zone_base - stride + n, n)

    barrier = pltpu.get_barrier_semaphore()

    def greet(k, carry):
        pl.semaphore_signal(
            barrier,
            inc=1,
            device_id=(zone_base + lax.rem(place + k, zone_tiles), mem),
            device_id_type=MESH,
        )
        return carry

    lax.fori_loop(1, zone_tiles, greet, 0)
    for side in (-1, 1):

        @pl.when(jnp.logical_and(zone + side >= 0, zone + side < ZONES))
        def _():
            def greet_side(t, carry):
                pl.semaphore_signal(
                    barrier,
                    inc=1,
                    device_id=(zone_base + side * zone_tiles + t, mem),
                    device_id_type=MESH,
                )
                return carry

            lax.fori_loop(0, zone_tiles, greet_side, 0)

    for k in range(1, nm):
        pl.semaphore_signal(
            barrier, inc=1, device_id=(tile, lax.rem(mem + k, nm)), device_id_type=MESH
        )

    lane_group = lax.broadcasted_iota(jnp.int32, (1, LANES), 1) // slots

    def build(origin, base, into, first_pick):
        row_id = lax.broadcasted_iota(jnp.int32, (groups * cols, 2 * LANES), 0)

        def want(t):
            row = tables_ref[origin // zone_tiles, pl.ds(base + t, 1), :]
            return jnp.maximum(row, 0) + lane_group * cols

        def pair(h, carry):
            wants = jnp.concatenate([want(2 * h), want(2 * h + 1)], axis=1)
            into[first_pick, h] = jnp.where(row_id == wants, 1.0, 0.0).astype(jnp.bfloat16)
            return carry

        lax.fori_loop(0, pairs, pair, 0)

    def build_near(block):
        build(source[block], zone_base, picks, block)

    def build_away(block):
        origin = source[block]
        if not tight:
            build(origin, away_base, away_picks, AWAY[block])
            return
        mask = needed(tables_ref, origin // zone_tiles, away_base, zone_tiles, cols)
        place_of = positions(mask, cols)[:, 0:1].astype(jnp.int32)
        place_of = jnp.where(mask > 0.0, place_of, -FOLD * CAP)
        lane = lax.broadcasted_iota(jnp.int32, (cols, FOLD * CAP), 1)
        for g in range(FOLD):
            away_picks[AWAY[block], g * cols : (g + 1) * cols, :] = jnp.where(
                lane == place_of + g * CAP, 1.0, 0.0
            ).astype(jnp.bfloat16)

    def build_open(i):
        origin = source[1 + i]
        mask = needed(tables_ref, origin // zone_tiles, zone_base, zone_tiles, cols)
        column = lax.broadcasted_iota(jnp.int32, (cols, LANES), 0)
        row_id = lax.broadcasted_iota(jnp.int32, (FOLD * CAP, 2 * LANES), 0)

        def one(t, carry):
            row = tables_ref[origin // zone_tiles, pl.ds(zone_base + t, 1), :]
            ahead_of = jnp.where(column < row, mask, 0.0)
            spot = jnp.sum(ahead_of, axis=0, keepdims=True).astype(jnp.int32)
            wants = jnp.concatenate(
                [spot + (2 * lane_group + v) * CAP for v in range(2)], axis=1
            )
            open_picks[i, t] = jnp.where(row_id == wants, 1.0, 0.0).astype(jnp.bfloat16)
            return carry

        lax.fori_loop(0, zone_tiles, one, 0)

    build_near(OWN)

    @pl.when(inner)
    def _():
        build_away(OWN)

    greeted = zone_tiles - 1 + nm - 1 + jnp.where(inner, 2, 1) * zone_tiles
    pl.semaphore_wait(barrier, greeted)

    def span(c):
        return pl.ds(pl.multiple_of(c * chunk, chunk), chunk)

    def narrow(c):
        return pl.ds(pl.multiple_of(c * part, part), part)

    landing = jnp.where(inner, 1, 0)

    def own_stream(c):
        return pltpu.make_async_remote_copy(
            src_ref=owned_ref.at[span(c)],
            dst_ref=block_buf.at[landing, span(c)],
            send_sem=stream_send.at[0],
            recv_sem=stream_recv.at[landing, c],
            device_id=(ahead, mem),
            device_id_type=MESH,
        )

    def forward_stream(c):
        return pltpu.make_async_remote_copy(
            src_ref=block_buf.at[0, span(c)],
            dst_ref=block_buf.at[2, span(c)],
            send_sem=stream_send.at[1],
            recv_sem=stream_recv.at[2, c],
            device_id=(ahead, mem),
            device_id_type=MESH,
        )

    def stream_arrival(block, c):
        return pltpu.make_async_remote_copy(
            src_ref=owned_ref.at[span(c)],
            dst_ref=block_buf.at[block - 1, span(c)],
            send_sem=stream_send.at[0],
            recv_sem=stream_recv.at[block - 1, c],
            device_id=(ahead, mem),
            device_id_type=MESH,
        )

    def member_copy(k):
        peer = lax.rem(mem + k, nm)
        return pltpu.make_async_remote_copy(
            src_ref=anom_ref,
            dst_ref=pieces.at[nm - 1 - k],
            send_sem=m_send.at[k],
            recv_sem=m_recv.at[nm - k],
            device_id=(tile, peer),
            device_id_type=MESH,
        )

    def parcel(block, t, rows_of):
        return pltpu.make_async_remote_copy(
            src_ref=send_buf.at[block, t, rows_of],
            dst_ref=recv_ref.at[source[block], rows_of],
            send_sem=p_send.at[block],
            recv_sem=a_recv.at[0],
            device_id=(zone_base + t, mem),
            device_id_type=MESH,
        )

    def away_parcel(block, t, rows_of):
        return pltpu.make_async_remote_copy(
            src_ref=away_buf.at[AWAY[block], t, rows_of],
            dst_ref=recv_ref.at[source[block], rows_of],
            send_sem=away_send.at[AWAY[block]],
            recv_sem=a_recv.at[0],
            device_id=(away_base + t, mem),
            device_id_type=MESH,
        )

    fold_part = chunk // FOLD

    def folded(c):
        return pl.ds(pl.multiple_of(c * fold_part, fold_part), fold_part)

    def compact(i, c):
        return pltpu.make_async_remote_copy(
            src_ref=away_buf.at[i, folded(c)],
            dst_ref=compact_buf.at[i, folded(c)],
            send_sem=away_send.at[i],
            recv_sem=away_recv.at[i, c],
            device_id=(along(-1), mem),
            device_id_type=MESH,
        )

    def spread_out_rows(block, c, count, size):
        block_ref = owned_ref if block == OWN else block_buf.at[block - 1]
        return jnp.concatenate(
            [
                block_ref[pl.ds(pl.multiple_of(c * chunk + g * size, size), size), :]
                for g in range(count)
            ],
            axis=1,
        )

    def pack(block, c, pick_ref, pick, out_ref):
        wide = spread_out_rows(block, c, groups, part)

        def pair(h, carry):
            out = jnp.dot(wide, pick_ref[pick, h], preferred_element_type=jnp.float32)
            out = out.astype(jnp.bfloat16)
            out_ref[pick, 2 * h, narrow(c)] = out[:, :LANES]
            out_ref[pick, 2 * h + 1, narrow(c)] = out[:, LANES:]
            return carry

        lax.fori_loop(0, pairs, pair, 0, unroll=pairs <= 2)

    def pack_near(block, c):
        pack(block, c, picks, block, send_buf)

    def pack_away(block, c):
        if not tight:
            pack(block, c, away_picks, AWAY[block], away_buf)
            return
        wide = spread_out_rows(block, c, FOLD, fold_part)
        out = jnp.dot(wide, away_picks[AWAY[block]], preferred_element_type=jnp.float32)
        away_buf[AWAY[block], folded(c)] = out.astype(jnp.bfloat16)

    def unpack(i, c):
        held = compact_buf[i, folded(c)]

        def one(t, carry):
            out = jnp.dot(held, open_picks[i, t], preferred_element_type=jnp.float32)
            out = out.astype(jnp.bfloat16)
            for v in range(2):
                rows_of = pl.ds(
                    pl.multiple_of(c * part + v * fold_part, fold_part), fold_part
                )
                send_buf[1 + i, t, rows_of] = out[:, v * LANES : (v + 1) * LANES]
            return carry

        lax.fori_loop(0, zone_tiles, one, 0, unroll=zone_tiles <= 4)

    def send_near(block, c):
        def one(t, carry):
            @pl.when(zone_base + t != tile)
            def _():
                parcel(block, t, narrow(c)).start()

            return carry

        lax.fori_loop(0, zone_tiles, one, 0)

    def send_away(block, c):
        if tight:
            compact(AWAY[block], c).start()
            return

        def one(t, carry):
            away_parcel(block, t, narrow(c)).start()
            return carry

        lax.fori_loop(0, zone_tiles, one, 0)

    def keep(block):
        return pltpu.make_async_copy(
            send_buf.at[block, place], recv_ref.at[source[block]], local_sem.at[4 + block]
        )

    def start_own(c, carry):
        own_stream(c).start()
        return carry

    lax.fori_loop(0, chunks, start_own, 0)

    @pl.when(inner)
    def _():
        def own_step(c, carry):
            pack_away(OWN, c)
            pack_near(OWN, c)
            send_away(OWN, c)

            @pl.when(c > 0)
            def _():
                send_near(OWN, c - 1)

            return carry

        lax.fori_loop(0, chunks, own_step, 0)

    @pl.when(outer)
    def _():
        def own_step(c, carry):
            pack_near(OWN, c)

            @pl.when(c > 0)
            def _():
                send_near(OWN, c - 1)

            return carry

        lax.fori_loop(0, chunks, own_step, 0)

    for k in range(1, nm):
        member_copy(k).start()

    @pl.when(inner)
    def _():
        build_away(PARTNER)
        build_near(PARTNER)
        build_near(OUTER)

    send_near(OWN, chunks - 1)
    keep(OWN).start()

    @pl.when(inner)
    def _():
        def mid_step(c, carry):
            stream_arrival(OUTER, c).wait_recv()
            forward_stream(c).start()
            stream_arrival(PARTNER, c).wait_recv()
            pack_away(PARTNER, c)
            pack_near(PARTNER, c)
            send_away(PARTNER, c)
            pack_near(OUTER, c)
            send_near(PARTNER, c)

            @pl.when(c > 0)
            def _():
                send_near(OUTER, c - 1)

            return carry

        lax.fori_loop(0, chunks, mid_step, 0)
        build_away(FAR)
        build_near(FAR)
        send_near(OUTER, chunks - 1)
        keep(OUTER).start()
        keep(PARTNER).start()

        def far_step(c, carry):
            stream_arrival(FAR, c).wait_recv()
            pack_away(FAR, c)
            pack_near(FAR, c)
            send_away(FAR, c)

            @pl.when(c > 0)
            def _():
                send_near(FAR, c - 1)

            return carry

        lax.fori_loop(0, chunks, far_step, 0)

    fweight = fweight_ref[...].astype(jnp.float32)

    def spread_rows(s, carry):
        ids = lax.broadcasted_iota(jnp.int32, (slots, obs), 0) + s * slots
        total = jnp.zeros((slots, obs), jnp.float32)
        for j in range(foot_ref.shape[0]):
            total = total + jnp.where(
                ids == foot_ref[j : j + 1, :], fweight[j : j + 1, :], 0.0
            )
        spread[pl.ds(pl.multiple_of(s * slots, slots), slots), :] = total.astype(jnp.bfloat16)
        return carry

    if tight:

        @pl.when(outer)
        def _():
            for i in range(3):
                build_open(i)

    lax.fori_loop(0, n, spread_rows, 0)

    @pl.when(inner)
    def _():
        send_near(FAR, chunks - 1)
        keep(FAR).start()

    if tight:

        def open_compact(i):
            def step(c, carry):
                compact(i, c).wait_recv()
                unpack(i, c)

                @pl.when(c > 0)
                def _():
                    send_near(1 + i, c - 1)

                return carry

            lax.fori_loop(0, chunks, step, 0)

        @pl.when(outer)
        def _():
            open_compact(0)
            send_near(1, chunks - 1)
            keep(1).start()
            open_compact(1)
            send_near(2, chunks - 1)
            keep(2).start()

    spread_out = pltpu.make_async_copy(spread, spread_ref, local_sem.at[2])
    spread_out.start()
    for k in range(1, nm):
        pltpu.make_async_remote_copy(
            src_ref=anom_ref,
            dst_ref=pieces.at[k - 1],
            send_sem=m_send.at[k],
            recv_sem=m_recv.at[k],
            device_id=(tile, lax.rem(mem + k, nm)),
            device_id_type=MESH,
        ).wait()

    mean_wide[...] = mean_ref[...].astype(jnp.float32)
    weight_wide[...] = jnp.transpose(weight_ref[...].astype(jnp.float32))
    mine = weight_wide[pl.ds(mem * mem_dev, mem_dev), :].astype(jnp.bfloat16)
    for p in range(nm):
        shares[p] = mine[:, p * mem_dev : (p + 1) * mem_dev]

    def mix(first, count):
        mixture = jnp.zeros((mem_dev, count * cols), jnp.float32)
        for k in range(nm):
            held = anom_ref if k == 0 else pieces.at[k - 1]
            side = jnp.concatenate([held[first + i] for i in range(count)], axis=1)
            share = shares[lax.rem(mem + k, nm)]
            mixture = mixture + jnp.dot(share, side, preferred_element_type=jnp.float32)
        for i in range(count):
            total = mean_wide[pl.ds(first + i, 1), :] + mixture[:, i * cols : (i + 1) * cols]
            mixed[first + i] = total.astype(jnp.bfloat16)

    def mix_block(b, carry):
        mix(b * MIX_LEVELS, MIX_LEVELS)
        return carry

    full = levels // MIX_LEVELS
    lax.fori_loop(0, full, mix_block, 0)
    if levels % MIX_LEVELS:
        mix(full * MIX_LEVELS, levels % MIX_LEVELS)

    analysis_out = pltpu.make_async_copy(mixed, analysis_ref, local_sem.at[3])
    analysis_out.start()

    if tight:

        @pl.when(outer)
        def _():
            open_compact(2)
            send_near(3, chunks - 1)
            keep(3).start()

    def gone(ref, sem):
        pltpu.make_async_remote_copy(
            src_ref=ref,
            dst_ref=ref,
            send_sem=sem,
            recv_sem=a_recv.at[0],
            device_id=(ahead, mem),
            device_id_type=MESH,
        ).wait_send()

    def come(count):
        pltpu.make_async_remote_copy(
            src_ref=recv_ref.at[pl.ds(0, count)],
            dst_ref=recv_ref.at[pl.ds(0, count)],
            send_sem=p_send.at[0],
            recv_sem=a_recv.at[0],
            device_id=(ahead, mem),
            device_id_type=MESH,
        ).wait_recv()

    gone(owned_ref, stream_send.at[0])
    gone(send_buf.at[OWN, pl.ds(0, zone_tiles - 1)], p_send.at[OWN])

    def line_sent():
        for block in (OUTER, PARTNER, FAR):
            gone(send_buf.at[block, pl.ds(0, zone_tiles - 1)], p_send.at[block])
            keep(block).wait()

    @pl.when(inner)
    def _():
        gone(block_buf.at[0], stream_send.at[1])
        for block in AWAY:
            gone(away_buf.at[AWAY[block]], away_send.at[AWAY[block]])
        line_sent()

    @pl.when(outer)
    def _():
        if tight:
            line_sent()
            come(n - ZONES)
        else:
            come(n - 1)

    @pl.when(inner)
    def _():
        come(n - ZONES)

    keep(OWN).wait()
    spread_out.wait()
    analysis_out.wait()


def combine_kernel(
    n, groups, bias_ref, recv_ref, spread_ref, mixed_ref, out_ref, analysis_ref, sem
):
    step = pl.program_id(0)
    carry_out = pltpu.make_async_copy(mixed_ref, analysis_ref, sem)

    @pl.when(step == 0)
    def _():
        carry_out.start()

    slots = spread_ref.shape[0] // n
    channels, members = out_ref.shape[0], out_ref.shape[1]
    stacked = jnp.concatenate(
        [
            jnp.concatenate(
                [recv_ref[s, :, g * slots : (g + 1) * slots] for s in range(n)], axis=1
            )
            for g in range(groups)
        ],
        axis=0,
    )
    prior = jnp.dot(stacked, spread_ref[...], preferred_element_type=jnp.float32)
    for c in range(channels):
        bias = bias_ref[step * channels + c]
        out_ref[c] = prior[c * members : (c + 1) * members, :] + bias

    @pl.when(step == pl.num_programs(0) - 1)
    def _():
        carry_out.wait()


def chunk_count(channels, mem_dev, groups):
    def fits(count):
        part = channels * mem_dev // (count * groups)
        return channels % count == 0 and part * count * groups == channels * mem_dev and part % 16 == 0

    return next(count for count in (6, 4, 3, 2, 1) if count == 1 or fits(count))


def shards(
    n,
    nm,
    anomalies,
    analysis_weights,
    background_mean,
    background,
    jacobian_table,
    channel_list,
    send_slots,
    footprint,
    footprint_weight,
    channel_bias,
):
    mem_dev, levels, cols = anomalies.shape
    channels = channel_list.shape[0]
    slots = send_slots.shape[2]
    obs, foot = footprint.shape
    groups = LANES // slots
    rows = channels * mem_dev
    members = analysis_weights.shape[1]
    chunks = chunk_count(channels, mem_dev, groups)
    zone_tiles = n // ZONES
    vmem = pl.BlockSpec(memory_space=pltpu.VMEM)
    hbm = pl.BlockSpec(memory_space=pl.ANY)
    far = pl.BlockSpec(memory_space=pltpu.HBM)
    dma = pltpu.SemaphoreType.DMA
    chunk = rows // chunks
    select = mem_dev % 8 == 0
    foldable = chunk % (16 * FOLD) == 0

    front_out = [
        jax.ShapeDtypeStruct((ZONES, n, LANES), jnp.int32),
        jax.ShapeDtypeStruct((1, 1), jnp.float32),
    ]
    front_scratch = [
        pltpu.VMEM((1, n, LANES), jnp.int32),
        pltpu.VMEM((ZONES, n, LANES), jnp.int32),
        pltpu.VMEM((1, 1, LANES), jnp.int32),
        pltpu.VMEM((n, 1, LANES), jnp.int32),
    ]
    front_args, front_specs = [send_slots[0]], [vmem]
    if select:
        spectrum = jacobian_table.shape[0]
        front_out.insert(0, jax.ShapeDtypeStruct((rows, cols), jnp.bfloat16))
        front_scratch += [
            pltpu.VMEM((levels, spectrum), jnp.bfloat16),
            pltpu.VMEM((levels, mem_dev, cols), jnp.bfloat16),
            pltpu.VMEM((levels, mem_dev, cols), jnp.float32),
            pltpu.VMEM((-(-levels // LANES) * LANES, -(-channels // LANES) * LANES), jnp.float32),
            pltpu.VMEM((rows, cols), jnp.float32),
        ]
        front_args = [
            jnp.transpose(jacobian_table),
            channel_list[None, :],
            jnp.transpose(background, (1, 0, 2)),
            send_slots[0],
        ]
        front_specs = [far, vmem, far, vmem]
    front = pl.pallas_call(
        functools.partial(front_kernel, n, select),
        out_shape=tuple(front_out),
        in_specs=front_specs,
        out_specs=(vmem,) * (len(front_out) - 1) + (pl.BlockSpec(memory_space=pltpu.SMEM),),
        scratch_shapes=front_scratch + [dma((2,)), dma((2,)), dma((2,))],
        compiler_params=pltpu.CompilerParams(
            collective_id=0, has_side_effects=True, vmem_limit_bytes=62 * 1024 * 1024
        ),
        name="front",
    )(*front_args)
    tables, count = front[-2:]
    if select:
        owned = front[0]
    else:
        chosen = (
            jnp.arange(jacobian_table.shape[0], dtype=jnp.int32)[:, None] == channel_list[None, :]
        ).astype(jnp.bfloat16)
        selected = jnp.einsum(
            "sl,sc->cl", jacobian_table, chosen, preferred_element_type=jnp.float32
        ).astype(jnp.bfloat16)
        owned = jnp.einsum(
            "cl,klx->ckx", selected, background, preferred_element_type=jnp.float32
        ).astype(jnp.bfloat16).reshape(rows, cols)

    def rest(tight, owned, tables, anomalies, weights, mean, footprint, footprint_weight, bias):
        part = rows // groups
        if tight:
            variant = [
                pltpu.VMEM((3, rows // FOLD, FOLD * CAP), jnp.bfloat16),
                pltpu.VMEM((3, rows, cols), jnp.bfloat16),
                pltpu.VMEM((3, rows // FOLD, FOLD * CAP), jnp.bfloat16),
                pltpu.VMEM((4, zone_tiles // 2, groups * cols, 2 * LANES), jnp.bfloat16),
                pltpu.VMEM((3, FOLD * cols, FOLD * CAP), jnp.bfloat16),
                pltpu.VMEM((3, zone_tiles, FOLD * CAP, 2 * LANES), jnp.bfloat16),
            ]
        else:
            spare = pltpu.VMEM((8, LANES), jnp.bfloat16)
            variant = [
                pltpu.VMEM((3, zone_tiles, part, LANES), jnp.bfloat16),
                pltpu.VMEM((3, rows, cols), jnp.bfloat16),
                spare,
                pltpu.VMEM((4, zone_tiles // 2, groups * cols, 2 * LANES), jnp.bfloat16),
                pltpu.VMEM((3, zone_tiles // 2, groups * cols, 2 * LANES), jnp.bfloat16),
                spare,
            ]
        received, mixed, spread = pl.pallas_call(
            functools.partial(exchange_kernel, n, nm, chunks, tight),
            out_shape=(
                jax.ShapeDtypeStruct((n, part, LANES), jnp.bfloat16),
                jax.ShapeDtypeStruct((levels, mem_dev, cols), jnp.bfloat16),
                jax.ShapeDtypeStruct((n * slots, obs), jnp.bfloat16),
            ),
            in_specs=[vmem] * 7,
            out_specs=(hbm, hbm, hbm),
            scratch_shapes=[pltpu.VMEM((4, zone_tiles, part, LANES), jnp.bfloat16)]
            + variant
            + [
                pltpu.VMEM((max(nm - 1, 1), levels, mem_dev, cols), jnp.bfloat16),
                pltpu.VMEM((levels, mem_dev, cols), jnp.bfloat16),
                pltpu.VMEM((n * slots, obs), jnp.bfloat16),
                pltpu.VMEM((levels, cols), jnp.float32),
                pltpu.VMEM((members, members), jnp.float32),
                pltpu.VMEM((nm, mem_dev, mem_dev), jnp.bfloat16),
                dma((2,)),
                dma((3, chunks)),
                dma((nm,)),
                dma((nm,)),
                dma((4,)),
                dma((3,)),
                dma((3, chunks)),
                dma((1,)),
                dma((8,)),
            ],
            compiler_params=pltpu.CompilerParams(
                collective_id=1 + tight, has_side_effects=True, vmem_limit_bytes=44 * 1024 * 1024
            ),
            name="exchange_tight" if tight else "exchange",
        )(owned, tables, anomalies, weights, mean, footprint, footprint_weight)
        return pl.pallas_call(
            functools.partial(combine_kernel, n, groups),
            out_shape=(
                jax.ShapeDtypeStruct((channels, mem_dev, obs), jnp.float32),
                jax.ShapeDtypeStruct(mixed.shape, mixed.dtype),
            ),
            grid=(chunks,),
            in_specs=[
                pl.BlockSpec(memory_space=pltpu.SMEM),
                pl.BlockSpec((n, part // chunks, LANES), lambda i: (0, i, 0)),
                pl.BlockSpec((n * slots, obs), lambda i: (0, 0)),
                vmem,
            ],
            out_specs=(
                pl.BlockSpec((channels // chunks, mem_dev, obs), lambda i: (i, 0, 0)),
                hbm,
            ),
            scratch_shapes=[dma],
            compiler_params=pltpu.CompilerParams(vmem_limit_bytes=24 * 1024 * 1024),
            name="combine",
        )(bias, received, spread, mixed)

    operands = (
        owned,
        tables,
        jnp.transpose(anomalies, (1, 0, 2)),
        analysis_weights[0],
        background_mean,
        jnp.transpose(footprint),
        jnp.transpose(footprint_weight),
        channel_bias,
    )
    if foldable:
        prior, analysis = lax.cond(
            count[0, 0] <= CAP,
            functools.partial(rest, True),
            functools.partial(rest, False),
            *operands,
        )
    else:
        prior, analysis = rest(False, *operands)
    return jnp.transpose(analysis, (1, 0, 2)), prior


def solution(mesh):
    placed = (
        P("mem", None, "tile"),
        P("tile", None, None),
        P(None, "tile"),
        P("mem", None, "tile"),
        P(),
        P(),
        P("tile", None, None),
        P("tile", None),
        P("tile", None),
        P(),
    )
    return jax.shard_map(
        functools.partial(shards, mesh.shape["tile"], mesh.shape["mem"]),
        mesh=mesh,
        in_specs=placed,
        out_specs=(P("mem", None, "tile"), P(None, "mem", "tile")),
        check_vma=False,
    )
```

```python
import functools

import jax
import jax.numpy as jnp
from jax import lax
from jax.experimental import pallas as pl
from jax.experimental.pallas import tpu as pltpu
from jax.sharding import PartitionSpec as P

LANES = 128
MESH = pl.DeviceIdType.MESH
ZONES = 4
MIX_LEVELS = 8

OWN, OUTER, PARTNER, FAR = range(4)
AWAY = {OWN: 0, PARTNER: 1, FAR: 2}
CAP = 80
WIDE = 112
FOLD = 8


def needed(table_ref, source, base, count, cols):
    column = lax.broadcasted_iota(jnp.int32, (cols, LANES), 0)

    def one(t, hit):
        row = table_ref[source, pl.ds(base + t, 1), :]
        return jnp.where(column == row, 1.0, hit)

    hit = lax.fori_loop(0, count, one, jnp.zeros((cols, LANES), jnp.float32))
    return jnp.max(hit, axis=1, keepdims=True)


def positions(mask, cols):
    before = lax.broadcasted_iota(jnp.int32, (cols, cols), 1) < lax.broadcasted_iota(
        jnp.int32, (cols, cols), 0
    )
    full = jnp.broadcast_to(mask, (cols, LANES)).astype(jnp.bfloat16)
    return jnp.dot(
        jnp.where(before, 1.0, 0.0).astype(jnp.bfloat16), full, preferred_element_type=jnp.float32
    )


def front_kernel(
    n,
    select,
    *refs,
):
    if select:
        (table_ref, list_ref, field_ref, slots_ref, owned_ref, tables_ref, count_ref,
         message, gathered, counted, counts, table, field, wide, chosen, radiance,
         sends, arrives, local_sem) = refs
    else:
        (slots_ref, tables_ref, count_ref, message, gathered, counted, counts,
         sends, arrives, local_sem) = refs
    tile = lax.axis_index("tile")
    mem = lax.axis_index("mem")
    slots = slots_ref.shape[1]
    groups = LANES // slots
    cols = LANES
    zone_tiles = n // ZONES
    zone = tile // zone_tiles
    barrier = pltpu.get_barrier_semaphore()

    def greet(k, carry):
        pl.semaphore_signal(
            barrier, inc=1, device_id=(lax.rem(tile + k, n), mem), device_id_type=MESH
        )
        return carry

    lax.fori_loop(1, n, greet, 0)
    if select:
        load_table = pltpu.make_async_copy(table_ref, table, local_sem.at[0])
        load_table.start()
        load_field = pltpu.make_async_copy(field_ref, field, local_sem.at[1])
        load_field.start()

    message[0] = jnp.concatenate([slots_ref[...]] * groups, axis=1)
    most = jnp.zeros((1, 1), jnp.float32)
    for far in (0, ZONES - 1):
        mask = needed(message, 0, far * zone_tiles, zone_tiles, cols)
        total = jnp.sum(mask, axis=0, keepdims=True)
        most = jnp.maximum(most, jnp.where(zone == far, 0.0, total - CAP))
    across = needed(message, 0, (1 - zone // 2) * (n // 2), n // 2, cols)
    most = jnp.maximum(most, jnp.sum(across, axis=0, keepdims=True) - WIDE)
    counted[0] = jnp.broadcast_to(most, (1, LANES)).astype(jnp.int32)
    pl.semaphore_wait(barrier, n - 1)

    def tell(k, carry):
        pltpu.make_async_remote_copy(
            src_ref=counted.at[0],
            dst_ref=counts.at[tile],
            send_sem=sends.at[0],
            recv_sem=arrives.at[0],
            device_id=(lax.rem(tile + k, n), mem),
            device_id_type=MESH,
        ).start()
        return carry

    lax.fori_loop(1, n, tell, 0)
    for k in range(1, ZONES):
        pltpu.make_async_remote_copy(
            src_ref=message.at[0],
            dst_ref=gathered.at[zone],
            send_sem=sends.at[1],
            recv_sem=arrives.at[1],
            device_id=(lax.rem(tile + k * zone_tiles, n), mem),
            device_id_type=MESH,
        ).start()

    if select:
        spectrum = table_ref.shape[1]
        levels, mem_dev = field_ref.shape[0], field_ref.shape[1]
        channels = list_ref.shape[1]
        load_field.wait()
        wide[...] = field[...].astype(jnp.float32)
        load_table.wait()
        block = 11 * LANES
        total = jnp.zeros((levels, channels), jnp.float32)
        for first in range(0, spectrum, block):
            size = min(block, spectrum - first)
            entry = lax.broadcasted_iota(jnp.int32, (size, channels), 0) + first
            pick = jnp.where(entry == list_ref[...], 1.0, 0.0).astype(jnp.bfloat16)
            total = total + jnp.dot(
                table[:, first : first + size], pick, preferred_element_type=jnp.float32
            )
        chosen[...] = jnp.zeros_like(chosen)
        chosen[0:levels, 0:channels] = total
        picked = jnp.transpose(chosen[...])[:channels, :levels].astype(jnp.bfloat16)
        flat = wide.reshape(levels * mem_dev, cols)

        def member(k, carry):
            profile = flat[pl.ds(k, levels, stride=mem_dev), :].astype(jnp.bfloat16)
            radiance[pl.ds(k, channels, stride=mem_dev), :] = jnp.dot(
                picked, profile, preferred_element_type=jnp.float32
            )
            return carry

        lax.fori_loop(0, mem_dev, member, 0, unroll=8)
        owned_ref[...] = radiance[...].astype(jnp.bfloat16)

    counts[tile] = counted[0]
    gathered[zone] = message[0]

    def everyone(ref, count, kind):
        span = ref.at[pl.ds(0, count)]
        return pltpu.make_async_remote_copy(
            src_ref=span,
            dst_ref=span,
            send_sem=sends.at[kind],
            recv_sem=arrives.at[kind],
            device_id=(lax.rem(tile + 1, n), mem),
            device_id_type=MESH,
        )

    everyone(gathered, ZONES - 1, 1).wait_recv()
    tables_ref[...] = gathered[...]
    everyone(counts, n - 1, 0).wait_recv()

    def highest(s, top):
        return jnp.maximum(top, counts[s])

    top = lax.fori_loop(0, n, highest, jnp.zeros((1, LANES), jnp.int32))
    count_ref[0, 0] = jnp.max(top.astype(jnp.float32))
    everyone(counts, n - 1, 0).wait_send()
    everyone(gathered, ZONES - 1, 1).wait_send()


def exchange_kernel(
    n,
    nm,
    chunks,
    tight,
    owned_ref,
    tables_ref,
    anom_ref,
    weight_ref,
    mean_ref,
    foot_ref,
    fweight_ref,
    recv_ref,
    analysis_ref,
    spread_ref,
    send_buf,
    away_buf,
    block_buf,
    compact_buf,
    picks,
    away_picks,
    open_picks,
    cross_buf,
    cross_in,
    cross_picks,
    narrow_picks,
    pieces,
    mixed,
    spread,
    mean_wide,
    weight_wide,
    shares,
    stream_send,
    stream_recv,
    m_send,
    m_recv,
    p_send,
    away_send,
    away_recv,
    cross_send,
    cross_recv,
    a_recv,
    local_sem,
):
    tile = lax.axis_index("tile")
    mem = lax.axis_index("mem")
    rows, cols = owned_ref.shape
    slots = spread_ref.shape[0] // n
    groups = LANES // slots
    obs = foot_ref.shape[1]
    levels, mem_dev = anom_ref.shape[0], anom_ref.shape[1]
    zone_tiles = n // ZONES
    pairs = zone_tiles // 2
    chunk = rows // chunks
    part = chunk // groups

    zone = tile // zone_tiles
    place = lax.rem(tile, zone_tiles)
    sign = 1 - 2 * (zone // 2)
    inner = jnp.logical_or(zone == 1, zone == 2)
    outer = jnp.logical_not(inner)
    stride = sign * zone_tiles
    ahead = lax.rem(tile + stride + n, n)

    def along(steps):
        return lax.rem(tile + steps * stride + ZONES * n, n)

    if tight:
        source = (tile, along(jnp.where(inner, -1, 1)), along(jnp.where(inner, 1, 2)),
                  along(jnp.where(inner, 2, 3)))
    else:
        source = (tile, along(-1), along(1), along(2))
    zone_base = zone * zone_tiles
    away_base = lax.rem(zone_base - stride + n, n)

    barrier = pltpu.get_barrier_semaphore()

    def greet(k, carry):
        pl.semaphore_signal(
            barrier,
            inc=1,
            device_id=(zone_base + lax.rem(place + k, zone_tiles), mem),
            device_id_type=MESH,
        )
        return carry

    lax.fori_loop(1, zone_tiles, greet, 0)
    for side in (-1, 1):

        @pl.when(jnp.logical_and(zone + side >= 0, zone + side < ZONES))
        def _():
            def greet_side(t, carry):
                pl.semaphore_signal(
                    barrier,
                    inc=1,
                    device_id=(zone_base + side * zone_tiles + t, mem),
                    device_id_type=MESH,
                )
                return carry

            lax.fori_loop(0, zone_tiles, greet_side, 0)

    for k in range(1, nm):
        pl.semaphore_signal(
            barrier, inc=1, device_id=(tile, lax.rem(mem + k, nm)), device_id_type=MESH
        )

    lane_group = lax.broadcasted_iota(jnp.int32, (1, LANES), 1) // slots

    def build(origin, base, into, first_pick):
        row_id = lax.broadcasted_iota(jnp.int32, (groups * cols, 2 * LANES), 0)

        def want(t):
            row = tables_ref[origin // zone_tiles, pl.ds(base + t, 1), :]
            return jnp.maximum(row, 0) + lane_group * cols

        def pair(h, carry):
            wants = jnp.concatenate([want(2 * h), want(2 * h + 1)], axis=1)
            into[first_pick, h] = jnp.where(row_id == wants, 1.0, 0.0).astype(jnp.bfloat16)
            return carry

        lax.fori_loop(0, pairs, pair, 0)

    def build_near(block):
        build(source[block], zone_base, picks, block)

    half = n // 2
    half_base = (zone // 2) * half
    other_base = half - half_base

    def fold_columns(mask, cap, g):
        place_of = positions(mask, cols)[:, 0:1].astype(jnp.int32) + g * cap
        place_of = jnp.where(mask > 0.0, place_of, -1)
        lane = lax.broadcasted_iota(jnp.int32, (cols, FOLD * cap), 1)
        return jnp.where(lane == place_of, 1.0, 0.0).astype(jnp.bfloat16)

    def build_fold(into, origin, base, count, cap):
        mask = needed(tables_ref, origin // zone_tiles, base, count, cols)
        for g in range(FOLD):
            into[g * cols : (g + 1) * cols, :] = fold_columns(mask, cap, g)

    def build_away(block):
        if tight:
            build_fold(away_picks.at[AWAY[block]], source[block], away_base, zone_tiles, CAP)
        else:
            build(source[block], away_base, away_picks, AWAY[block])

    def build_cross(i):
        build_fold(cross_picks.at[i], source[i], other_base, half, WIDE)

    def build_narrow(block):
        line = source[block] // zone_tiles
        wide_mask = needed(tables_ref, line, half_base, half, cols)
        wide_place = jnp.where(wide_mask > 0.0, positions(wide_mask, cols), -1.0)
        wide_place = jnp.transpose(wide_place)[0:1, :].astype(jnp.int32)
        row_id = lax.broadcasted_iota(jnp.int32, (WIDE, cols), 0)
        back = jnp.where(row_id == wide_place, 1.0, 0.0).astype(jnp.bfloat16)
        mask = needed(tables_ref, line, away_base, zone_tiles, cols)
        for g in range(FOLD):
            narrow_picks[block - PARTNER, g * WIDE : (g + 1) * WIDE, :] = jnp.dot(
                back, fold_columns(mask, CAP, g), preferred_element_type=jnp.float32
            ).astype(jnp.bfloat16)

    def build_open(i, origin, base, count, cap):
        line = origin // zone_tiles
        mask = needed(tables_ref, line, base, count, cols)
        column = lax.broadcasted_iota(jnp.int32, (cols, LANES), 0)
        row_id = lax.broadcasted_iota(jnp.int32, (FOLD * cap, 2 * LANES), 0)

        def one(t, carry):
            row = tables_ref[line, pl.ds(zone_base + t, 1), :]
            ahead_of = jnp.where(column < row, mask, 0.0)
            spot = jnp.sum(ahead_of, axis=0, keepdims=True).astype(jnp.int32)
            wants = jnp.concatenate(
                [spot + (2 * lane_group + v) * cap for v in range(2)], axis=1
            )
            open_picks[i, t, 0 : FOLD * cap] = jnp.where(row_id == wants, 1.0, 0.0).astype(
                jnp.bfloat16
            )
            return carry

        lax.fori_loop(0, zone_tiles, one, 0)

    @pl.when(inner)
    def _():
        if tight:
            build_cross(OWN)
        build_away(OWN)

    build_near(OWN)

    greeted = zone_tiles - 1 + nm - 1 + jnp.where(inner, 2, 1) * zone_tiles
    pl.semaphore_wait(barrier, greeted)

    def span(c):
        return pl.ds(pl.multiple_of(c * chunk, chunk), chunk)

    def narrow(c):
        return pl.ds(pl.multiple_of(c * part, part), part)

    landing = 0 if tight else jnp.where(inner, 1, 0)

    def own_stream(c):
        return pltpu.make_async_remote_copy(
            src_ref=owned_ref.at[span(c)],
            dst_ref=block_buf.at[landing, span(c)],
            send_sem=stream_send.at[0],
            recv_sem=stream_recv.at[landing, c],
            device_id=(ahead, mem),
            device_id_type=MESH,
        )

    def forward_stream(c):
        return pltpu.make_async_remote_copy(
            src_ref=block_buf.at[0, span(c)],
            dst_ref=block_buf.at[2, span(c)],
            send_sem=stream_send.at[1],
            recv_sem=stream_recv.at[2, c],
            device_id=(ahead, mem),
            device_id_type=MESH,
        )

    def stream_arrival(block, c):
        return pltpu.make_async_remote_copy(
            src_ref=owned_ref.at[span(c)],
            dst_ref=block_buf.at[block - 1, span(c)],
            send_sem=stream_send.at[0],
            recv_sem=stream_recv.at[block - 1, c],
            device_id=(ahead, mem),
            device_id_type=MESH,
        )

    def member_copy(k):
        peer = lax.rem(mem + k, nm)
        return pltpu.make_async_remote_copy(
            src_ref=anom_ref,
            dst_ref=pieces.at[nm - 1 - k],
            send_sem=m_send.at[k],
            recv_sem=m_recv.at[nm - k],
            device_id=(tile, peer),
            device_id_type=MESH,
        )

    def parcel(block, t, rows_of):
        return pltpu.make_async_remote_copy(
            src_ref=send_buf.at[block, t, rows_of],
            dst_ref=recv_ref.at[source[block], rows_of],
            send_sem=p_send.at[block],
            recv_sem=a_recv.at[0],
            device_id=(zone_base + t, mem),
            device_id_type=MESH,
        )

    def away_parcel(block, t, rows_of):
        return pltpu.make_async_remote_copy(
            src_ref=away_buf.at[AWAY[block], t, rows_of],
            dst_ref=recv_ref.at[source[block], rows_of],
            send_sem=away_send.at[AWAY[block]],
            recv_sem=a_recv.at[0],
            device_id=(away_base + t, mem),
            device_id_type=MESH,
        )

    fold_part = chunk // FOLD

    def folded(c):
        return pl.ds(pl.multiple_of(c * fold_part, fold_part), fold_part)

    def compact(i, c):
        return pltpu.make_async_remote_copy(
            src_ref=away_buf.at[i, folded(c)],
            dst_ref=compact_buf.at[i, folded(c)],
            send_sem=away_send.at[i],
            recv_sem=away_recv.at[i, c],
            device_id=(along(-1), mem),
            device_id_type=MESH,
        )

    def cross(i, c):
        return pltpu.make_async_remote_copy(
            src_ref=cross_buf.at[i, folded(c)],
            dst_ref=cross_in.at[i, folded(c)],
            send_sem=cross_send.at[i],
            recv_sem=cross_recv.at[i, c],
            device_id=(ahead, mem),
            device_id_type=MESH,
        )

    def spread_out_rows(block, c, count, size):
        block_ref = owned_ref if block == OWN else block_buf.at[block - 1]
        return jnp.concatenate(
            [
                block_ref[pl.ds(pl.multiple_of(c * chunk + g * size, size), size), :]
                for g in range(count)
            ],
            axis=1,
        )

    def pack(block, c, pick_ref, pick, out_ref):
        wide = spread_out_rows(block, c, groups, part)

        def pair(h, carry):
            out = jnp.dot(wide, pick_ref[pick, h], preferred_element_type=jnp.float32)
            out = out.astype(jnp.bfloat16)
            out_ref[pick, 2 * h, narrow(c)] = out[:, :LANES]
            out_ref[pick, 2 * h + 1, narrow(c)] = out[:, LANES:]
            return carry

        lax.fori_loop(0, pairs, pair, 0, unroll=pairs <= 2)

    def pack_near(block, c):
        pack(block, c, picks, block, send_buf)

    def pack_cross(i, c):
        wide = spread_out_rows(i, c, FOLD, fold_part)
        out = jnp.dot(wide, cross_picks[i], preferred_element_type=jnp.float32)
        cross_buf[i, folded(c)] = out.astype(jnp.bfloat16)

    def pack_away(block, c):
        if not tight:
            pack(block, c, away_picks, AWAY[block], away_buf)
            return
        if block == OWN:
            wide, pick = spread_out_rows(OWN, c, FOLD, fold_part), away_picks[AWAY[OWN]]
        else:
            i = block - PARTNER
            wide, pick = cross_in[i, folded(c)], narrow_picks[i]
        out = jnp.dot(wide, pick, preferred_element_type=jnp.float32)
        away_buf[AWAY[block], folded(c)] = out.astype(jnp.bfloat16)

    def unpack(held, i, cap, c):
        def one(t, carry):
            out = jnp.dot(
                held, open_picks[i, t, 0 : FOLD * cap], preferred_element_type=jnp.float32
            )
            out = out.astype(jnp.bfloat16)
            for v in range(2):
                rows_of = pl.ds(
                    pl.multiple_of(c * part + v * fold_part, fold_part), fold_part
                )
                send_buf[1 + i, t, rows_of] = out[:, v * LANES : (v + 1) * LANES]
            return carry

        lax.fori_loop(0, zone_tiles, one, 0, unroll=zone_tiles <= 4)

    def send_near(block, c):
        def one(t, carry):
            @pl.when(zone_base + t != tile)
            def _():
                parcel(block, t, narrow(c)).start()

            return carry

        lax.fori_loop(0, zone_tiles, one, 0)

    def send_away(block, c):
        if tight:
            compact(AWAY[block], c).start()
            return

        def one(t, carry):
            away_parcel(block, t, narrow(c)).start()
            return carry

        lax.fori_loop(0, zone_tiles, one, 0)

    def keep(block):
        return pltpu.make_async_copy(
            send_buf.at[block, place], recv_ref.at[source[block]], local_sem.at[4 + block]
        )

    def start_own(c, carry):
        own_stream(c).start()
        return carry

    if tight:

        @pl.when(outer)
        def _():
            lax.fori_loop(0, chunks, start_own, 0)
    else:
        lax.fori_loop(0, chunks, start_own, 0)

    def later(block, c):
        @pl.when(c > 0)
        def _():
            send_near(block, c - 1)

    @pl.when(inner)
    def _():
        def own_step(c, carry):
            if tight:
                pack_cross(OWN, c)
            pack_away(OWN, c)
            if tight:
                cross(OWN, c).start()
            pack_near(OWN, c)
            send_away(OWN, c)
            later(OWN, c)
            return carry

        lax.fori_loop(0, chunks, own_step, 0)

    @pl.when(outer)
    def _():
        def own_step(c, carry):
            pack_near(OWN, c)
            later(OWN, c)
            return carry

        lax.fori_loop(0, chunks, own_step, 0)

    for k in range(1, nm):
        member_copy(k).start()

    @pl.when(inner)
    def _():
        if tight:
            build_cross(OUTER)
            build_narrow(PARTNER)
            build_open(PARTNER - 1, source[PARTNER], half_base, half, WIDE)
        else:
            build_away(PARTNER)
            build_near(PARTNER)
        build_near(OUTER)

    send_near(OWN, chunks - 1)
    keep(OWN).start()

    @pl.when(inner)
    def _():
        def mid_step(c, carry):
            stream_arrival(OUTER, c).wait_recv()
            if tight:
                pack_cross(OUTER, c)
                cross(PARTNER - PARTNER, c).wait_recv()
                pack_away(PARTNER, c)
                cross(OUTER, c).start()
                unpack(cross_in[0, folded(c)], PARTNER - 1, WIDE, c)
            else:
                forward_stream(c).start()
                stream_arrival(PARTNER, c).wait_recv()
                pack_away(PARTNER, c)
                pack_near(PARTNER, c)
            send_away(PARTNER, c)
            pack_near(OUTER, c)
            send_near(PARTNER, c)
            later(OUTER, c)
            return carry

        lax.fori_loop(0, chunks, mid_step, 0)
        if tight:
            build_narrow(FAR)
            build_open(FAR - 1, source[FAR], half_base, half, WIDE)
        else:
            build_away(FAR)
            build_near(FAR)
        send_near(OUTER, chunks - 1)
        keep(OUTER).start()
        keep(PARTNER).start()

        def far_step(c, carry):
            if tight:
                cross(FAR - PARTNER, c).wait_recv()
                pack_away(FAR, c)
                unpack(cross_in[1, folded(c)], FAR - 1, WIDE, c)
            else:
                stream_arrival(FAR, c).wait_recv()
                pack_away(FAR, c)
                pack_near(FAR, c)
            send_away(FAR, c)
            later(FAR, c)
            return carry

        lax.fori_loop(0, chunks, far_step, 0)

    fweight = fweight_ref[...].astype(jnp.float32)

    def spread_rows(s, carry):
        ids = lax.broadcasted_iota(jnp.int32, (slots, obs), 0) + s * slots
        total = jnp.zeros((slots, obs), jnp.float32)
        for j in range(foot_ref.shape[0]):
            total = total + jnp.where(
                ids == foot_ref[j : j + 1, :], fweight[j : j + 1, :], 0.0
            )
        spread[pl.ds(pl.multiple_of(s * slots, slots), slots), :] = total.astype(jnp.bfloat16)
        return carry

    if tight:

        @pl.when(outer)
        def _():
            for i in range(3):
                build_open(i, source[1 + i], zone_base, zone_tiles, CAP)

    lax.fori_loop(0, n, spread_rows, 0)

    @pl.when(inner)
    def _():
        send_near(FAR, chunks - 1)
        keep(FAR).start()

    if tight:

        def open_compact(i):
            def step(c, carry):
                compact(i, c).wait_recv()
                unpack(compact_buf[i, folded(c)], i, CAP, c)

                @pl.when(c > 0)
                def _():
                    send_near(1 + i, c - 1)

                return carry

            lax.fori_loop(0, chunks, step, 0)

        @pl.when(outer)
        def _():
            open_compact(0)
            send_near(1, chunks - 1)
            keep(1).start()
            open_compact(1)
            send_near(2, chunks - 1)
            keep(2).start()

    spread_out = pltpu.make_async_copy(spread, spread_ref, local_sem.at[2])
    spread_out.start()
    for k in range(1, nm):
        pltpu.make_async_remote_copy(
            src_ref=anom_ref,
            dst_ref=pieces.at[k - 1],
            send_sem=m_send.at[k],
            recv_sem=m_recv.at[k],
            device_id=(tile, lax.rem(mem + k, nm)),
            device_id_type=MESH,
        ).wait()

    mean_wide[...] = mean_ref[...].astype(jnp.float32)
    weight_wide[...] = jnp.transpose(weight_ref[...].astype(jnp.float32))
    mine = weight_wide[pl.ds(mem * mem_dev, mem_dev), :].astype(jnp.bfloat16)
    for p in range(nm):
        shares[p] = mine[:, p * mem_dev : (p + 1) * mem_dev]

    def mix(first, count):
        mixture = jnp.zeros((mem_dev, count * cols), jnp.float32)
        for k in range(nm):
            held = anom_ref if k == 0 else pieces.at[k - 1]
            side = jnp.concatenate([held[first + i] for i in range(count)], axis=1)
            share = shares[lax.rem(mem + k, nm)]
            mixture = mixture + jnp.dot(share, side, preferred_element_type=jnp.float32)
        for i in range(count):
            total = mean_wide[pl.ds(first + i, 1), :] + mixture[:, i * cols : (i + 1) * cols]
            mixed[first + i] = total.astype(jnp.bfloat16)

    def mix_block(b, carry):
        mix(b * MIX_LEVELS, MIX_LEVELS)
        return carry

    full = levels // MIX_LEVELS
    lax.fori_loop(0, full, mix_block, 0)
    if levels % MIX_LEVELS:
        mix(full * MIX_LEVELS, levels % MIX_LEVELS)

    analysis_out = pltpu.make_async_copy(mixed, analysis_ref, local_sem.at[3])
    analysis_out.start()

    if tight:

        @pl.when(outer)
        def _():
            open_compact(2)
            send_near(3, chunks - 1)
            keep(3).start()

    def gone(ref, sem):
        pltpu.make_async_remote_copy(
            src_ref=ref,
            dst_ref=ref,
            send_sem=sem,
            recv_sem=a_recv.at[0],
            device_id=(ahead, mem),
            device_id_type=MESH,
        ).wait_send()

    def come(count):
        pltpu.make_async_remote_copy(
            src_ref=recv_ref.at[pl.ds(0, count)],
            dst_ref=recv_ref.at[pl.ds(0, count)],
            send_sem=p_send.at[0],
            recv_sem=a_recv.at[0],
            device_id=(ahead, mem),
            device_id_type=MESH,
        ).wait_recv()

    if not tight:
        gone(owned_ref, stream_send.at[0])
    gone(send_buf.at[OWN, pl.ds(0, zone_tiles - 1)], p_send.at[OWN])

    def line_sent():
        for block in (OUTER, PARTNER, FAR):
            gone(send_buf.at[block, pl.ds(0, zone_tiles - 1)], p_send.at[block])
            keep(block).wait()

    @pl.when(inner)
    def _():
        if tight:
            for i in (OWN, OUTER):
                gone(cross_buf.at[i], cross_send.at[i])
        else:
            gone(block_buf.at[0], stream_send.at[1])
        for block in AWAY:
            gone(away_buf.at[AWAY[block]], away_send.at[AWAY[block]])
        line_sent()

    @pl.when(outer)
    def _():
        if tight:
            gone(owned_ref, stream_send.at[0])
            line_sent()
            come(n - ZONES)
        else:
            come(n - 1)

    @pl.when(inner)
    def _():
        come(n - ZONES)

    keep(OWN).wait()
    spread_out.wait()
    analysis_out.wait()


def combine_kernel(
    n, steps, bias_ref, recv_ref, spread_ref, mixed_ref, out_ref, analysis_ref, prior, sems
):
    carry_out = pltpu.make_async_copy(mixed_ref, analysis_ref, sems.at[steps])
    slots = spread_ref.shape[0] // n
    groups = LANES // slots
    members = prior.shape[1]
    channels = prior.shape[0] // steps
    part = recv_ref.shape[1] // steps

    def move(step):
        span = pl.ds(step * channels, channels)
        return pltpu.make_async_copy(prior.at[span], out_ref.at[span], sems.at[step])

    for step in range(steps):
        rows_of = slice(step * part, (step + 1) * part)
        stacked = jnp.concatenate(
            [
                jnp.concatenate(
                    [recv_ref[s, rows_of, g * slots : (g + 1) * slots] for s in range(n)], axis=1
                )
                for g in range(groups)
            ],
            axis=0,
        )
        total = jnp.dot(stacked, spread_ref[...], preferred_element_type=jnp.float32)
        for c in range(channels):
            bias = bias_ref[step * channels + c]
            prior[step * channels + c] = total[c * members : (c + 1) * members, :] + bias
        move(step).start()
    carry_out.start()
    for step in range(steps):
        move(step).wait()
    carry_out.wait()


def chunk_count(channels, mem_dev, groups):
    def fits(count):
        part = channels * mem_dev // (count * groups)
        return channels % count == 0 and part * count * groups == channels * mem_dev and part % 16 == 0

    return next(count for count in (6, 4, 3, 2, 1) if count == 1 or fits(count))


def shards(
    n,
    nm,
    anomalies,
    analysis_weights,
    background_mean,
    background,
    jacobian_table,
    channel_list,
    send_slots,
    footprint,
    footprint_weight,
    channel_bias,
):
    mem_dev, levels, cols = anomalies.shape
    channels = channel_list.shape[0]
    slots = send_slots.shape[2]
    obs, foot = footprint.shape
    groups = LANES // slots
    rows = channels * mem_dev
    members = analysis_weights.shape[1]
    chunks = chunk_count(channels, mem_dev, groups)
    zone_tiles = n // ZONES
    vmem = pl.BlockSpec(memory_space=pltpu.VMEM)
    hbm = pl.BlockSpec(memory_space=pl.ANY)
    far = pl.BlockSpec(memory_space=pltpu.HBM)
    dma = pltpu.SemaphoreType.DMA
    chunk = rows // chunks
    select = mem_dev % 8 == 0
    foldable = chunk % (16 * FOLD) == 0

    front_out = [
        jax.ShapeDtypeStruct((ZONES, n, LANES), jnp.int32),
        jax.ShapeDtypeStruct((1, 1), jnp.float32),
    ]
    front_scratch = [
        pltpu.VMEM((1, n, LANES), jnp.int32),
        pltpu.VMEM((ZONES, n, LANES), jnp.int32),
        pltpu.VMEM((1, 1, LANES), jnp.int32),
        pltpu.VMEM((n, 1, LANES), jnp.int32),
    ]
    front_args, front_specs = [send_slots[0]], [vmem]
    if select:
        spectrum = jacobian_table.shape[0]
        front_out.insert(0, jax.ShapeDtypeStruct((rows, cols), jnp.bfloat16))
        front_scratch += [
            pltpu.VMEM((levels, spectrum), jnp.bfloat16),
            pltpu.VMEM((levels, mem_dev, cols), jnp.bfloat16),
            pltpu.VMEM((levels, mem_dev, cols), jnp.float32),
            pltpu.VMEM((-(-levels // LANES) * LANES, -(-channels // LANES) * LANES), jnp.float32),
            pltpu.VMEM((rows, cols), jnp.float32),
        ]
        front_args = [
            jnp.transpose(jacobian_table),
            channel_list[None, :],
            jnp.transpose(background, (1, 0, 2)),
            send_slots[0],
        ]
        front_specs = [far, vmem, far, vmem]
    front = pl.pallas_call(
        functools.partial(front_kernel, n, select),
        out_shape=tuple(front_out),
        in_specs=front_specs,
        out_specs=(vmem,) * (len(front_out) - 1) + (pl.BlockSpec(memory_space=pltpu.SMEM),),
        scratch_shapes=front_scratch + [dma((2,)), dma((2,)), dma((2,))],
        compiler_params=pltpu.CompilerParams(
            collective_id=0, has_side_effects=True, vmem_limit_bytes=62 * 1024 * 1024
        ),
        name="front",
    )(*front_args)
    tables, count = front[-2:]
    if select:
        owned = front[0]
    else:
        chosen = (
            jnp.arange(jacobian_table.shape[0], dtype=jnp.int32)[:, None] == channel_list[None, :]
        ).astype(jnp.bfloat16)
        selected = jnp.einsum(
            "sl,sc->cl", jacobian_table, chosen, preferred_element_type=jnp.float32
        ).astype(jnp.bfloat16)
        owned = jnp.einsum(
            "cl,klx->ckx", selected, background, preferred_element_type=jnp.float32
        ).astype(jnp.bfloat16).reshape(rows, cols)

    def rest(tight, owned, tables, anomalies, weights, mean, footprint, footprint_weight, bias):
        part = rows // groups
        pairs = zone_tiles // 2
        spare = (8, LANES)
        fold_rows, capped, widened = rows // FOLD, FOLD * CAP, FOLD * WIDE
        if tight:
            variant = [
                (3, fold_rows, capped),
                (1, rows, cols),
                (3, fold_rows, capped),
                (2, pairs, groups * cols, 2 * LANES),
                (1, FOLD * cols, capped),
                (3, zone_tiles, widened, 2 * LANES),
                (2, fold_rows, widened),
                (2, fold_rows, widened),
                (2, FOLD * cols, widened),
                (2, widened, capped),
            ]
        else:
            variant = [
                (3, zone_tiles, part, LANES),
                (3, rows, cols),
                spare,
                (4, pairs, groups * cols, 2 * LANES),
                (3, pairs, groups * cols, 2 * LANES),
            ] + [spare] * 5
        variant = [pltpu.VMEM(shape, jnp.bfloat16) for shape in variant]
        received, mixed, spread = pl.pallas_call(
            functools.partial(exchange_kernel, n, nm, chunks, tight),
            out_shape=(
                jax.ShapeDtypeStruct((n, part, LANES), jnp.bfloat16),
                jax.ShapeDtypeStruct((levels, mem_dev, cols), jnp.bfloat16),
                jax.ShapeDtypeStruct((n * slots, obs), jnp.bfloat16),
            ),
            in_specs=[vmem] * 7,
            out_specs=(hbm, hbm, hbm),
            scratch_shapes=[pltpu.VMEM((4, zone_tiles, part, LANES), jnp.bfloat16)]
            + variant
            + [
                pltpu.VMEM((max(nm - 1, 1), levels, mem_dev, cols), jnp.bfloat16),
                pltpu.VMEM((levels, mem_dev, cols), jnp.bfloat16),
                pltpu.VMEM((n * slots, obs), jnp.bfloat16),
                pltpu.VMEM((levels, cols), jnp.float32),
                pltpu.VMEM((members, members), jnp.float32),
                pltpu.VMEM((nm, mem_dev, mem_dev), jnp.bfloat16),
                dma((2,)),
                dma((3, chunks)),
                dma((nm,)),
                dma((nm,)),
                dma((4,)),
                dma((3,)),
                dma((3, chunks)),
                dma((2,)),
                dma((2, chunks)),
                dma((1,)),
                dma((8,)),
            ],
            compiler_params=pltpu.CompilerParams(
                collective_id=1 + tight, has_side_effects=True, vmem_limit_bytes=44 * 1024 * 1024
            ),
            name="exchange_tight" if tight else "exchange",
        )(owned, tables, anomalies, weights, mean, footprint, footprint_weight)
        return pl.pallas_call(
            functools.partial(combine_kernel, n, chunks),
            out_shape=(
                jax.ShapeDtypeStruct((channels, mem_dev, obs), jnp.float32),
                jax.ShapeDtypeStruct(mixed.shape, mixed.dtype),
            ),
            in_specs=[pl.BlockSpec(memory_space=pltpu.SMEM), vmem, vmem, vmem],
            out_specs=(hbm, hbm),
            scratch_shapes=[
                pltpu.VMEM((channels, mem_dev, obs), jnp.float32),
                dma((chunks + 1,)),
            ],
            compiler_params=pltpu.CompilerParams(vmem_limit_bytes=40 * 1024 * 1024),
            name="combine",
        )(bias, received, spread, mixed)

    operands = (
        owned,
        tables,
        jnp.transpose(anomalies, (1, 0, 2)),
        analysis_weights[0],
        background_mean,
        jnp.transpose(footprint),
        jnp.transpose(footprint_weight),
        channel_bias,
    )
    if foldable:
        prior, analysis = lax.cond(
            count[0, 0] <= 0,
            functools.partial(rest, True),
            functools.partial(rest, False),
            *operands,
        )
    else:
        prior, analysis = rest(False, *operands)
    return jnp.transpose(analysis, (1, 0, 2)), prior


def solution(mesh):
    placed = (
        P("mem", None, "tile"),
        P("tile", None, None),
        P(None, "tile"),
        P("mem", None, "tile"),
        P(),
        P(),
        P("tile", None, None),
        P("tile", None),
        P("tile", None),
        P(),
    )
    return jax.shard_map(
        functools.partial(shards, mesh.shape["tile"], mesh.shape["mem"]),
        mesh=mesh,
        in_specs=placed,
        out_specs=(P("mem", None, "tile"), P(None, "mem", "tile")),
        check_vma=False,
    )
```

```python
import functools

import jax
import jax.numpy as jnp
from jax import lax
from jax.experimental import pallas as pl
from jax.experimental.pallas import tpu as pltpu
from jax.sharding import PartitionSpec as P

LANES = 128
MESH = pl.DeviceIdType.MESH
ZONES = 4
MIX_LEVELS = 8

OWN, OUTER, PARTNER, FAR = range(4)
AWAY = {OWN: 0, PARTNER: 1, FAR: 2}
CAP = 80
WIDE = 112
FOLD = 8


def needed(table_ref, source, base, count, cols):
    column = lax.broadcasted_iota(jnp.int32, (cols, LANES), 0)

    def one(t, hit):
        row = table_ref[source, pl.ds(base + t, 1), :]
        return jnp.where(column == row, 1.0, hit)

    hit = lax.fori_loop(0, count, one, jnp.zeros((cols, LANES), jnp.float32))
    return jnp.max(hit, axis=1, keepdims=True)


def positions(mask, cols):
    before = lax.broadcasted_iota(jnp.int32, (cols, cols), 1) < lax.broadcasted_iota(
        jnp.int32, (cols, cols), 0
    )
    full = jnp.broadcast_to(mask, (cols, LANES)).astype(jnp.bfloat16)
    return jnp.dot(
        jnp.where(before, 1.0, 0.0).astype(jnp.bfloat16), full, preferred_element_type=jnp.float32
    )


def front_kernel(
    n,
    select,
    *refs,
):
    if select:
        (table_ref, list_ref, field_ref, slots_ref, owned_ref, tables_ref, count_ref,
         message, gathered, counted, counts, table, field, wide, chosen, radiance,
         sends, arrives, local_sem) = refs
    else:
        (slots_ref, tables_ref, count_ref, message, gathered, counted, counts,
         sends, arrives, local_sem) = refs
    tile = lax.axis_index("tile")
    mem = lax.axis_index("mem")
    slots = slots_ref.shape[1]
    groups = LANES // slots
    cols = LANES
    zone_tiles = n // ZONES
    zone = tile // zone_tiles
    barrier = pltpu.get_barrier_semaphore()

    def greet(k, carry):
        pl.semaphore_signal(
            barrier, inc=1, device_id=(lax.rem(tile + k, n), mem), device_id_type=MESH
        )
        return carry

    lax.fori_loop(1, n, greet, 0)
    if select:
        load_table = pltpu.make_async_copy(table_ref, table, local_sem.at[0])
        load_table.start()
        load_field = pltpu.make_async_copy(field_ref, field, local_sem.at[1])
        load_field.start()

    message[0] = jnp.concatenate([slots_ref[...]] * groups, axis=1)
    most = jnp.zeros((1, 1), jnp.float32)
    for far in (0, ZONES - 1):
        mask = needed(message, 0, far * zone_tiles, zone_tiles, cols)
        total = jnp.sum(mask, axis=0, keepdims=True)
        most = jnp.maximum(most, jnp.where(zone == far, 0.0, total - CAP))
    across = needed(message, 0, (1 - zone // 2) * (n // 2), n // 2, cols)
    most = jnp.maximum(most, jnp.sum(across, axis=0, keepdims=True) - WIDE)
    counted[0] = jnp.broadcast_to(most, (1, LANES)).astype(jnp.int32)
    pl.semaphore_wait(barrier, n - 1)

    def tell(k, carry):
        pltpu.make_async_remote_copy(
            src_ref=counted.at[0],
            dst_ref=counts.at[tile],
            send_sem=sends.at[0],
            recv_sem=arrives.at[0],
            device_id=(lax.rem(tile + k, n), mem),
            device_id_type=MESH,
        ).start()
        return carry

    lax.fori_loop(1, n, tell, 0)
    for k in range(1, ZONES):
        pltpu.make_async_remote_copy(
            src_ref=message.at[0],
            dst_ref=gathered.at[zone],
            send_sem=sends.at[1],
            recv_sem=arrives.at[1],
            device_id=(lax.rem(tile + k * zone_tiles, n), mem),
            device_id_type=MESH,
        ).start()

    if select:
        spectrum = table_ref.shape[1]
        levels, mem_dev = field_ref.shape[0], field_ref.shape[1]
        channels = list_ref.shape[1]
        load_field.wait()
        wide[...] = field[...].astype(jnp.float32)
        load_table.wait()
        block = 11 * LANES
        total = jnp.zeros((levels, channels), jnp.float32)
        for first in range(0, spectrum, block):
            size = min(block, spectrum - first)
            entry = lax.broadcasted_iota(jnp.int32, (size, channels), 0) + first
            pick = jnp.where(entry == list_ref[...], 1.0, 0.0).astype(jnp.bfloat16)
            total = total + jnp.dot(
                table[:, first : first + size], pick, preferred_element_type=jnp.float32
            )
        chosen[...] = jnp.zeros_like(chosen)
        chosen[0:levels, 0:channels] = total
        picked = jnp.transpose(chosen[...])[:channels, :levels].astype(jnp.bfloat16)
        flat = wide.reshape(levels * mem_dev, cols)

        def member(k, carry):
            profile = flat[pl.ds(k, levels, stride=mem_dev), :].astype(jnp.bfloat16)
            radiance[pl.ds(k, channels, stride=mem_dev), :] = jnp.dot(
                picked, profile, preferred_element_type=jnp.float32
            )
            return carry

        lax.fori_loop(0, mem_dev, member, 0, unroll=8)
        owned_ref[...] = radiance[...].astype(jnp.bfloat16)

    counts[tile] = counted[0]
    gathered[zone] = message[0]

    def everyone(ref, count, kind):
        span = ref.at[pl.ds(0, count)]
        return pltpu.make_async_remote_copy(
            src_ref=span,
            dst_ref=span,
            send_sem=sends.at[kind],
            recv_sem=arrives.at[kind],
            device_id=(lax.rem(tile + 1, n), mem),
            device_id_type=MESH,
        )

    everyone(gathered, ZONES - 1, 1).wait_recv()
    tables_ref[...] = gathered[...]
    everyone(counts, n - 1, 0).wait_recv()

    def highest(s, top):
        return jnp.maximum(top, counts[s])

    top = lax.fori_loop(0, n, highest, jnp.zeros((1, LANES), jnp.int32))
    count_ref[0, 0] = jnp.max(top.astype(jnp.float32))
    everyone(counts, n - 1, 0).wait_send()
    everyone(gathered, ZONES - 1, 1).wait_send()


def exchange_kernel(
    n,
    nm,
    chunks,
    tight,
    owned_ref,
    tables_ref,
    anom_ref,
    weight_ref,
    mean_ref,
    foot_ref,
    fweight_ref,
    recv_ref,
    analysis_ref,
    spread_ref,
    send_buf,
    away_buf,
    block_buf,
    compact_buf,
    picks,
    away_picks,
    open_picks,
    cross_buf,
    cross_in,
    cross_picks,
    narrow_picks,
    pieces,
    mixed,
    spread,
    mean_wide,
    weight_wide,
    shares,
    stream_send,
    stream_recv,
    m_send,
    m_recv,
    p_send,
    away_send,
    away_recv,
    cross_send,
    cross_recv,
    a_recv,
    local_sem,
):
    tile = lax.axis_index("tile")
    mem = lax.axis_index("mem")
    rows, cols = owned_ref.shape
    slots = spread_ref.shape[0] // n
    groups = LANES // slots
    obs = foot_ref.shape[1]
    levels, mem_dev = anom_ref.shape[0], anom_ref.shape[1]
    zone_tiles = n // ZONES
    pairs = zone_tiles // 2
    chunk = rows // chunks
    part = chunk // groups

    zone = tile // zone_tiles
    place = lax.rem(tile, zone_tiles)
    sign = 1 - 2 * (zone // 2)
    inner = jnp.logical_or(zone == 1, zone == 2)
    outer = jnp.logical_not(inner)
    stride = sign * zone_tiles
    ahead = lax.rem(tile + stride + n, n)

    def along(steps):
        return lax.rem(tile + steps * stride + ZONES * n, n)

    if tight:
        source = (tile, along(jnp.where(inner, -1, 1)), along(jnp.where(inner, 1, 2)),
                  along(jnp.where(inner, 2, 3)))
    else:
        source = (tile, along(-1), along(1), along(2))
    zone_base = zone * zone_tiles
    away_base = lax.rem(zone_base - stride + n, n)

    barrier = pltpu.get_barrier_semaphore()

    def greet(k, carry):
        pl.semaphore_signal(
            barrier,
            inc=1,
            device_id=(zone_base + lax.rem(place + k, zone_tiles), mem),
            device_id_type=MESH,
        )
        return carry

    lax.fori_loop(1, zone_tiles, greet, 0)
    for side in (-1, 1):

        @pl.when(jnp.logical_and(zone + side >= 0, zone + side < ZONES))
        def _():
            def greet_side(t, carry):
                pl.semaphore_signal(
                    barrier,
                    inc=1,
                    device_id=(zone_base + side * zone_tiles + t, mem),
                    device_id_type=MESH,
                )
                return carry

            lax.fori_loop(0, zone_tiles, greet_side, 0)

    for k in range(1, nm):
        pl.semaphore_signal(
            barrier, inc=1, device_id=(tile, lax.rem(mem + k, nm)), device_id_type=MESH
        )

    lane_group = lax.broadcasted_iota(jnp.int32, (1, LANES), 1) // slots

    def build(origin, base, into, first_pick):
        row_id = lax.broadcasted_iota(jnp.int32, (groups * cols, 2 * LANES), 0)

        def want(t):
            row = tables_ref[origin // zone_tiles, pl.ds(base + t, 1), :]
            return jnp.maximum(row, 0) + lane_group * cols

        def pair(h, carry):
            wants = jnp.concatenate([want(2 * h), want(2 * h + 1)], axis=1)
            into[first_pick, h] = jnp.where(row_id == wants, 1.0, 0.0).astype(jnp.bfloat16)
            return carry

        lax.fori_loop(0, pairs, pair, 0)

    def build_near(block):
        build(source[block], zone_base, picks, block)

    half = n // 2
    half_base = (zone // 2) * half
    other_base = half - half_base

    def fold_columns(mask, cap, g):
        place_of = positions(mask, cols)[:, 0:1].astype(jnp.int32) + g * cap
        place_of = jnp.where(mask > 0.0, place_of, -1)
        lane = lax.broadcasted_iota(jnp.int32, (cols, FOLD * cap), 1)
        return jnp.where(lane == place_of, 1.0, 0.0).astype(jnp.bfloat16)

    def build_fold(into, origin, base, count, cap):
        mask = needed(tables_ref, origin // zone_tiles, base, count, cols)
        for g in range(FOLD):
            into[g * cols : (g + 1) * cols, :] = fold_columns(mask, cap, g)

    def build_away(block):
        if tight:
            build_fold(away_picks.at[AWAY[block]], source[block], away_base, zone_tiles, CAP)
        else:
            build(source[block], away_base, away_picks, AWAY[block])

    def build_cross(i):
        build_fold(cross_picks.at[i], source[i], other_base, half, WIDE)

    def build_narrow(block):
        line = source[block] // zone_tiles
        wide_mask = needed(tables_ref, line, half_base, half, cols)
        wide_place = jnp.where(wide_mask > 0.0, positions(wide_mask, cols), -1.0)
        wide_place = jnp.transpose(wide_place)[0:1, :].astype(jnp.int32)
        row_id = lax.broadcasted_iota(jnp.int32, (WIDE, cols), 0)
        back = jnp.where(row_id == wide_place, 1.0, 0.0).astype(jnp.bfloat16)
        mask = needed(tables_ref, line, away_base, zone_tiles, cols)
        for g in range(FOLD):
            narrow_picks[block - PARTNER, g * WIDE : (g + 1) * WIDE, :] = jnp.dot(
                back, fold_columns(mask, CAP, g), preferred_element_type=jnp.float32
            ).astype(jnp.bfloat16)

    def build_open(i, origin, base, count, cap):
        line = origin // zone_tiles
        mask = needed(tables_ref, line, base, count, cols)
        column = lax.broadcasted_iota(jnp.int32, (cols, LANES), 0)
        row_id = lax.broadcasted_iota(jnp.int32, (FOLD * cap, 2 * LANES), 0)

        def one(t, carry):
            row = tables_ref[line, pl.ds(zone_base + t, 1), :]
            ahead_of = jnp.where(column < row, mask, 0.0)
            spot = jnp.sum(ahead_of, axis=0, keepdims=True).astype(jnp.int32)
            wants = jnp.concatenate(
                [spot + (2 * lane_group + v) * cap for v in range(2)], axis=1
            )
            open_picks[i, t, 0 : FOLD * cap] = jnp.where(row_id == wants, 1.0, 0.0).astype(
                jnp.bfloat16
            )
            return carry

        lax.fori_loop(0, zone_tiles, one, 0)

    @pl.when(inner)
    def _():
        if tight:
            build_cross(OWN)
        build_away(OWN)

    build_near(OWN)

    greeted = zone_tiles - 1 + nm - 1 + jnp.where(inner, 2, 1) * zone_tiles
    pl.semaphore_wait(barrier, greeted)

    def span(c):
        return pl.ds(pl.multiple_of(c * chunk, chunk), chunk)

    def narrow(c):
        return pl.ds(pl.multiple_of(c * part, part), part)

    landing = 0 if tight else jnp.where(inner, 1, 0)

    def own_stream(c):
        return pltpu.make_async_remote_copy(
            src_ref=owned_ref.at[span(c)],
            dst_ref=block_buf.at[landing, span(c)],
            send_sem=stream_send.at[0],
            recv_sem=stream_recv.at[landing, c],
            device_id=(ahead, mem),
            device_id_type=MESH,
        )

    def forward_stream(c):
        return pltpu.make_async_remote_copy(
            src_ref=block_buf.at[0, span(c)],
            dst_ref=block_buf.at[2, span(c)],
            send_sem=stream_send.at[1],
            recv_sem=stream_recv.at[2, c],
            device_id=(ahead, mem),
            device_id_type=MESH,
        )

    def stream_arrival(block, c):
        return pltpu.make_async_remote_copy(
            src_ref=owned_ref.at[span(c)],
            dst_ref=block_buf.at[block - 1, span(c)],
            send_sem=stream_send.at[0],
            recv_sem=stream_recv.at[block - 1, c],
            device_id=(ahead, mem),
            device_id_type=MESH,
        )

    def member_copy(k):
        peer = lax.rem(mem + k, nm)
        return pltpu.make_async_remote_copy(
            src_ref=anom_ref,
            dst_ref=pieces.at[nm - 1 - k],
            send_sem=m_send.at[k],
            recv_sem=m_recv.at[nm - k],
            device_id=(tile, peer),
            device_id_type=MESH,
        )

    def parcel(block, t, rows_of):
        return pltpu.make_async_remote_copy(
            src_ref=send_buf.at[block, t, rows_of],
            dst_ref=recv_ref.at[source[block], rows_of],
            send_sem=p_send.at[block],
            recv_sem=a_recv.at[0],
            device_id=(zone_base + t, mem),
            device_id_type=MESH,
        )

    def away_parcel(block, t, rows_of):
        return pltpu.make_async_remote_copy(
            src_ref=away_buf.at[AWAY[block], t, rows_of],
            dst_ref=recv_ref.at[source[block], rows_of],
            send_sem=away_send.at[AWAY[block]],
            recv_sem=a_recv.at[0],
            device_id=(away_base + t, mem),
            device_id_type=MESH,
        )

    fold_part = chunk // FOLD

    def folded(c):
        return pl.ds(pl.multiple_of(c * fold_part, fold_part), fold_part)

    def compact(i, c):
        return pltpu.make_async_remote_copy(
            src_ref=away_buf.at[i, folded(c)],
            dst_ref=compact_buf.at[i, folded(c)],
            send_sem=away_send.at[i],
            recv_sem=away_recv.at[i, c],
            device_id=(along(-1), mem),
            device_id_type=MESH,
        )

    def cross(i, c):
        return pltpu.make_async_remote_copy(
            src_ref=cross_buf.at[i, folded(c)],
            dst_ref=cross_in.at[i, folded(c)],
            send_sem=cross_send.at[i],
            recv_sem=cross_recv.at[i, c],
            device_id=(ahead, mem),
            device_id_type=MESH,
        )

    def spread_out_rows(block, c, count, size):
        block_ref = owned_ref if block == OWN else block_buf.at[block - 1]
        return jnp.concatenate(
            [
                block_ref[pl.ds(pl.multiple_of(c * chunk + g * size, size), size), :]
                for g in range(count)
            ],
            axis=1,
        )

    def pack(block, c, pick_ref, pick, out_ref):
        wide = spread_out_rows(block, c, groups, part)

        def pair(h, carry):
            out = jnp.dot(wide, pick_ref[pick, h], preferred_element_type=jnp.float32)
            out = out.astype(jnp.bfloat16)
            out_ref[pick, 2 * h, narrow(c)] = out[:, :LANES]
            out_ref[pick, 2 * h + 1, narrow(c)] = out[:, LANES:]
            return carry

        lax.fori_loop(0, pairs, pair, 0, unroll=pairs <= 2)

    def pack_near(block, c):
        pack(block, c, picks, block, send_buf)

    def pack_cross(i, c):
        wide = spread_out_rows(i, c, FOLD, fold_part)
        out = jnp.dot(wide, cross_picks[i], preferred_element_type=jnp.float32)
        cross_buf[i, folded(c)] = out.astype(jnp.bfloat16)

    def pack_away(block, c):
        if not tight:
            pack(block, c, away_picks, AWAY[block], away_buf)
            return
        if block == OWN:
            wide, pick = spread_out_rows(OWN, c, FOLD, fold_part), away_picks[AWAY[OWN]]
        else:
            i = block - PARTNER
            wide, pick = cross_in[i, folded(c)], narrow_picks[i]
        out = jnp.dot(wide, pick, preferred_element_type=jnp.float32)
        away_buf[AWAY[block], folded(c)] = out.astype(jnp.bfloat16)

    def unpack(held, i, cap, c):
        def one(t, carry):
            out = jnp.dot(
                held, open_picks[i, t, 0 : FOLD * cap], preferred_element_type=jnp.float32
            )
            out = out.astype(jnp.bfloat16)
            for v in range(2):
                rows_of = pl.ds(
                    pl.multiple_of(c * part + v * fold_part, fold_part), fold_part
                )
                send_buf[1 + i, t, rows_of] = out[:, v * LANES : (v + 1) * LANES]
            return carry

        lax.fori_loop(0, zone_tiles, one, 0, unroll=zone_tiles <= 4)

    def send_near(block, c):
        def one(t, carry):
            @pl.when(zone_base + t != tile)
            def _():
                parcel(block, t, narrow(c)).start()

            return carry

        lax.fori_loop(0, zone_tiles, one, 0)

    def send_away(block, c):
        if tight:
            compact(AWAY[block], c).start()
            return

        def one(t, carry):
            away_parcel(block, t, narrow(c)).start()
            return carry

        lax.fori_loop(0, zone_tiles, one, 0)

    def keep(block):
        return pltpu.make_async_copy(
            send_buf.at[block, place], recv_ref.at[source[block]], local_sem.at[4 + block]
        )

    for k in range(1, nm):
        member_copy(k).start()

    def start_own(c, carry):
        own_stream(c).start()
        return carry

    if tight:

        @pl.when(outer)
        def _():
            lax.fori_loop(0, chunks, start_own, 0)
    else:
        lax.fori_loop(0, chunks, start_own, 0)

    def later(block, c):
        @pl.when(c > 0)
        def _():
            send_near(block, c - 1)

    @pl.when(inner)
    def _():
        def own_step(c, carry):
            if tight:
                pack_cross(OWN, c)
            pack_away(OWN, c)
            if tight:
                cross(OWN, c).start()
            pack_near(OWN, c)
            send_away(OWN, c)
            later(OWN, c)
            return carry

        lax.fori_loop(0, chunks, own_step, 0)

    @pl.when(outer)
    def _():
        def own_step(c, carry):
            pack_near(OWN, c)
            later(OWN, c)
            return carry

        lax.fori_loop(0, chunks, own_step, 0)

    @pl.when(inner)
    def _():
        if tight:
            build_cross(OUTER)
            build_narrow(PARTNER)
            build_open(PARTNER - 1, source[PARTNER], half_base, half, WIDE)
        else:
            build_away(PARTNER)
            build_near(PARTNER)
        build_near(OUTER)

    send_near(OWN, chunks - 1)
    keep(OWN).start()

    @pl.when(inner)
    def _():
        def mid_step(c, carry):
            stream_arrival(OUTER, c).wait_recv()
            if tight:
                pack_cross(OUTER, c)
                cross(PARTNER - PARTNER, c).wait_recv()
                pack_away(PARTNER, c)
                cross(OUTER, c).start()
                unpack(cross_in[0, folded(c)], PARTNER - 1, WIDE, c)
            else:
                forward_stream(c).start()
                stream_arrival(PARTNER, c).wait_recv()
                pack_away(PARTNER, c)
                pack_near(PARTNER, c)
            send_away(PARTNER, c)
            pack_near(OUTER, c)
            send_near(PARTNER, c)
            later(OUTER, c)
            return carry

        lax.fori_loop(0, chunks, mid_step, 0)
        if tight:
            build_narrow(FAR)
            build_open(FAR - 1, source[FAR], half_base, half, WIDE)
        else:
            build_away(FAR)
            build_near(FAR)
        send_near(OUTER, chunks - 1)
        keep(OUTER).start()
        keep(PARTNER).start()

        def far_step(c, carry):
            if tight:
                cross(FAR - PARTNER, c).wait_recv()
                pack_away(FAR, c)
                unpack(cross_in[1, folded(c)], FAR - 1, WIDE, c)
            else:
                stream_arrival(FAR, c).wait_recv()
                pack_away(FAR, c)
                pack_near(FAR, c)
            send_away(FAR, c)
            later(FAR, c)
            return carry

        lax.fori_loop(0, chunks, far_step, 0)

    fweight = fweight_ref[...].astype(jnp.float32)

    def spread_rows(s, carry):
        ids = lax.broadcasted_iota(jnp.int32, (slots, obs), 0) + s * slots
        total = jnp.zeros((slots, obs), jnp.float32)
        for j in range(foot_ref.shape[0]):
            total = total + jnp.where(
                ids == foot_ref[j : j + 1, :], fweight[j : j + 1, :], 0.0
            )
        spread[pl.ds(pl.multiple_of(s * slots, slots), slots), :] = total.astype(jnp.bfloat16)
        return carry

    if tight:

        @pl.when(outer)
        def _():
            for i in range(3):
                build_open(i, source[1 + i], zone_base, zone_tiles, CAP)

    lax.fori_loop(0, n, spread_rows, 0)

    @pl.when(inner)
    def _():
        send_near(FAR, chunks - 1)
        keep(FAR).start()

    spread_out = pltpu.make_async_copy(spread, spread_ref, local_sem.at[2])
    spread_out.start()
    mean_wide[...] = mean_ref[...].astype(jnp.float32)
    weight_wide[...] = jnp.transpose(weight_ref[...].astype(jnp.float32))
    mine = weight_wide[pl.ds(mem * mem_dev, mem_dev), :].astype(jnp.bfloat16)
    for p in range(nm):
        shares[p] = mine[:, p * mem_dev : (p + 1) * mem_dev]

    def members_here():
        for k in range(1, nm):
            pltpu.make_async_remote_copy(
                src_ref=anom_ref,
                dst_ref=pieces.at[k - 1],
                send_sem=m_send.at[k],
                recv_sem=m_recv.at[k],
                device_id=(tile, lax.rem(mem + k, nm)),
                device_id_type=MESH,
            ).wait()

    def mix(first, count):
        mixture = jnp.zeros((mem_dev, count * cols), jnp.float32)
        for k in range(nm):
            held = anom_ref if k == 0 else pieces.at[k - 1]
            side = jnp.concatenate([held[first + i] for i in range(count)], axis=1)
            share = shares[lax.rem(mem + k, nm)]
            mixture = mixture + jnp.dot(share, side, preferred_element_type=jnp.float32)
        for i in range(count):
            total = mean_wide[pl.ds(first + i, 1), :] + mixture[:, i * cols : (i + 1) * cols]
            mixed[first + i] = total.astype(jnp.bfloat16)

    def mix_block(b, carry):
        mix(b * MIX_LEVELS, MIX_LEVELS)
        return carry

    full = levels // MIX_LEVELS
    per = -(-full // chunks)

    def mix_share(c):
        lax.fori_loop(c * per, jnp.minimum((c + 1) * per, full), mix_block, 0)

    def mix_step(c, carry):
        mix_share(c)
        return carry

    if tight:

        def open_compact(i, mixing):
            def step(c, carry):
                compact(i, c).wait_recv()
                unpack(compact_buf[i, folded(c)], i, CAP, c)
                later(1 + i, c)
                if mixing:
                    mix_share(c)
                return carry

            lax.fori_loop(0, chunks, step, 0)
            send_near(1 + i, chunks - 1)
            keep(1 + i).start()

        @pl.when(outer)
        def _():
            open_compact(0, False)
            open_compact(1, False)
            members_here()
            open_compact(2, True)

        @pl.when(inner)
        def _():
            members_here()
            lax.fori_loop(0, chunks, mix_step, 0)

    else:
        members_here()
        lax.fori_loop(0, chunks, mix_step, 0)

    if levels % MIX_LEVELS:
        mix(full * MIX_LEVELS, levels % MIX_LEVELS)

    analysis_out = pltpu.make_async_copy(mixed, analysis_ref, local_sem.at[3])
    analysis_out.start()

    def gone(ref, sem):
        pltpu.make_async_remote_copy(
            src_ref=ref,
            dst_ref=ref,
            send_sem=sem,
            recv_sem=a_recv.at[0],
            device_id=(ahead, mem),
            device_id_type=MESH,
        ).wait_send()

    def come(count):
        pltpu.make_async_remote_copy(
            src_ref=recv_ref.at[pl.ds(0, count)],
            dst_ref=recv_ref.at[pl.ds(0, count)],
            send_sem=p_send.at[0],
            recv_sem=a_recv.at[0],
            device_id=(ahead, mem),
            device_id_type=MESH,
        ).wait_recv()

    if not tight:
        gone(owned_ref, stream_send.at[0])
    gone(send_buf.at[OWN, pl.ds(0, zone_tiles - 1)], p_send.at[OWN])

    def line_sent():
        for block in (OUTER, PARTNER, FAR):
            gone(send_buf.at[block, pl.ds(0, zone_tiles - 1)], p_send.at[block])
            keep(block).wait()

    @pl.when(inner)
    def _():
        if tight:
            for i in (OWN, OUTER):
                gone(cross_buf.at[i], cross_send.at[i])
        else:
            gone(block_buf.at[0], stream_send.at[1])
        for block in AWAY:
            gone(away_buf.at[AWAY[block]], away_send.at[AWAY[block]])
        line_sent()

    @pl.when(outer)
    def _():
        if tight:
            gone(owned_ref, stream_send.at[0])
            line_sent()
            come(n - ZONES)
        else:
            come(n - 1)

    @pl.when(inner)
    def _():
        come(n - ZONES)

    keep(OWN).wait()
    spread_out.wait()
    analysis_out.wait()


def combine_kernel(
    n, steps, bias_ref, recv_ref, spread_ref, mixed_ref, out_ref, analysis_ref, prior, sems
):
    carry_out = pltpu.make_async_copy(mixed_ref, analysis_ref, sems.at[steps])
    slots = spread_ref.shape[0] // n
    groups = LANES // slots
    members = prior.shape[1]
    channels = prior.shape[0] // steps
    part = recv_ref.shape[1] // steps

    def move(step):
        span = pl.ds(step * channels, channels)
        return pltpu.make_async_copy(prior.at[span], out_ref.at[span], sems.at[step])

    carry_out.start()
    for step in range(steps):
        rows_of = slice(step * part, (step + 1) * part)
        stacked = jnp.concatenate(
            [
                jnp.concatenate(
                    [recv_ref[s, rows_of, g * slots : (g + 1) * slots] for s in range(n)], axis=1
                )
                for g in range(groups)
            ],
            axis=0,
        )
        total = jnp.dot(stacked, spread_ref[...], preferred_element_type=jnp.float32)
        for c in range(channels):
            bias = bias_ref[step * channels + c]
            prior[step * channels + c] = total[c * members : (c + 1) * members, :] + bias
        move(step).start()
    for step in range(steps):
        move(step).wait()
    carry_out.wait()


def chunk_count(channels, mem_dev, groups):
    def fits(count):
        part = channels * mem_dev // (count * groups)
        return channels % count == 0 and part * count * groups == channels * mem_dev and part % 16 == 0

    return next(count for count in (6, 4, 3, 2, 1) if count == 1 or fits(count))


def shards(
    n,
    nm,
    anomalies,
    analysis_weights,
    background_mean,
    background,
    jacobian_table,
    channel_list,
    send_slots,
    footprint,
    footprint_weight,
    channel_bias,
):
    mem_dev, levels, cols = anomalies.shape
    channels = channel_list.shape[0]
    slots = send_slots.shape[2]
    obs, foot = footprint.shape
    groups = LANES // slots
    rows = channels * mem_dev
    members = analysis_weights.shape[1]
    chunks = chunk_count(channels, mem_dev, groups)
    zone_tiles = n // ZONES
    vmem = pl.BlockSpec(memory_space=pltpu.VMEM)
    hbm = pl.BlockSpec(memory_space=pl.ANY)
    far = pl.BlockSpec(memory_space=pltpu.HBM)
    dma = pltpu.SemaphoreType.DMA
    chunk = rows // chunks
    select = mem_dev % 8 == 0
    foldable = chunk % (16 * FOLD) == 0

    front_out = [
        jax.ShapeDtypeStruct((ZONES, n, LANES), jnp.int32),
        jax.ShapeDtypeStruct((1, 1), jnp.float32),
    ]
    front_scratch = [
        pltpu.VMEM((1, n, LANES), jnp.int32),
        pltpu.VMEM((ZONES, n, LANES), jnp.int32),
        pltpu.VMEM((1, 1, LANES), jnp.int32),
        pltpu.VMEM((n, 1, LANES), jnp.int32),
    ]
    front_args, front_specs = [send_slots[0]], [vmem]
    if select:
        spectrum = jacobian_table.shape[0]
        front_out.insert(0, jax.ShapeDtypeStruct((rows, cols), jnp.bfloat16))
        front_scratch += [
            pltpu.VMEM((levels, spectrum), jnp.bfloat16),
            pltpu.VMEM((levels, mem_dev, cols), jnp.bfloat16),
            pltpu.VMEM((levels, mem_dev, cols), jnp.float32),
            pltpu.VMEM((-(-levels // LANES) * LANES, -(-channels // LANES) * LANES), jnp.float32),
            pltpu.VMEM((rows, cols), jnp.float32),
        ]
        front_args = [
            jnp.transpose(jacobian_table),
            channel_list[None, :],
            jnp.transpose(background, (1, 0, 2)),
            send_slots[0],
        ]
        front_specs = [far, vmem, far, vmem]
    front = pl.pallas_call(
        functools.partial(front_kernel, n, select),
        out_shape=tuple(front_out),
        in_specs=front_specs,
        out_specs=(vmem,) * (len(front_out) - 1) + (pl.BlockSpec(memory_space=pltpu.SMEM),),
        scratch_shapes=front_scratch + [dma((2,)), dma((2,)), dma((2,))],
        compiler_params=pltpu.CompilerParams(
            collective_id=0, has_side_effects=True, vmem_limit_bytes=58 * 1024 * 1024
        ),
        name="front",
    )(*front_args)
    tables, count = front[-2:]
    if select:
        owned = front[0]
    else:
        chosen = (
            jnp.arange(jacobian_table.shape[0], dtype=jnp.int32)[:, None] == channel_list[None, :]
        ).astype(jnp.bfloat16)
        selected = jnp.einsum(
            "sl,sc->cl", jacobian_table, chosen, preferred_element_type=jnp.float32
        ).astype(jnp.bfloat16)
        owned = jnp.einsum(
            "cl,klx->ckx", selected, background, preferred_element_type=jnp.float32
        ).astype(jnp.bfloat16).reshape(rows, cols)

    def rest(tight, owned, tables, anomalies, weights, mean, footprint, footprint_weight, bias):
        part = rows // groups
        pairs = zone_tiles // 2
        spare = (8, LANES)
        fold_rows, capped, widened = rows // FOLD, FOLD * CAP, FOLD * WIDE
        if tight:
            variant = [
                (3, fold_rows, capped),
                (1, rows, cols),
                (3, fold_rows, capped),
                (2, pairs, groups * cols, 2 * LANES),
                (1, FOLD * cols, capped),
                (3, zone_tiles, widened, 2 * LANES),
                (2, fold_rows, widened),
                (2, fold_rows, widened),
                (2, FOLD * cols, widened),
                (2, widened, capped),
            ]
        else:
            variant = [
                (3, zone_tiles, part, LANES),
                (3, rows, cols),
                spare,
                (4, pairs, groups * cols, 2 * LANES),
                (3, pairs, groups * cols, 2 * LANES),
            ] + [spare] * 5
        variant = [pltpu.VMEM(shape, jnp.bfloat16) for shape in variant]
        received, mixed, spread = pl.pallas_call(
            functools.partial(exchange_kernel, n, nm, chunks, tight),
            out_shape=(
                jax.ShapeDtypeStruct((n, part, LANES), jnp.bfloat16),
                jax.ShapeDtypeStruct((levels, mem_dev, cols), jnp.bfloat16),
                jax.ShapeDtypeStruct((n * slots, obs), jnp.bfloat16),
            ),
            in_specs=[vmem] * 7,
            out_specs=(hbm, hbm, hbm),
            scratch_shapes=[pltpu.VMEM((4, zone_tiles, part, LANES), jnp.bfloat16)]
            + variant
            + [
                pltpu.VMEM((max(nm - 1, 1), levels, mem_dev, cols), jnp.bfloat16),
                pltpu.VMEM((levels, mem_dev, cols), jnp.bfloat16),
                pltpu.VMEM((n * slots, obs), jnp.bfloat16),
                pltpu.VMEM((levels, cols), jnp.float32),
                pltpu.VMEM((members, members), jnp.float32),
                pltpu.VMEM((nm, mem_dev, mem_dev), jnp.bfloat16),
                dma((2,)),
                dma((3, chunks)),
                dma((nm,)),
                dma((nm,)),
                dma((4,)),
                dma((3,)),
                dma((3, chunks)),
                dma((2,)),
                dma((2, chunks)),
                dma((1,)),
                dma((8,)),
            ],
            compiler_params=pltpu.CompilerParams(
                collective_id=1 + tight, has_side_effects=True, vmem_limit_bytes=44 * 1024 * 1024
            ),
            name="exchange_tight" if tight else "exchange",
        )(owned, tables, anomalies, weights, mean, footprint, footprint_weight)
        return pl.pallas_call(
            functools.partial(combine_kernel, n, chunks),
            out_shape=(
                jax.ShapeDtypeStruct((channels, mem_dev, obs), jnp.float32),
                jax.ShapeDtypeStruct(mixed.shape, mixed.dtype),
            ),
            in_specs=[pl.BlockSpec(memory_space=pltpu.SMEM), vmem, vmem, vmem],
            out_specs=(hbm, hbm),
            scratch_shapes=[
                pltpu.VMEM((channels, mem_dev, obs), jnp.float32),
                dma((chunks + 1,)),
            ],
            compiler_params=pltpu.CompilerParams(vmem_limit_bytes=40 * 1024 * 1024),
            name="combine",
        )(bias, received, spread, mixed)

    operands = (
        owned,
        tables,
        jnp.transpose(anomalies, (1, 0, 2)),
        analysis_weights[0],
        background_mean,
        jnp.transpose(footprint),
        jnp.transpose(footprint_weight),
        channel_bias,
    )
    if foldable:
        prior, analysis = lax.cond(
            count[0, 0] <= 0,
            functools.partial(rest, True),
            functools.partial(rest, False),
            *operands,
        )
    else:
        prior, analysis = rest(False, *operands)
    return jnp.transpose(analysis, (1, 0, 2)), prior


def solution(mesh):
    placed = (
        P("mem", None, "tile"),
        P("tile", None, None),
        P(None, "tile"),
        P("mem", None, "tile"),
        P(),
        P(),
        P("tile", None, None),
        P("tile", None),
        P("tile", None),
        P(),
    )
    return jax.shard_map(
        functools.partial(shards, mesh.shape["tile"], mesh.shape["mem"]),
        mesh=mesh,
        in_specs=placed,
        out_specs=(P("mem", None, "tile"), P(None, "mem", "tile")),
        check_vma=False,
    )
```

```python
import functools

import jax
import jax.numpy as jnp
from jax import lax
from jax.experimental import pallas as pl
from jax.experimental.pallas import tpu as pltpu
from jax.sharding import PartitionSpec as P

LANES = 128
MESH = pl.DeviceIdType.MESH
ZONES = 4
MIX_LEVELS = 8

OWN, OUTER, PARTNER, FAR = range(4)
AWAY = {OWN: 0, PARTNER: 1, FAR: 2}
CAPS = ((64, 96), (80, 112))
FOLD = 8


def needed(table_ref, source, base, count, cols):
    column = lax.broadcasted_iota(jnp.int32, (cols, LANES), 0)

    def one(t, hit):
        row = table_ref[source, pl.ds(base + t, 1), :]
        return jnp.where(column == row, 1.0, hit)

    hit = lax.fori_loop(0, count, one, jnp.zeros((cols, LANES), jnp.float32))
    return jnp.max(hit, axis=1, keepdims=True)


def positions(mask, cols):
    before = lax.broadcasted_iota(jnp.int32, (cols, cols), 1) < lax.broadcasted_iota(
        jnp.int32, (cols, cols), 0
    )
    full = jnp.broadcast_to(mask, (cols, LANES)).astype(jnp.bfloat16)
    return jnp.dot(
        jnp.where(before, 1.0, 0.0).astype(jnp.bfloat16), full, preferred_element_type=jnp.float32
    )


def front_kernel(
    n,
    select,
    *refs,
):
    if select:
        (table_ref, list_ref, field_ref, slots_ref, owned_ref, tables_ref, count_ref,
         message, gathered, counted, counts, table, field, wide, chosen, radiance,
         sends, arrives, local_sem) = refs
    else:
        (slots_ref, tables_ref, count_ref, message, gathered, counted, counts,
         sends, arrives, local_sem) = refs
    tile = lax.axis_index("tile")
    mem = lax.axis_index("mem")
    slots = slots_ref.shape[1]
    groups = LANES // slots
    cols = LANES
    zone_tiles = n // ZONES
    zone = tile // zone_tiles
    barrier = pltpu.get_barrier_semaphore()

    def greet(k, carry):
        pl.semaphore_signal(
            barrier, inc=1, device_id=(lax.rem(tile + k, n), mem), device_id_type=MESH
        )
        return carry

    lax.fori_loop(1, n, greet, 0)
    if select:
        load_table = pltpu.make_async_copy(table_ref, table, local_sem.at[0])
        load_table.start()
        load_field = pltpu.make_async_copy(field_ref, field, local_sem.at[1])
        load_field.start()

    message[0] = jnp.concatenate([slots_ref[...]] * groups, axis=1)
    most = jnp.zeros((1, 1), jnp.float32)
    for far in (0, ZONES - 1):
        mask = needed(message, 0, far * zone_tiles, zone_tiles, cols)
        total = jnp.sum(mask, axis=0, keepdims=True)
        most = jnp.maximum(most, jnp.where(zone == far, 0.0, total))
    across = needed(message, 0, (1 - zone // 2) * (n // 2), n // 2, cols)
    across = jnp.sum(across, axis=0, keepdims=True)
    level = jnp.zeros((1, 1), jnp.float32)
    for zone_cap, half_cap in CAPS:
        over = jnp.maximum(most - zone_cap, across - half_cap) > 0.0
        level = level + jnp.where(over, 1.0, 0.0)
    most = level
    counted[0] = jnp.broadcast_to(most, (1, LANES)).astype(jnp.int32)
    pl.semaphore_wait(barrier, n - 1)

    def tell(k, carry):
        pltpu.make_async_remote_copy(
            src_ref=counted.at[0],
            dst_ref=counts.at[tile],
            send_sem=sends.at[0],
            recv_sem=arrives.at[0],
            device_id=(lax.rem(tile + k, n), mem),
            device_id_type=MESH,
        ).start()
        return carry

    lax.fori_loop(1, n, tell, 0)
    for k in range(1, ZONES):
        pltpu.make_async_remote_copy(
            src_ref=message.at[0],
            dst_ref=gathered.at[zone],
            send_sem=sends.at[1],
            recv_sem=arrives.at[1],
            device_id=(lax.rem(tile + k * zone_tiles, n), mem),
            device_id_type=MESH,
        ).start()

    if select:
        spectrum = table_ref.shape[1]
        levels, mem_dev = field_ref.shape[0], field_ref.shape[1]
        channels = list_ref.shape[1]
        load_field.wait()
        wide[...] = field[...].astype(jnp.float32)
        load_table.wait()
        block = 11 * LANES
        total = jnp.zeros((levels, channels), jnp.float32)
        for first in range(0, spectrum, block):
            size = min(block, spectrum - first)
            entry = lax.broadcasted_iota(jnp.int32, (size, channels), 0) + first
            pick = jnp.where(entry == list_ref[...], 1.0, 0.0).astype(jnp.bfloat16)
            total = total + jnp.dot(
                table[:, first : first + size], pick, preferred_element_type=jnp.float32
            )
        chosen[...] = jnp.zeros_like(chosen)
        chosen[0:levels, 0:channels] = total
        picked = jnp.transpose(chosen[...])[:channels, :levels].astype(jnp.bfloat16)
        flat = wide.reshape(levels * mem_dev, cols)

        def member(k, carry):
            profile = flat[pl.ds(k, levels, stride=mem_dev), :].astype(jnp.bfloat16)
            radiance[pl.ds(k, channels, stride=mem_dev), :] = jnp.dot(
                picked, profile, preferred_element_type=jnp.float32
            )
            return carry

        lax.fori_loop(0, mem_dev, member, 0, unroll=8)
        owned_ref[...] = radiance[...].astype(jnp.bfloat16)

    counts[tile] = counted[0]
    gathered[zone] = message[0]

    def everyone(ref, count, kind):
        span = ref.at[pl.ds(0, count)]
        return pltpu.make_async_remote_copy(
            src_ref=span,
            dst_ref=span,
            send_sem=sends.at[kind],
            recv_sem=arrives.at[kind],
            device_id=(lax.rem(tile + 1, n), mem),
            device_id_type=MESH,
        )

    everyone(gathered, ZONES - 1, 1).wait_recv()
    tables_ref[...] = gathered[...]
    everyone(counts, n - 1, 0).wait_recv()

    def highest(s, top):
        return jnp.maximum(top, counts[s])

    top = lax.fori_loop(0, n, highest, jnp.zeros((1, LANES), jnp.int32))
    count_ref[0, 0] = jnp.max(top.astype(jnp.float32))
    everyone(counts, n - 1, 0).wait_send()
    everyone(gathered, ZONES - 1, 1).wait_send()


def exchange_kernel(
    n,
    nm,
    chunks,
    caps,
    owned_ref,
    tables_ref,
    anom_ref,
    weight_ref,
    mean_ref,
    foot_ref,
    fweight_ref,
    recv_ref,
    analysis_ref,
    spread_ref,
    send_buf,
    away_buf,
    block_buf,
    compact_buf,
    picks,
    away_picks,
    open_picks,
    cross_buf,
    cross_in,
    cross_picks,
    narrow_picks,
    pieces,
    mixed,
    spread,
    mean_wide,
    weight_wide,
    shares,
    stream_send,
    stream_recv,
    m_send,
    m_recv,
    p_send,
    away_send,
    away_recv,
    cross_send,
    cross_recv,
    a_recv,
    local_sem,
):
    tight = caps is not None
    zone_cap, half_cap = caps or (LANES, LANES)
    tile = lax.axis_index("tile")
    mem = lax.axis_index("mem")
    rows, cols = owned_ref.shape
    slots = spread_ref.shape[0] // n
    groups = LANES // slots
    obs = foot_ref.shape[1]
    levels, mem_dev = anom_ref.shape[0], anom_ref.shape[1]
    zone_tiles = n // ZONES
    pairs = zone_tiles // 2
    chunk = rows // chunks
    part = chunk // groups

    zone = tile // zone_tiles
    place = lax.rem(tile, zone_tiles)
    sign = 1 - 2 * (zone // 2)
    inner = jnp.logical_or(zone == 1, zone == 2)
    outer = jnp.logical_not(inner)
    stride = sign * zone_tiles
    ahead = lax.rem(tile + stride + n, n)

    def along(steps):
        return lax.rem(tile + steps * stride + ZONES * n, n)

    if tight:
        source = (tile, along(jnp.where(inner, -1, 1)), along(jnp.where(inner, 1, 2)),
                  along(jnp.where(inner, 2, 3)))
    else:
        source = (tile, along(-1), along(1), along(2))
    zone_base = zone * zone_tiles
    away_base = lax.rem(zone_base - stride + n, n)

    barrier = pltpu.get_barrier_semaphore()

    def greet(k, carry):
        pl.semaphore_signal(
            barrier,
            inc=1,
            device_id=(zone_base + lax.rem(place + k, zone_tiles), mem),
            device_id_type=MESH,
        )
        return carry

    lax.fori_loop(1, zone_tiles, greet, 0)
    for side in (-1, 1):

        @pl.when(jnp.logical_and(zone + side >= 0, zone + side < ZONES))
        def _():
            def greet_side(t, carry):
                pl.semaphore_signal(
                    barrier,
                    inc=1,
                    device_id=(zone_base + side * zone_tiles + t, mem),
                    device_id_type=MESH,
                )
                return carry

            lax.fori_loop(0, zone_tiles, greet_side, 0)

    for k in range(1, nm):
        pl.semaphore_signal(
            barrier, inc=1, device_id=(tile, lax.rem(mem + k, nm)), device_id_type=MESH
        )

    lane_group = lax.broadcasted_iota(jnp.int32, (1, LANES), 1) // slots

    def build(origin, base, into, first_pick):
        row_id = lax.broadcasted_iota(jnp.int32, (groups * cols, 2 * LANES), 0)

        def want(t):
            row = tables_ref[origin // zone_tiles, pl.ds(base + t, 1), :]
            return jnp.maximum(row, 0) + lane_group * cols

        def pair(h, carry):
            wants = jnp.concatenate([want(2 * h), want(2 * h + 1)], axis=1)
            into[first_pick, h] = jnp.where(row_id == wants, 1.0, 0.0).astype(jnp.bfloat16)
            return carry

        lax.fori_loop(0, pairs, pair, 0)

    def build_near(block):
        build(source[block], zone_base, picks, block)

    half = n // 2
    half_base = (zone // 2) * half
    other_base = half - half_base

    def fold_columns(mask, cap, g):
        place_of = positions(mask, cols)[:, 0:1].astype(jnp.int32) + g * cap
        place_of = jnp.where(mask > 0.0, place_of, -1)
        lane = lax.broadcasted_iota(jnp.int32, (cols, FOLD * cap), 1)
        return jnp.where(lane == place_of, 1.0, 0.0).astype(jnp.bfloat16)

    def build_fold(into, origin, base, count, cap):
        mask = needed(tables_ref, origin // zone_tiles, base, count, cols)
        for g in range(FOLD):
            into[g * cols : (g + 1) * cols, :] = fold_columns(mask, cap, g)

    def build_away(block):
        if tight:
            build_fold(away_picks.at[AWAY[block]], source[block], away_base, zone_tiles, zone_cap)
        else:
            build(source[block], away_base, away_picks, AWAY[block])

    def build_cross(i):
        build_fold(cross_picks.at[i], source[i], other_base, half, half_cap)

    def build_narrow(block):
        line = source[block] // zone_tiles
        wide_mask = needed(tables_ref, line, half_base, half, cols)
        wide_place = jnp.where(wide_mask > 0.0, positions(wide_mask, cols), -1.0)
        wide_place = jnp.transpose(wide_place)[0:1, :].astype(jnp.int32)
        row_id = lax.broadcasted_iota(jnp.int32, (half_cap, cols), 0)
        back = jnp.where(row_id == wide_place, 1.0, 0.0).astype(jnp.bfloat16)
        mask = needed(tables_ref, line, away_base, zone_tiles, cols)
        for g in range(FOLD):
            narrow_picks[block - PARTNER, g * half_cap : (g + 1) * half_cap, :] = jnp.dot(
                back, fold_columns(mask, zone_cap, g), preferred_element_type=jnp.float32
            ).astype(jnp.bfloat16)

    def build_open(i, origin, base, count, cap):
        line = origin // zone_tiles
        mask = needed(tables_ref, line, base, count, cols)
        column = lax.broadcasted_iota(jnp.int32, (cols, LANES), 0)
        row_id = lax.broadcasted_iota(jnp.int32, (FOLD * cap, 2 * LANES), 0)

        def one(t, carry):
            row = tables_ref[line, pl.ds(zone_base + t, 1), :]
            ahead_of = jnp.where(column < row, mask, 0.0)
            spot = jnp.sum(ahead_of, axis=0, keepdims=True).astype(jnp.int32)
            wants = jnp.concatenate(
                [spot + (2 * lane_group + v) * cap for v in range(2)], axis=1
            )
            open_picks[i, t, 0 : FOLD * cap] = jnp.where(row_id == wants, 1.0, 0.0).astype(
                jnp.bfloat16
            )
            return carry

        lax.fori_loop(0, zone_tiles, one, 0)

    @pl.when(inner)
    def _():
        if tight:
            build_cross(OWN)
        build_away(OWN)

    build_near(OWN)

    greeted = zone_tiles - 1 + nm - 1 + jnp.where(inner, 2, 1) * zone_tiles
    pl.semaphore_wait(barrier, greeted)

    def span(c):
        return pl.ds(pl.multiple_of(c * chunk, chunk), chunk)

    def narrow(c):
        return pl.ds(pl.multiple_of(c * part, part), part)

    landing = 0 if tight else jnp.where(inner, 1, 0)

    def own_stream(c):
        return pltpu.make_async_remote_copy(
            src_ref=owned_ref.at[span(c)],
            dst_ref=block_buf.at[landing, span(c)],
            send_sem=stream_send.at[0],
            recv_sem=stream_recv.at[landing, c],
            device_id=(ahead, mem),
            device_id_type=MESH,
        )

    def forward_stream(c):
        return pltpu.make_async_remote_copy(
            src_ref=block_buf.at[0, span(c)],
            dst_ref=block_buf.at[2, span(c)],
            send_sem=stream_send.at[1],
            recv_sem=stream_recv.at[2, c],
            device_id=(ahead, mem),
            device_id_type=MESH,
        )

    def stream_arrival(block, c):
        return pltpu.make_async_remote_copy(
            src_ref=owned_ref.at[span(c)],
            dst_ref=block_buf.at[block - 1, span(c)],
            send_sem=stream_send.at[0],
            recv_sem=stream_recv.at[block - 1, c],
            device_id=(ahead, mem),
            device_id_type=MESH,
        )

    def member_copy(k):
        peer = lax.rem(mem + k, nm)
        return pltpu.make_async_remote_copy(
            src_ref=anom_ref,
            dst_ref=pieces.at[nm - 1 - k],
            send_sem=m_send.at[k],
            recv_sem=m_recv.at[nm - k],
            device_id=(tile, peer),
            device_id_type=MESH,
        )

    def parcel(block, t, rows_of):
        return pltpu.make_async_remote_copy(
            src_ref=send_buf.at[block, t, rows_of],
            dst_ref=recv_ref.at[source[block], rows_of],
            send_sem=p_send.at[block],
            recv_sem=a_recv.at[0],
            device_id=(zone_base + t, mem),
            device_id_type=MESH,
        )

    def away_parcel(block, t, rows_of):
        return pltpu.make_async_remote_copy(
            src_ref=away_buf.at[AWAY[block], t, rows_of],
            dst_ref=recv_ref.at[source[block], rows_of],
            send_sem=away_send.at[AWAY[block]],
            recv_sem=a_recv.at[0],
            device_id=(away_base + t, mem),
            device_id_type=MESH,
        )

    fold_part = chunk // FOLD

    def folded(c):
        return pl.ds(pl.multiple_of(c * fold_part, fold_part), fold_part)

    def compact(i, c):
        return pltpu.make_async_remote_copy(
            src_ref=away_buf.at[i, folded(c)],
            dst_ref=compact_buf.at[i, folded(c)],
            send_sem=away_send.at[i],
            recv_sem=away_recv.at[i, c],
            device_id=(along(-1), mem),
            device_id_type=MESH,
        )

    def cross(i, c):
        return pltpu.make_async_remote_copy(
            src_ref=cross_buf.at[i, folded(c)],
            dst_ref=cross_in.at[i, folded(c)],
            send_sem=cross_send.at[i],
            recv_sem=cross_recv.at[i, c],
            device_id=(ahead, mem),
            device_id_type=MESH,
        )

    def spread_out_rows(block, c, count, size):
        block_ref = owned_ref if block == OWN else block_buf.at[block - 1]
        return jnp.concatenate(
            [
                block_ref[pl.ds(pl.multiple_of(c * chunk + g * size, size), size), :]
                for g in range(count)
            ],
            axis=1,
        )

    def pack(block, c, pick_ref, pick, out_ref):
        wide = spread_out_rows(block, c, groups, part)

        def pair(h, carry):
            out = jnp.dot(wide, pick_ref[pick, h], preferred_element_type=jnp.float32)
            out = out.astype(jnp.bfloat16)
            out_ref[pick, 2 * h, narrow(c)] = out[:, :LANES]
            out_ref[pick, 2 * h + 1, narrow(c)] = out[:, LANES:]
            return carry

        lax.fori_loop(0, pairs, pair, 0, unroll=pairs <= 2)

    def pack_near(block, c):
        pack(block, c, picks, block, send_buf)

    def pack_cross(i, c):
        wide = spread_out_rows(i, c, FOLD, fold_part)
        out = jnp.dot(wide, cross_picks[i], preferred_element_type=jnp.float32)
        cross_buf[i, folded(c)] = out.astype(jnp.bfloat16)

    def pack_away(block, c):
        if not tight:
            pack(block, c, away_picks, AWAY[block], away_buf)
            return
        if block == OWN:
            wide, pick = spread_out_rows(OWN, c, FOLD, fold_part), away_picks[AWAY[OWN]]
        else:
            i = block - PARTNER
            wide, pick = cross_in[i, folded(c)], narrow_picks[i]
        out = jnp.dot(wide, pick, preferred_element_type=jnp.float32)
        away_buf[AWAY[block], folded(c)] = out.astype(jnp.bfloat16)

    def unpack(held, i, cap, c):
        def one(t, carry):
            out = jnp.dot(
                held, open_picks[i, t, 0 : FOLD * cap], preferred_element_type=jnp.float32
            )
            out = out.astype(jnp.bfloat16)
            for v in range(2):
                rows_of = pl.ds(
                    pl.multiple_of(c * part + v * fold_part, fold_part), fold_part
                )
                send_buf[1 + i, t, rows_of] = out[:, v * LANES : (v + 1) * LANES]
            return carry

        lax.fori_loop(0, zone_tiles, one, 0, unroll=zone_tiles <= 4)

    def send_near(block, c):
        def one(t, carry):
            @pl.when(zone_base + t != tile)
            def _():
                parcel(block, t, narrow(c)).start()

            return carry

        lax.fori_loop(0, zone_tiles, one, 0)

    def send_away(block, c):
        if tight:
            compact(AWAY[block], c).start()
            return

        def one(t, carry):
            away_parcel(block, t, narrow(c)).start()
            return carry

        lax.fori_loop(0, zone_tiles, one, 0)

    def keep(block):
        return pltpu.make_async_copy(
            send_buf.at[block, place], recv_ref.at[source[block]], local_sem.at[4 + block]
        )

    for k in range(1, nm):
        member_copy(k).start()

    def start_own(c, carry):
        own_stream(c).start()
        return carry

    if tight:

        @pl.when(outer)
        def _():
            lax.fori_loop(0, chunks, start_own, 0)
    else:
        lax.fori_loop(0, chunks, start_own, 0)

    def later(block, c):
        @pl.when(c > 0)
        def _():
            send_near(block, c - 1)

    @pl.when(inner)
    def _():
        def own_step(c, carry):
            if tight:
                pack_cross(OWN, c)
            pack_away(OWN, c)
            if tight:
                cross(OWN, c).start()
            pack_near(OWN, c)
            send_away(OWN, c)
            later(OWN, c)
            return carry

        lax.fori_loop(0, chunks, own_step, 0)

    @pl.when(outer)
    def _():
        def own_step(c, carry):
            pack_near(OWN, c)
            later(OWN, c)
            return carry

        lax.fori_loop(0, chunks, own_step, 0)

    @pl.when(inner)
    def _():
        if tight:
            build_cross(OUTER)
            build_narrow(PARTNER)
            build_open(PARTNER - 1, source[PARTNER], half_base, half, half_cap)
        else:
            build_away(PARTNER)
            build_near(PARTNER)
        build_near(OUTER)

    send_near(OWN, chunks - 1)
    keep(OWN).start()

    @pl.when(inner)
    def _():
        def mid_step(c, carry):
            stream_arrival(OUTER, c).wait_recv()
            if tight:
                pack_cross(OUTER, c)
                cross(PARTNER - PARTNER, c).wait_recv()
                pack_away(PARTNER, c)
                cross(OUTER, c).start()
                unpack(cross_in[0, folded(c)], PARTNER - 1, half_cap, c)
            else:
                forward_stream(c).start()
                stream_arrival(PARTNER, c).wait_recv()
                pack_away(PARTNER, c)
                pack_near(PARTNER, c)
            send_away(PARTNER, c)
            pack_near(OUTER, c)
            send_near(PARTNER, c)
            later(OUTER, c)
            return carry

        lax.fori_loop(0, chunks, mid_step, 0)
        if tight:
            build_narrow(FAR)
            build_open(FAR - 1, source[FAR], half_base, half, half_cap)
        else:
            build_away(FAR)
            build_near(FAR)
        send_near(OUTER, chunks - 1)
        keep(OUTER).start()
        keep(PARTNER).start()

        def far_step(c, carry):
            if tight:
                cross(FAR - PARTNER, c).wait_recv()
                pack_away(FAR, c)
                later(FAR, c)
                send_away(FAR, c)
                unpack(cross_in[1, folded(c)], FAR - 1, half_cap, c)
                return carry
            else:
                stream_arrival(FAR, c).wait_recv()
                pack_away(FAR, c)
                pack_near(FAR, c)
            send_away(FAR, c)
            later(FAR, c)
            return carry

        lax.fori_loop(0, chunks, far_step, 0)

    fweight = fweight_ref[...].astype(jnp.float32)

    def spread_rows(s, carry):
        ids = lax.broadcasted_iota(jnp.int32, (slots, obs), 0) + s * slots
        total = jnp.zeros((slots, obs), jnp.float32)
        for j in range(foot_ref.shape[0]):
            total = total + jnp.where(
                ids == foot_ref[j : j + 1, :], fweight[j : j + 1, :], 0.0
            )
        spread[pl.ds(pl.multiple_of(s * slots, slots), slots), :] = total.astype(jnp.bfloat16)
        return carry

    if tight:

        @pl.when(outer)
        def _():
            for i in range(3):
                build_open(i, source[1 + i], zone_base, zone_tiles, zone_cap)

    lax.fori_loop(0, n, spread_rows, 0)

    @pl.when(inner)
    def _():
        send_near(FAR, chunks - 1)
        keep(FAR).start()

    spread_out = pltpu.make_async_copy(spread, spread_ref, local_sem.at[2])
    spread_out.start()
    mean_wide[...] = mean_ref[...].astype(jnp.float32)
    weight_wide[...] = jnp.transpose(weight_ref[...].astype(jnp.float32))
    mine = weight_wide[pl.ds(mem * mem_dev, mem_dev), :].astype(jnp.bfloat16)
    for p in range(nm):
        shares[p] = mine[:, p * mem_dev : (p + 1) * mem_dev]

    def members_here():
        for k in range(1, nm):
            pltpu.make_async_remote_copy(
                src_ref=anom_ref,
                dst_ref=pieces.at[k - 1],
                send_sem=m_send.at[k],
                recv_sem=m_recv.at[k],
                device_id=(tile, lax.rem(mem + k, nm)),
                device_id_type=MESH,
            ).wait()

    def mix(first, count):
        mixture = jnp.zeros((mem_dev, count * cols), jnp.float32)
        for k in range(nm):
            held = anom_ref if k == 0 else pieces.at[k - 1]
            side = jnp.concatenate([held[first + i] for i in range(count)], axis=1)
            share = shares[lax.rem(mem + k, nm)]
            mixture = mixture + jnp.dot(share, side, preferred_element_type=jnp.float32)
        for i in range(count):
            total = mean_wide[pl.ds(first + i, 1), :] + mixture[:, i * cols : (i + 1) * cols]
            mixed[first + i] = total.astype(jnp.bfloat16)

    def mix_block(b, carry):
        mix(b * MIX_LEVELS, MIX_LEVELS)
        return carry

    full = levels // MIX_LEVELS
    per = -(-full // chunks)

    def mix_share(c):
        lax.fori_loop(c * per, jnp.minimum((c + 1) * per, full), mix_block, 0)

    def mix_step(c, carry):
        mix_share(c)
        return carry

    if tight:

        def open_compact(i, mixing):
            def step(c, carry):
                compact(i, c).wait_recv()
                unpack(compact_buf[i, folded(c)], i, zone_cap, c)
                later(1 + i, c)
                if mixing:
                    mix_share(c)
                return carry

            lax.fori_loop(0, chunks, step, 0)
            send_near(1 + i, chunks - 1)
            keep(1 + i).start()

        @pl.when(outer)
        def _():
            open_compact(0, False)
            open_compact(1, False)
            members_here()
            open_compact(2, True)

        @pl.when(inner)
        def _():
            members_here()
            lax.fori_loop(0, chunks, mix_step, 0)

    else:
        members_here()
        lax.fori_loop(0, chunks, mix_step, 0)

    if levels % MIX_LEVELS:
        mix(full * MIX_LEVELS, levels % MIX_LEVELS)

    analysis_out = pltpu.make_async_copy(mixed, analysis_ref, local_sem.at[3])
    analysis_out.start()

    def gone(ref, sem):
        pltpu.make_async_remote_copy(
            src_ref=ref,
            dst_ref=ref,
            send_sem=sem,
            recv_sem=a_recv.at[0],
            device_id=(ahead, mem),
            device_id_type=MESH,
        ).wait_send()

    def come(count):
        pltpu.make_async_remote_copy(
            src_ref=recv_ref.at[pl.ds(0, count)],
            dst_ref=recv_ref.at[pl.ds(0, count)],
            send_sem=p_send.at[0],
            recv_sem=a_recv.at[0],
            device_id=(ahead, mem),
            device_id_type=MESH,
        ).wait_recv()

    if not tight:
        gone(owned_ref, stream_send.at[0])
    gone(send_buf.at[OWN, pl.ds(0, zone_tiles - 1)], p_send.at[OWN])

    def line_sent():
        for block in (OUTER, PARTNER, FAR):
            gone(send_buf.at[block, pl.ds(0, zone_tiles - 1)], p_send.at[block])
            keep(block).wait()

    @pl.when(inner)
    def _():
        if tight:
            for i in (OWN, OUTER):
                gone(cross_buf.at[i], cross_send.at[i])
        else:
            gone(block_buf.at[0], stream_send.at[1])
        for block in AWAY:
            gone(away_buf.at[AWAY[block]], away_send.at[AWAY[block]])
        line_sent()

    @pl.when(outer)
    def _():
        if tight:
            gone(owned_ref, stream_send.at[0])
            line_sent()
            come(n - ZONES)
        else:
            come(n - 1)

    @pl.when(inner)
    def _():
        come(n - ZONES)

    keep(OWN).wait()
    spread_out.wait()
    analysis_out.wait()


def combine_kernel(
    n, steps, bias_ref, recv_ref, spread_ref, mixed_ref, out_ref, analysis_ref, prior, sems
):
    carry_out = pltpu.make_async_copy(mixed_ref, analysis_ref, sems.at[steps])
    slots = spread_ref.shape[0] // n
    groups = LANES // slots
    members = prior.shape[1]
    channels = prior.shape[0] // steps
    part = recv_ref.shape[1] // steps

    def move(step):
        span = pl.ds(step * channels, channels)
        return pltpu.make_async_copy(prior.at[span], out_ref.at[span], sems.at[step])

    carry_out.start()
    for step in range(steps):
        rows_of = slice(step * part, (step + 1) * part)
        stacked = jnp.concatenate(
            [
                jnp.concatenate(
                    [recv_ref[s, rows_of, g * slots : (g + 1) * slots] for s in range(n)], axis=1
                )
                for g in range(groups)
            ],
            axis=0,
        )
        total = jnp.dot(stacked, spread_ref[...], preferred_element_type=jnp.float32)
        for c in range(channels):
            bias = bias_ref[step * channels + c]
            prior[step * channels + c] = total[c * members : (c + 1) * members, :] + bias
        move(step).start()
    for step in range(steps):
        move(step).wait()
    carry_out.wait()


def chunk_count(channels, mem_dev, groups):
    def fits(count):
        part = channels * mem_dev // (count * groups)
        return channels % count == 0 and part * count * groups == channels * mem_dev and part % 16 == 0

    return next(count for count in (6, 4, 3, 2, 1) if count == 1 or fits(count))


def shards(
    n,
    nm,
    anomalies,
    analysis_weights,
    background_mean,
    background,
    jacobian_table,
    channel_list,
    send_slots,
    footprint,
    footprint_weight,
    channel_bias,
):
    mem_dev, levels, cols = anomalies.shape
    channels = channel_list.shape[0]
    slots = send_slots.shape[2]
    obs, foot = footprint.shape
    groups = LANES // slots
    rows = channels * mem_dev
    members = analysis_weights.shape[1]
    chunks = chunk_count(channels, mem_dev, groups)
    zone_tiles = n // ZONES
    vmem = pl.BlockSpec(memory_space=pltpu.VMEM)
    hbm = pl.BlockSpec(memory_space=pl.ANY)
    far = pl.BlockSpec(memory_space=pltpu.HBM)
    dma = pltpu.SemaphoreType.DMA
    chunk = rows // chunks
    select = mem_dev % 8 == 0
    foldable = chunk % (16 * FOLD) == 0

    front_out = [
        jax.ShapeDtypeStruct((ZONES, n, LANES), jnp.int32),
        jax.ShapeDtypeStruct((1, 1), jnp.float32),
    ]
    front_scratch = [
        pltpu.VMEM((1, n, LANES), jnp.int32),
        pltpu.VMEM((ZONES, n, LANES), jnp.int32),
        pltpu.VMEM((1, 1, LANES), jnp.int32),
        pltpu.VMEM((n, 1, LANES), jnp.int32),
    ]
    front_args, front_specs = [send_slots[0]], [vmem]
    if select:
        spectrum = jacobian_table.shape[0]
        front_out.insert(0, jax.ShapeDtypeStruct((rows, cols), jnp.bfloat16))
        front_scratch += [
            pltpu.VMEM((levels, spectrum), jnp.bfloat16),
            pltpu.VMEM((levels, mem_dev, cols), jnp.bfloat16),
            pltpu.VMEM((levels, mem_dev, cols), jnp.float32),
            pltpu.VMEM((-(-levels // LANES) * LANES, -(-channels // LANES) * LANES), jnp.float32),
            pltpu.VMEM((rows, cols), jnp.float32),
        ]
        front_args = [
            jnp.transpose(jacobian_table),
            channel_list[None, :],
            jnp.transpose(background, (1, 0, 2)),
            send_slots[0],
        ]
        front_specs = [far, vmem, far, vmem]
    front = pl.pallas_call(
        functools.partial(front_kernel, n, select),
        out_shape=tuple(front_out),
        in_specs=front_specs,
        out_specs=(vmem,) * (len(front_out) - 1) + (pl.BlockSpec(memory_space=pltpu.SMEM),),
        scratch_shapes=front_scratch + [dma((2,)), dma((2,)), dma((2,))],
        compiler_params=pltpu.CompilerParams(
            collective_id=0, has_side_effects=True, vmem_limit_bytes=58 * 1024 * 1024
        ),
        name="front",
    )(*front_args)
    tables, count = front[-2:]
    if select:
        owned = front[0]
    else:
        chosen = (
            jnp.arange(jacobian_table.shape[0], dtype=jnp.int32)[:, None] == channel_list[None, :]
        ).astype(jnp.bfloat16)
        selected = jnp.einsum(
            "sl,sc->cl", jacobian_table, chosen, preferred_element_type=jnp.float32
        ).astype(jnp.bfloat16)
        owned = jnp.einsum(
            "cl,klx->ckx", selected, background, preferred_element_type=jnp.float32
        ).astype(jnp.bfloat16).reshape(rows, cols)

    def rest(choice, owned, tables, anomalies, weights, mean, footprint, footprint_weight, bias):
        part = rows // groups
        caps = CAPS[choice] if choice < len(CAPS) else None
        tight = caps is not None
        zone_cap, half_cap = caps or (LANES, LANES)
        pairs = zone_tiles // 2
        spare = (8, LANES)
        fold_rows, capped, widened = rows // FOLD, FOLD * zone_cap, FOLD * half_cap
        if tight:
            variant = [
                (3, fold_rows, capped),
                (1, rows, cols),
                (3, fold_rows, capped),
                (2, pairs, groups * cols, 2 * LANES),
                (1, FOLD * cols, capped),
                (3, zone_tiles, widened, 2 * LANES),
                (2, fold_rows, widened),
                (2, fold_rows, widened),
                (2, FOLD * cols, widened),
                (2, widened, capped),
            ]
        else:
            variant = [
                (3, zone_tiles, part, LANES),
                (3, rows, cols),
                spare,
                (4, pairs, groups * cols, 2 * LANES),
                (3, pairs, groups * cols, 2 * LANES),
            ] + [spare] * 5
        variant = [pltpu.VMEM(shape, jnp.bfloat16) for shape in variant]
        received, mixed, spread = pl.pallas_call(
            functools.partial(exchange_kernel, n, nm, chunks, caps),
            out_shape=(
                jax.ShapeDtypeStruct((n, part, LANES), jnp.bfloat16),
                jax.ShapeDtypeStruct((levels, mem_dev, cols), jnp.bfloat16),
                jax.ShapeDtypeStruct((n * slots, obs), jnp.bfloat16),
            ),
            in_specs=[vmem] * 7,
            out_specs=(hbm, hbm, hbm),
            scratch_shapes=[pltpu.VMEM((4, zone_tiles, part, LANES), jnp.bfloat16)]
            + variant
            + [
                pltpu.VMEM((max(nm - 1, 1), levels, mem_dev, cols), jnp.bfloat16),
                pltpu.VMEM((levels, mem_dev, cols), jnp.bfloat16),
                pltpu.VMEM((n * slots, obs), jnp.bfloat16),
                pltpu.VMEM((levels, cols), jnp.float32),
                pltpu.VMEM((members, members), jnp.float32),
                pltpu.VMEM((nm, mem_dev, mem_dev), jnp.bfloat16),
                dma((2,)),
                dma((3, chunks)),
                dma((nm,)),
                dma((nm,)),
                dma((4,)),
                dma((3,)),
                dma((3, chunks)),
                dma((2,)),
                dma((2, chunks)),
                dma((1,)),
                dma((8,)),
            ],
            compiler_params=pltpu.CompilerParams(
                collective_id=1 + choice, has_side_effects=True, vmem_limit_bytes=44 * 1024 * 1024
            ),
            name=f"exchange_{zone_cap}",
        )(owned, tables, anomalies, weights, mean, footprint, footprint_weight)
        return pl.pallas_call(
            functools.partial(combine_kernel, n, chunks),
            out_shape=(
                jax.ShapeDtypeStruct((channels, mem_dev, obs), jnp.float32),
                jax.ShapeDtypeStruct(mixed.shape, mixed.dtype),
            ),
            in_specs=[pl.BlockSpec(memory_space=pltpu.SMEM), vmem, vmem, vmem],
            out_specs=(hbm, hbm),
            scratch_shapes=[
                pltpu.VMEM((channels, mem_dev, obs), jnp.float32),
                dma((chunks + 1,)),
            ],
            compiler_params=pltpu.CompilerParams(vmem_limit_bytes=40 * 1024 * 1024),
            name="combine",
        )(bias, received, spread, mixed)

    operands = (
        owned,
        tables,
        jnp.transpose(anomalies, (1, 0, 2)),
        analysis_weights[0],
        background_mean,
        jnp.transpose(footprint),
        jnp.transpose(footprint_weight),
        channel_bias,
    )
    if foldable:
        prior, analysis = lax.switch(
            count[0, 0].astype(jnp.int32),
            [functools.partial(rest, choice) for choice in range(len(CAPS) + 1)],
            *operands,
        )
    else:
        prior, analysis = rest(len(CAPS), *operands)
    return jnp.transpose(analysis, (1, 0, 2)), prior


def solution(mesh):
    placed = (
        P("mem", None, "tile"),
        P("tile", None, None),
        P(None, "tile"),
        P("mem", None, "tile"),
        P(),
        P(),
        P("tile", None, None),
        P("tile", None),
        P("tile", None),
        P(),
    )
    return jax.shard_map(
        functools.partial(shards, mesh.shape["tile"], mesh.shape["mem"]),
        mesh=mesh,
        in_specs=placed,
        out_specs=(P("mem", None, "tile"), P(None, "mem", "tile")),
        check_vma=False,
    )
```

```python
import functools

import jax
import jax.numpy as jnp
from jax import lax
from jax.experimental import pallas as pl
from jax.experimental.pallas import tpu as pltpu
from jax.sharding import PartitionSpec as P

LANES = 128
MESH = pl.DeviceIdType.MESH
ZONES = 4
MIX_LEVELS = 8

OWN, OUTER, PARTNER, FAR = range(4)
AWAY = {OWN: 0, PARTNER: 1, FAR: 2}
CAPS = ((64, 96), (80, 112))
FOLD = 8


def needed(table_ref, source, base, count, cols):
    column = lax.broadcasted_iota(jnp.int32, (cols, LANES), 0)

    def one(t, hit):
        row = table_ref[source, pl.ds(base + t, 1), :]
        return jnp.where(column == row, 1.0, hit)

    hit = lax.fori_loop(0, count, one, jnp.zeros((cols, LANES), jnp.float32))
    return jnp.max(hit, axis=1, keepdims=True)


def positions(mask, cols):
    before = lax.broadcasted_iota(jnp.int32, (cols, cols), 1) < lax.broadcasted_iota(
        jnp.int32, (cols, cols), 0
    )
    full = jnp.broadcast_to(mask, (cols, LANES)).astype(jnp.bfloat16)
    return jnp.dot(
        jnp.where(before, 1.0, 0.0).astype(jnp.bfloat16), full, preferred_element_type=jnp.float32
    )


def front_kernel(
    n,
    select,
    *refs,
):
    if select:
        (table_ref, list_ref, field_ref, slots_ref, owned_ref, tables_ref, count_ref,
         message, gathered, counted, counts, table, field, wide, chosen, radiance,
         sends, arrives, local_sem) = refs
    else:
        (slots_ref, tables_ref, count_ref, message, gathered, counted, counts,
         sends, arrives, local_sem) = refs
    tile = lax.axis_index("tile")
    mem = lax.axis_index("mem")
    slots = slots_ref.shape[1]
    groups = LANES // slots
    cols = LANES
    zone_tiles = n // ZONES
    zone = tile // zone_tiles
    barrier = pltpu.get_barrier_semaphore()

    def greet(k, carry):
        pl.semaphore_signal(
            barrier, inc=1, device_id=(lax.rem(tile + k, n), mem), device_id_type=MESH
        )
        return carry

    lax.fori_loop(1, n, greet, 0)
    if select:
        load_table = pltpu.make_async_copy(table_ref, table, local_sem.at[0])
        load_table.start()
        load_field = pltpu.make_async_copy(field_ref, field, local_sem.at[1])
        load_field.start()

    message[0] = jnp.concatenate([slots_ref[...]] * groups, axis=1)
    most = jnp.zeros((1, 1), jnp.float32)
    for far in (0, ZONES - 1):
        mask = needed(message, 0, far * zone_tiles, zone_tiles, cols)
        total = jnp.sum(mask, axis=0, keepdims=True)
        most = jnp.maximum(most, jnp.where(zone == far, 0.0, total))
    across = needed(message, 0, (1 - zone // 2) * (n // 2), n // 2, cols)
    across = jnp.sum(across, axis=0, keepdims=True)
    level = jnp.zeros((1, 1), jnp.float32)
    for zone_cap, half_cap in CAPS:
        over = jnp.maximum(most - zone_cap, across - half_cap) > 0.0
        level = level + jnp.where(over, 1.0, 0.0)
    most = level
    counted[0] = jnp.broadcast_to(most, (1, LANES)).astype(jnp.int32)
    pl.semaphore_wait(barrier, n - 1)

    def tell(k, carry):
        pltpu.make_async_remote_copy(
            src_ref=counted.at[0],
            dst_ref=counts.at[tile],
            send_sem=sends.at[0],
            recv_sem=arrives.at[0],
            device_id=(lax.rem(tile + k, n), mem),
            device_id_type=MESH,
        ).start()
        return carry

    lax.fori_loop(1, n, tell, 0)
    for k in range(1, ZONES):
        pltpu.make_async_remote_copy(
            src_ref=message.at[0],
            dst_ref=gathered.at[zone],
            send_sem=sends.at[1],
            recv_sem=arrives.at[1],
            device_id=(lax.rem(tile + k * zone_tiles, n), mem),
            device_id_type=MESH,
        ).start()

    if select:
        spectrum = table_ref.shape[1]
        levels, mem_dev = field_ref.shape[0], field_ref.shape[1]
        channels = list_ref.shape[1]
        load_field.wait()
        wide[...] = field[...].astype(jnp.float32)
        load_table.wait()
        block = 11 * LANES
        total = jnp.zeros((levels, channels), jnp.float32)
        for first in range(0, spectrum, block):
            size = min(block, spectrum - first)
            entry = lax.broadcasted_iota(jnp.int32, (size, channels), 0) + first
            pick = jnp.where(entry == list_ref[...], 1.0, 0.0).astype(jnp.bfloat16)
            total = total + jnp.dot(
                table[:, first : first + size], pick, preferred_element_type=jnp.float32
            )
        chosen[...] = jnp.zeros_like(chosen)
        chosen[0:levels, 0:channels] = total
        picked = jnp.transpose(chosen[...])[:channels, :levels].astype(jnp.bfloat16)
        flat = wide.reshape(levels * mem_dev, cols)

        def member(k, carry):
            profile = flat[pl.ds(k, levels, stride=mem_dev), :].astype(jnp.bfloat16)
            radiance[pl.ds(k, channels, stride=mem_dev), :] = jnp.dot(
                picked, profile, preferred_element_type=jnp.float32
            )
            return carry

        lax.fori_loop(0, mem_dev, member, 0, unroll=8)
        owned_ref[...] = radiance[...].astype(jnp.bfloat16)

    counts[tile] = counted[0]
    gathered[zone] = message[0]

    def everyone(ref, count, kind):
        span = ref.at[pl.ds(0, count)]
        return pltpu.make_async_remote_copy(
            src_ref=span,
            dst_ref=span,
            send_sem=sends.at[kind],
            recv_sem=arrives.at[kind],
            device_id=(lax.rem(tile + 1, n), mem),
            device_id_type=MESH,
        )

    everyone(gathered, ZONES - 1, 1).wait_recv()
    tables_ref[...] = gathered[...]
    everyone(counts, n - 1, 0).wait_recv()

    def highest(s, top):
        return jnp.maximum(top, counts[s])

    top = lax.fori_loop(0, n, highest, jnp.zeros((1, LANES), jnp.int32))
    count_ref[0, 0] = jnp.max(top.astype(jnp.float32))
    everyone(counts, n - 1, 0).wait_send()
    everyone(gathered, ZONES - 1, 1).wait_send()


def exchange_kernel(
    n,
    nm,
    chunks,
    caps,
    owned_ref,
    tables_ref,
    anom_ref,
    weight_ref,
    mean_ref,
    foot_ref,
    fweight_ref,
    recv_ref,
    analysis_ref,
    spread_ref,
    send_buf,
    away_buf,
    block_buf,
    compact_buf,
    picks,
    away_picks,
    open_picks,
    cross_buf,
    cross_in,
    cross_picks,
    narrow_picks,
    pieces,
    mixed,
    spread,
    mean_wide,
    weight_wide,
    shares,
    stream_send,
    stream_recv,
    m_send,
    m_recv,
    p_send,
    away_send,
    away_recv,
    cross_send,
    cross_recv,
    a_recv,
    local_sem,
):
    tight = caps is not None
    zone_cap, half_cap = caps or (LANES, LANES)
    tile = lax.axis_index("tile")
    mem = lax.axis_index("mem")
    rows, cols = owned_ref.shape
    slots = spread_ref.shape[0] // n
    groups = LANES // slots
    obs = foot_ref.shape[1]
    levels, mem_dev = anom_ref.shape[0], anom_ref.shape[1]
    zone_tiles = n // ZONES
    pairs = zone_tiles // 2
    chunk = rows // chunks
    part = chunk // groups

    zone = tile // zone_tiles
    place = lax.rem(tile, zone_tiles)
    sign = 1 - 2 * (zone // 2)
    inner = jnp.logical_or(zone == 1, zone == 2)
    outer = jnp.logical_not(inner)
    stride = sign * zone_tiles
    ahead = lax.rem(tile + stride + n, n)

    def along(steps):
        return lax.rem(tile + steps * stride + ZONES * n, n)

    if tight:
        source = (tile, along(jnp.where(inner, -1, 1)), along(jnp.where(inner, 1, 2)),
                  along(jnp.where(inner, 2, 3)))
    else:
        source = (tile, along(-1), along(1), along(2))
    zone_base = zone * zone_tiles
    away_base = lax.rem(zone_base - stride + n, n)

    barrier = pltpu.get_barrier_semaphore()

    def greet(k, carry):
        pl.semaphore_signal(
            barrier,
            inc=1,
            device_id=(zone_base + lax.rem(place + k, zone_tiles), mem),
            device_id_type=MESH,
        )
        return carry

    lax.fori_loop(1, zone_tiles, greet, 0)
    for side in (-1, 1):

        @pl.when(jnp.logical_and(zone + side >= 0, zone + side < ZONES))
        def _():
            def greet_side(t, carry):
                pl.semaphore_signal(
                    barrier,
                    inc=1,
                    device_id=(zone_base + side * zone_tiles + t, mem),
                    device_id_type=MESH,
                )
                return carry

            lax.fori_loop(0, zone_tiles, greet_side, 0)

    for k in range(1, nm):
        pl.semaphore_signal(
            barrier, inc=1, device_id=(tile, lax.rem(mem + k, nm)), device_id_type=MESH
        )

    lane_group = lax.broadcasted_iota(jnp.int32, (1, LANES), 1) // slots

    def build(origin, base, into, first_pick):
        row_id = lax.broadcasted_iota(jnp.int32, (groups * cols, 2 * LANES), 0)

        def want(t):
            row = tables_ref[origin // zone_tiles, pl.ds(base + t, 1), :]
            return jnp.maximum(row, 0) + lane_group * cols

        def pair(h, carry):
            wants = jnp.concatenate([want(2 * h), want(2 * h + 1)], axis=1)
            into[first_pick, h] = jnp.where(row_id == wants, 1.0, 0.0).astype(jnp.bfloat16)
            return carry

        lax.fori_loop(0, pairs, pair, 0)

    def build_near(block):
        build(source[block], zone_base, picks, block)

    half = n // 2
    half_base = (zone // 2) * half
    other_base = half - half_base

    def fold_columns(mask, cap, g):
        place_of = positions(mask, cols)[:, 0:1].astype(jnp.int32) + g * cap
        place_of = jnp.where(mask > 0.0, place_of, -1)
        lane = lax.broadcasted_iota(jnp.int32, (cols, FOLD * cap), 1)
        return jnp.where(lane == place_of, 1.0, 0.0).astype(jnp.bfloat16)

    def build_fold(into, origin, base, count, cap):
        mask = needed(tables_ref, origin // zone_tiles, base, count, cols)
        for g in range(FOLD):
            into[g * cols : (g + 1) * cols, :] = fold_columns(mask, cap, g)

    def build_away(block):
        if tight:
            build_fold(away_picks.at[AWAY[block]], source[block], away_base, zone_tiles, zone_cap)
        else:
            build(source[block], away_base, away_picks, AWAY[block])

    def build_cross(i):
        build_fold(cross_picks.at[i], source[i], other_base, half, half_cap)

    def build_narrow(block):
        line = source[block] // zone_tiles
        wide_mask = needed(tables_ref, line, half_base, half, cols)
        wide_place = jnp.where(wide_mask > 0.0, positions(wide_mask, cols), -1.0)
        wide_place = jnp.transpose(wide_place)[0:1, :].astype(jnp.int32)
        row_id = lax.broadcasted_iota(jnp.int32, (half_cap, cols), 0)
        back = jnp.where(row_id == wide_place, 1.0, 0.0).astype(jnp.bfloat16)
        mask = needed(tables_ref, line, away_base, zone_tiles, cols)
        for g in range(FOLD):
            narrow_picks[block - PARTNER, g * half_cap : (g + 1) * half_cap, :] = jnp.dot(
                back, fold_columns(mask, zone_cap, g), preferred_element_type=jnp.float32
            ).astype(jnp.bfloat16)

    def build_open(i, origin, base, count, cap):
        line = origin // zone_tiles
        mask = needed(tables_ref, line, base, count, cols)
        column = lax.broadcasted_iota(jnp.int32, (cols, LANES), 0)
        row_id = lax.broadcasted_iota(jnp.int32, (FOLD * cap, 2 * LANES), 0)

        def one(t, carry):
            row = tables_ref[line, pl.ds(zone_base + t, 1), :]
            ahead_of = jnp.where(column < row, mask, 0.0)
            spot = jnp.sum(ahead_of, axis=0, keepdims=True).astype(jnp.int32)
            wants = jnp.concatenate(
                [spot + (2 * lane_group + v) * cap for v in range(2)], axis=1
            )
            open_picks[i, t, 0 : FOLD * cap] = jnp.where(row_id == wants, 1.0, 0.0).astype(
                jnp.bfloat16
            )
            return carry

        lax.fori_loop(0, zone_tiles, one, 0)

    @pl.when(inner)
    def _():
        if tight:
            build_cross(OWN)
        build_away(OWN)

    build_near(OWN)

    greeted = zone_tiles - 1 + nm - 1 + jnp.where(inner, 2, 1) * zone_tiles
    pl.semaphore_wait(barrier, greeted)

    def span(c):
        return pl.ds(pl.multiple_of(c * chunk, chunk), chunk)

    def narrow(c):
        return pl.ds(pl.multiple_of(c * part, part), part)

    landing = 0 if tight else jnp.where(inner, 1, 0)

    def own_stream(c):
        return pltpu.make_async_remote_copy(
            src_ref=owned_ref.at[span(c)],
            dst_ref=block_buf.at[landing, span(c)],
            send_sem=stream_send.at[0],
            recv_sem=stream_recv.at[landing, c],
            device_id=(ahead, mem),
            device_id_type=MESH,
        )

    def forward_stream(c):
        return pltpu.make_async_remote_copy(
            src_ref=block_buf.at[0, span(c)],
            dst_ref=block_buf.at[2, span(c)],
            send_sem=stream_send.at[1],
            recv_sem=stream_recv.at[2, c],
            device_id=(ahead, mem),
            device_id_type=MESH,
        )

    def stream_arrival(block, c):
        return pltpu.make_async_remote_copy(
            src_ref=owned_ref.at[span(c)],
            dst_ref=block_buf.at[block - 1, span(c)],
            send_sem=stream_send.at[0],
            recv_sem=stream_recv.at[block - 1, c],
            device_id=(ahead, mem),
            device_id_type=MESH,
        )

    def member_copy(k):
        peer = lax.rem(mem + k, nm)
        return pltpu.make_async_remote_copy(
            src_ref=anom_ref,
            dst_ref=pieces.at[nm - 1 - k],
            send_sem=m_send.at[k],
            recv_sem=m_recv.at[nm - k],
            device_id=(tile, peer),
            device_id_type=MESH,
        )

    def parcel(block, t, rows_of):
        return pltpu.make_async_remote_copy(
            src_ref=send_buf.at[block, t, rows_of],
            dst_ref=recv_ref.at[source[block], rows_of],
            send_sem=p_send.at[block],
            recv_sem=a_recv.at[0],
            device_id=(zone_base + t, mem),
            device_id_type=MESH,
        )

    def away_parcel(block, t, rows_of):
        return pltpu.make_async_remote_copy(
            src_ref=away_buf.at[AWAY[block], t, rows_of],
            dst_ref=recv_ref.at[source[block], rows_of],
            send_sem=away_send.at[AWAY[block]],
            recv_sem=a_recv.at[0],
            device_id=(away_base + t, mem),
            device_id_type=MESH,
        )

    fold_part = chunk // FOLD

    def folded(c):
        return pl.ds(pl.multiple_of(c * fold_part, fold_part), fold_part)

    def compact(i, c):
        return pltpu.make_async_remote_copy(
            src_ref=away_buf.at[i, folded(c)],
            dst_ref=compact_buf.at[i, folded(c)],
            send_sem=away_send.at[i],
            recv_sem=away_recv.at[i, c],
            device_id=(along(-1), mem),
            device_id_type=MESH,
        )

    def cross(i, c):
        return pltpu.make_async_remote_copy(
            src_ref=cross_buf.at[i, folded(c)],
            dst_ref=cross_in.at[i, folded(c)],
            send_sem=cross_send.at[i],
            recv_sem=cross_recv.at[i, c],
            device_id=(ahead, mem),
            device_id_type=MESH,
        )

    def spread_out_rows(block, c, count, size):
        block_ref = owned_ref if block == OWN else block_buf.at[block - 1]
        return jnp.concatenate(
            [
                block_ref[pl.ds(pl.multiple_of(c * chunk + g * size, size), size), :]
                for g in range(count)
            ],
            axis=1,
        )

    def pack(block, c, pick_ref, pick, out_ref):
        wide = spread_out_rows(block, c, groups, part)

        def pair(h, carry):
            out = jnp.dot(wide, pick_ref[pick, h], preferred_element_type=jnp.float32)
            out = out.astype(jnp.bfloat16)
            out_ref[pick, 2 * h, narrow(c)] = out[:, :LANES]
            out_ref[pick, 2 * h + 1, narrow(c)] = out[:, LANES:]
            return carry

        lax.fori_loop(0, pairs, pair, 0, unroll=pairs <= 2)

    def pack_near(block, c):
        pack(block, c, picks, block, send_buf)

    def pack_cross(i, c):
        wide = spread_out_rows(i, c, FOLD, fold_part)
        out = jnp.dot(wide, cross_picks[i], preferred_element_type=jnp.float32)
        cross_buf[i, folded(c)] = out.astype(jnp.bfloat16)

    def pack_away(block, c):
        if not tight:
            pack(block, c, away_picks, AWAY[block], away_buf)
            return
        if block == OWN:
            wide, pick = spread_out_rows(OWN, c, FOLD, fold_part), away_picks[AWAY[OWN]]
        else:
            i = block - PARTNER
            wide, pick = cross_in[i, folded(c)], narrow_picks[i]
        out = jnp.dot(wide, pick, preferred_element_type=jnp.float32)
        away_buf[AWAY[block], folded(c)] = out.astype(jnp.bfloat16)

    def unpack(held, i, cap, c):
        def one(t, carry):
            out = jnp.dot(
                held, open_picks[i, t, 0 : FOLD * cap], preferred_element_type=jnp.float32
            )
            out = out.astype(jnp.bfloat16)
            for v in range(2):
                rows_of = pl.ds(
                    pl.multiple_of(c * part + v * fold_part, fold_part), fold_part
                )
                send_buf[1 + i, t, rows_of] = out[:, v * LANES : (v + 1) * LANES]
            return carry

        lax.fori_loop(0, zone_tiles, one, 0, unroll=zone_tiles <= 4)

    def send_near(block, c):
        def one(t, carry):
            @pl.when(zone_base + t != tile)
            def _():
                parcel(block, t, narrow(c)).start()

            return carry

        lax.fori_loop(0, zone_tiles, one, 0)

    def send_away(block, c):
        if tight:
            compact(AWAY[block], c).start()
            return

        def one(t, carry):
            away_parcel(block, t, narrow(c)).start()
            return carry

        lax.fori_loop(0, zone_tiles, one, 0)

    def keep(block):
        return pltpu.make_async_copy(
            send_buf.at[block, place], recv_ref.at[source[block]], local_sem.at[4 + block]
        )

    for k in range(1, nm):
        member_copy(k).start()

    def start_own(c, carry):
        own_stream(c).start()
        return carry

    if tight:

        @pl.when(outer)
        def _():
            lax.fori_loop(0, chunks, start_own, 0)
    else:
        lax.fori_loop(0, chunks, start_own, 0)

    def later(block, c):
        @pl.when(c > 0)
        def _():
            send_near(block, c - 1)

    @pl.when(inner)
    def _():
        def own_step(c, carry):
            if tight:
                pack_cross(OWN, c)
            pack_away(OWN, c)
            if tight:
                cross(OWN, c).start()
            pack_near(OWN, c)
            send_away(OWN, c)
            later(OWN, c)
            return carry

        lax.fori_loop(0, chunks, own_step, 0)

    @pl.when(outer)
    def _():
        def own_step(c, carry):
            pack_near(OWN, c)
            later(OWN, c)
            return carry

        lax.fori_loop(0, chunks, own_step, 0)

    @pl.when(inner)
    def _():
        if tight:
            build_cross(OUTER)
            build_narrow(PARTNER)
            build_open(PARTNER - 1, source[PARTNER], half_base, half, half_cap)
        else:
            build_away(PARTNER)
            build_near(PARTNER)
        build_near(OUTER)

    fweight = fweight_ref[...].astype(jnp.float32)

    def spread_rows(s, carry):
        ids = lax.broadcasted_iota(jnp.int32, (slots, obs), 0) + s * slots
        total = jnp.zeros((slots, obs), jnp.float32)
        for j in range(foot_ref.shape[0]):
            total = total + jnp.where(
                ids == foot_ref[j : j + 1, :], fweight[j : j + 1, :], 0.0
            )
        spread[pl.ds(pl.multiple_of(s * slots, slots), slots), :] = total.astype(jnp.bfloat16)
        return carry

    if tight:

        @pl.when(outer)
        def _():
            for i in range(3):
                build_open(i, source[1 + i], zone_base, zone_tiles, zone_cap)

    spread_per = -(-n // chunks)

    def spread_share(c):
        lax.fori_loop(c * spread_per, jnp.minimum((c + 1) * spread_per, n), spread_rows, 0)

    send_near(OWN, chunks - 1)
    keep(OWN).start()

    @pl.when(inner)
    def _():
        def mid_step(c, carry):
            stream_arrival(OUTER, c).wait_recv()
            if tight:
                pack_cross(OUTER, c)
                cross(PARTNER - PARTNER, c).wait_recv()
                pack_away(PARTNER, c)
                cross(OUTER, c).start()
                unpack(cross_in[0, folded(c)], PARTNER - 1, half_cap, c)
            else:
                forward_stream(c).start()
                stream_arrival(PARTNER, c).wait_recv()
                pack_away(PARTNER, c)
                pack_near(PARTNER, c)
            send_away(PARTNER, c)
            pack_near(OUTER, c)
            send_near(PARTNER, c)
            later(OUTER, c)
            return carry

        lax.fori_loop(0, chunks, mid_step, 0)
        if tight:
            build_narrow(FAR)
            build_open(FAR - 1, source[FAR], half_base, half, half_cap)
        else:
            build_away(FAR)
            build_near(FAR)
        send_near(OUTER, chunks - 1)
        keep(OUTER).start()
        keep(PARTNER).start()

        def far_step(c, carry):
            if tight:
                cross(FAR - PARTNER, c).wait_recv()
                pack_away(FAR, c)
                unpack(cross_in[1, folded(c)], FAR - 1, half_cap, c)
            else:
                stream_arrival(FAR, c).wait_recv()
                pack_away(FAR, c)
                pack_near(FAR, c)
            send_away(FAR, c)
            spread_share(c)
            send_near(FAR, c)
            return carry

        lax.fori_loop(0, chunks, far_step, 0)

    @pl.when(outer)
    def _():
        lax.fori_loop(0, n, spread_rows, 0)

    @pl.when(inner)
    def _():
        keep(FAR).start()

    spread_out = pltpu.make_async_copy(spread, spread_ref, local_sem.at[2])
    spread_out.start()
    mean_wide[...] = mean_ref[...].astype(jnp.float32)
    weight_wide[...] = jnp.transpose(weight_ref[...].astype(jnp.float32))
    mine = weight_wide[pl.ds(mem * mem_dev, mem_dev), :].astype(jnp.bfloat16)
    for p in range(nm):
        shares[p] = mine[:, p * mem_dev : (p + 1) * mem_dev]

    def members_here():
        for k in range(1, nm):
            pltpu.make_async_remote_copy(
                src_ref=anom_ref,
                dst_ref=pieces.at[k - 1],
                send_sem=m_send.at[k],
                recv_sem=m_recv.at[k],
                device_id=(tile, lax.rem(mem + k, nm)),
                device_id_type=MESH,
            ).wait()

    def mix(first, count):
        mixture = jnp.zeros((mem_dev, count * cols), jnp.float32)
        for k in range(nm):
            held = anom_ref if k == 0 else pieces.at[k - 1]
            side = jnp.concatenate([held[first + i] for i in range(count)], axis=1)
            share = shares[lax.rem(mem + k, nm)]
            mixture = mixture + jnp.dot(share, side, preferred_element_type=jnp.float32)
        for i in range(count):
            total = mean_wide[pl.ds(first + i, 1), :] + mixture[:, i * cols : (i + 1) * cols]
            mixed[first + i] = total.astype(jnp.bfloat16)

    def mix_block(b, carry):
        mix(b * MIX_LEVELS, MIX_LEVELS)
        return carry

    full = levels // MIX_LEVELS
    per = -(-full // max(chunks - 1, 1))

    def mix_share(c):
        lax.fori_loop(c * per, jnp.minimum((c + 1) * per, full), mix_block, 0)

    def mix_step(c, carry):
        mix_share(c)
        return carry

    if tight:

        def open_compact(i, mixing):
            def step(c, carry):
                compact(i, c).wait_recv()
                unpack(compact_buf[i, folded(c)], i, zone_cap, c)
                if mixing:
                    mix_share(c)
                    send_near(1 + i, c)
                else:
                    later(1 + i, c)
                return carry

            lax.fori_loop(0, chunks, step, 0)
            if not mixing:
                send_near(1 + i, chunks - 1)
            keep(1 + i).start()

        @pl.when(outer)
        def _():
            open_compact(0, False)
            open_compact(1, False)
            members_here()
            open_compact(2, True)

        @pl.when(inner)
        def _():
            members_here()
            lax.fori_loop(0, chunks, mix_step, 0)

    else:
        members_here()
        lax.fori_loop(0, chunks, mix_step, 0)

    if levels % MIX_LEVELS:
        mix(full * MIX_LEVELS, levels % MIX_LEVELS)

    analysis_out = pltpu.make_async_copy(mixed, analysis_ref, local_sem.at[3])
    analysis_out.start()

    def gone(ref, sem):
        pltpu.make_async_remote_copy(
            src_ref=ref,
            dst_ref=ref,
            send_sem=sem,
            recv_sem=a_recv.at[0],
            device_id=(ahead, mem),
            device_id_type=MESH,
        ).wait_send()

    def come(count):
        pltpu.make_async_remote_copy(
            src_ref=recv_ref.at[pl.ds(0, count)],
            dst_ref=recv_ref.at[pl.ds(0, count)],
            send_sem=p_send.at[0],
            recv_sem=a_recv.at[0],
            device_id=(ahead, mem),
            device_id_type=MESH,
        ).wait_recv()

    if not tight:
        gone(owned_ref, stream_send.at[0])
    gone(send_buf.at[OWN, pl.ds(0, zone_tiles - 1)], p_send.at[OWN])

    def line_sent():
        for block in (OUTER, PARTNER, FAR):
            gone(send_buf.at[block, pl.ds(0, zone_tiles - 1)], p_send.at[block])
            keep(block).wait()

    @pl.when(inner)
    def _():
        if tight:
            for i in (OWN, OUTER):
                gone(cross_buf.at[i], cross_send.at[i])
        else:
            gone(block_buf.at[0], stream_send.at[1])
        for block in AWAY:
            gone(away_buf.at[AWAY[block]], away_send.at[AWAY[block]])
        line_sent()

    @pl.when(outer)
    def _():
        if tight:
            gone(owned_ref, stream_send.at[0])
            line_sent()
            come(n - ZONES)
        else:
            come(n - 1)

    @pl.when(inner)
    def _():
        come(n - ZONES)

    keep(OWN).wait()
    spread_out.wait()
    analysis_out.wait()


def combine_kernel(
    n, steps, bias_ref, recv_ref, spread_ref, mixed_ref, out_ref, analysis_ref, prior, sems
):
    carry_out = pltpu.make_async_copy(mixed_ref, analysis_ref, sems.at[steps])
    slots = spread_ref.shape[0] // n
    groups = LANES // slots
    members = prior.shape[1]
    channels = prior.shape[0] // steps
    part = recv_ref.shape[1] // steps

    def move(step):
        span = pl.ds(step * channels, channels)
        return pltpu.make_async_copy(prior.at[span], out_ref.at[span], sems.at[step])

    carry_out.start()
    for step in range(steps):
        rows_of = slice(step * part, (step + 1) * part)
        stacked = jnp.concatenate(
            [
                jnp.concatenate(
                    [recv_ref[s, rows_of, g * slots : (g + 1) * slots] for s in range(n)], axis=1
                )
                for g in range(groups)
            ],
            axis=0,
        )
        total = jnp.dot(stacked, spread_ref[...], preferred_element_type=jnp.float32)
        for c in range(channels):
            bias = bias_ref[step * channels + c]
            prior[step * channels + c] = total[c * members : (c + 1) * members, :] + bias
        move(step).start()
    for step in range(steps):
        move(step).wait()
    carry_out.wait()


def chunk_count(channels, mem_dev, groups):
    def fits(count):
        part = channels * mem_dev // (count * groups)
        return channels % count == 0 and part * count * groups == channels * mem_dev and part % 16 == 0

    return next(count for count in (6, 4, 3, 2, 1) if count == 1 or fits(count))


def shards(
    n,
    nm,
    anomalies,
    analysis_weights,
    background_mean,
    background,
    jacobian_table,
    channel_list,
    send_slots,
    footprint,
    footprint_weight,
    channel_bias,
):
    mem_dev, levels, cols = anomalies.shape
    channels = channel_list.shape[0]
    slots = send_slots.shape[2]
    obs, foot = footprint.shape
    groups = LANES // slots
    rows = channels * mem_dev
    members = analysis_weights.shape[1]
    chunks = chunk_count(channels, mem_dev, groups)
    zone_tiles = n // ZONES
    vmem = pl.BlockSpec(memory_space=pltpu.VMEM)
    hbm = pl.BlockSpec(memory_space=pl.ANY)
    far = pl.BlockSpec(memory_space=pltpu.HBM)
    dma = pltpu.SemaphoreType.DMA
    chunk = rows // chunks
    select = mem_dev % 8 == 0
    foldable = chunk % (16 * FOLD) == 0

    front_out = [
        jax.ShapeDtypeStruct((ZONES, n, LANES), jnp.int32),
        jax.ShapeDtypeStruct((1, 1), jnp.float32),
    ]
    front_scratch = [
        pltpu.VMEM((1, n, LANES), jnp.int32),
        pltpu.VMEM((ZONES, n, LANES), jnp.int32),
        pltpu.VMEM((1, 1, LANES), jnp.int32),
        pltpu.VMEM((n, 1, LANES), jnp.int32),
    ]
    front_args, front_specs = [send_slots[0]], [vmem]
    if select:
        spectrum = jacobian_table.shape[0]
        front_out.insert(0, jax.ShapeDtypeStruct((rows, cols), jnp.bfloat16))
        front_scratch += [
            pltpu.VMEM((levels, spectrum), jnp.bfloat16),
            pltpu.VMEM((levels, mem_dev, cols), jnp.bfloat16),
            pltpu.VMEM((levels, mem_dev, cols), jnp.float32),
            pltpu.VMEM((-(-levels // LANES) * LANES, -(-channels // LANES) * LANES), jnp.float32),
            pltpu.VMEM((rows, cols), jnp.float32),
        ]
        front_args = [
            jnp.transpose(jacobian_table),
            channel_list[None, :],
            jnp.transpose(background, (1, 0, 2)),
            send_slots[0],
        ]
        front_specs = [far, vmem, far, vmem]
    front = pl.pallas_call(
        functools.partial(front_kernel, n, select),
        out_shape=tuple(front_out),
        in_specs=front_specs,
        out_specs=(vmem,) * (len(front_out) - 1) + (pl.BlockSpec(memory_space=pltpu.SMEM),),
        scratch_shapes=front_scratch + [dma((2,)), dma((2,)), dma((2,))],
        compiler_params=pltpu.CompilerParams(
            collective_id=0, has_side_effects=True, vmem_limit_bytes=58 * 1024 * 1024
        ),
        name="front",
    )(*front_args)
    tables, count = front[-2:]
    if select:
        owned = front[0]
    else:
        chosen = (
            jnp.arange(jacobian_table.shape[0], dtype=jnp.int32)[:, None] == channel_list[None, :]
        ).astype(jnp.bfloat16)
        selected = jnp.einsum(
            "sl,sc->cl", jacobian_table, chosen, preferred_element_type=jnp.float32
        ).astype(jnp.bfloat16)
        owned = jnp.einsum(
            "cl,klx->ckx", selected, background, preferred_element_type=jnp.float32
        ).astype(jnp.bfloat16).reshape(rows, cols)

    def rest(choice, owned, tables, anomalies, weights, mean, footprint, footprint_weight, bias):
        part = rows // groups
        caps = CAPS[choice] if choice < len(CAPS) else None
        tight = caps is not None
        zone_cap, half_cap = caps or (LANES, LANES)
        pairs = zone_tiles // 2
        spare = (8, LANES)
        fold_rows, capped, widened = rows // FOLD, FOLD * zone_cap, FOLD * half_cap
        if tight:
            variant = [
                (3, fold_rows, capped),
                (1, rows, cols),
                (3, fold_rows, capped),
                (2, pairs, groups * cols, 2 * LANES),
                (1, FOLD * cols, capped),
                (3, zone_tiles, widened, 2 * LANES),
                (2, fold_rows, widened),
                (2, fold_rows, widened),
                (2, FOLD * cols, widened),
                (2, widened, capped),
            ]
        else:
            variant = [
                (3, zone_tiles, part, LANES),
                (3, rows, cols),
                spare,
                (4, pairs, groups * cols, 2 * LANES),
                (3, pairs, groups * cols, 2 * LANES),
            ] + [spare] * 5
        variant = [pltpu.VMEM(shape, jnp.bfloat16) for shape in variant]
        received, mixed, spread = pl.pallas_call(
            functools.partial(exchange_kernel, n, nm, chunks, caps),
            out_shape=(
                jax.ShapeDtypeStruct((n, part, LANES), jnp.bfloat16),
                jax.ShapeDtypeStruct((levels, mem_dev, cols), jnp.bfloat16),
                jax.ShapeDtypeStruct((n * slots, obs), jnp.bfloat16),
            ),
            in_specs=[vmem] * 7,
            out_specs=(hbm, hbm, hbm),
            scratch_shapes=[pltpu.VMEM((4, zone_tiles, part, LANES), jnp.bfloat16)]
            + variant
            + [
                pltpu.VMEM((max(nm - 1, 1), levels, mem_dev, cols), jnp.bfloat16),
                pltpu.VMEM((levels, mem_dev, cols), jnp.bfloat16),
                pltpu.VMEM((n * slots, obs), jnp.bfloat16),
                pltpu.VMEM((levels, cols), jnp.float32),
                pltpu.VMEM((members, members), jnp.float32),
                pltpu.VMEM((nm, mem_dev, mem_dev), jnp.bfloat16),
                dma((2,)),
                dma((3, chunks)),
                dma((nm,)),
                dma((nm,)),
                dma((4,)),
                dma((3,)),
                dma((3, chunks)),
                dma((2,)),
                dma((2, chunks)),
                dma((1,)),
                dma((8,)),
            ],
            compiler_params=pltpu.CompilerParams(
                collective_id=1 + choice, has_side_effects=True, vmem_limit_bytes=44 * 1024 * 1024
            ),
            name=f"exchange_{zone_cap}",
        )(owned, tables, anomalies, weights, mean, footprint, footprint_weight)
        return pl.pallas_call(
            functools.partial(combine_kernel, n, chunks),
            out_shape=(
                jax.ShapeDtypeStruct((channels, mem_dev, obs), jnp.float32),
                jax.ShapeDtypeStruct(mixed.shape, mixed.dtype),
            ),
            in_specs=[pl.BlockSpec(memory_space=pltpu.SMEM), vmem, vmem, vmem],
            out_specs=(hbm, hbm),
            scratch_shapes=[
                pltpu.VMEM((channels, mem_dev, obs), jnp.float32),
                dma((chunks + 1,)),
            ],
            compiler_params=pltpu.CompilerParams(vmem_limit_bytes=40 * 1024 * 1024),
            name="combine",
        )(bias, received, spread, mixed)

    operands = (
        owned,
        tables,
        jnp.transpose(anomalies, (1, 0, 2)),
        analysis_weights[0],
        background_mean,
        jnp.transpose(footprint),
        jnp.transpose(footprint_weight),
        channel_bias,
    )
    if foldable:
        prior, analysis = lax.switch(
            count[0, 0].astype(jnp.int32),
            [functools.partial(rest, choice) for choice in range(len(CAPS) + 1)],
            *operands,
        )
    else:
        prior, analysis = rest(len(CAPS), *operands)
    return jnp.transpose(analysis, (1, 0, 2)), prior


def solution(mesh):
    placed = (
        P("mem", None, "tile"),
        P("tile", None, None),
        P(None, "tile"),
        P("mem", None, "tile"),
        P(),
        P(),
        P("tile", None, None),
        P("tile", None),
        P("tile", None),
        P(),
    )
    return jax.shard_map(
        functools.partial(shards, mesh.shape["tile"], mesh.shape["mem"]),
        mesh=mesh,
        in_specs=placed,
        out_specs=(P("mem", None, "tile"), P(None, "mem", "tile")),
        check_vma=False,
    )
```
